128 devices in a mesh: ops: 32 (over z, y, core), site: 4 (over x).
Axes of the slice: x: 4, y: 4, z: 4, core: 2. Of those that a mesh axis runs over, the one named last changes fastest.
Arguments:
- wavefunction: bfloat16 [2048, 2048], replicated, may hold values from -6 to 6
- left_blocks: bfloat16 [256, 16, 192, 192], P('ops', 'site'), may hold values from -0.4375 to 0.4375
- right_blocks: bfloat16 [256, 16, 192, 192], P('ops', 'site'), may hold values from -0.078125 to 0.078125
- left_sector: int32 [2048], replicated, may hold values from 0 to 15, as said below
- right_sector: int32 [2048], replicated, may hold values from 0 to 15, as said below
- term_count: int32 [32], P('ops'), may hold values from 1 to 8, as said below
- left_energy: float32 [2048], replicated, may hold values from -1 to 1
- right_energy: float32 [2048], replicated, may hold values from -1 to 1
- subspace: bfloat16 [2, 16, 192, 2048], P(None, 'site'), may hold values from -0.0078125 to 0.0078125
Outputs:
- sigma: bfloat16 [16, 192, 2048], P('site')
- projections: float32 [2], replicated
The draws below stay inside these ranges and needn't reach their ends.
Inputs may be any that keep to these rules, and one draw needn't show every extreme that they name: `left_sector`: sector ids never fall along the bond; each of the 16 sectors has 1 to 192 states and one has exactly 192. `right_sector`: sector ids never fall along the bond; each of the 16 sectors has 1 to 192 states and one has exactly 192. `term_count`: some group has all 8 slots live.
All inputs are finite; a program needn't handle non-finite values.
Results may differ from the reference program's by a relative error of at most 0.0045.
Values may be sent and summed in bfloat16 or wider, within the bound.
No kernel may reach another device: no remote copies, remote signals or barrier semaphores. Data moves between devices by JAX's collectives and lax.ppermute only.
A program may use at most 192 MiB of HBM per device.

```python
import jax
import jax.numpy as jnp
from jax import lax

M = 2048
NB = 16
MAXB = 192
TERMS_DEV = 8
SUB = 2
TERMS = 256
N_OPS = 32


def draw_term_count(key, part):
    base_counts = jax.random.randint(jax.random.fold_in(key, 11), (N_OPS,), 1, TERMS_DEV // 2 + 1)
    fullest = jax.random.randint(jax.random.fold_in(key, 12), (), 0, N_OPS)
    return jnp.where(jnp.arange(N_OPS) == fullest, TERMS_DEV, base_counts).astype(jnp.int32)


def sector_draw(key):
    biggest = jax.random.randint(jax.random.fold_in(key, 1), (), 0, NB)
    remaining = jnp.int32(M - MAXB)
    sizes = []
    for label in range(NB):
        after = jnp.int32(NB - 1 - label) - (biggest > label).astype(jnp.int32)
        lower = jnp.maximum(1, remaining - after * MAXB)
        upper = jnp.minimum(MAXB, remaining - after)
        picked = jax.random.randint(jax.random.fold_in(key, 100 + label), (), lower, upper + 1)
        is_big = biggest == label
        size_now = jnp.where(is_big, jnp.int32(MAXB), picked).astype(jnp.int32)
        remaining = jnp.where(is_big, remaining, remaining - picked).astype(jnp.int32)
        sizes.append(size_now)
    ends = jnp.cumsum(jnp.stack(sizes)).astype(jnp.int32)
    positions = jnp.arange(M, dtype=jnp.int32)
    return jnp.sum((ends[None, :] <= positions[:, None]).astype(jnp.int32), axis=1).astype(jnp.int32)


def draw_left_sector(key, part):
    return sector_draw(jax.random.fold_in(key, 31))


def draw_right_sector(key, part):
    return sector_draw(jax.random.fold_in(key, 32))


def shard_levels(own_key, shape, shards, low, top_value):
    def one(axis_at, parts):
        heights = jax.random.uniform(jax.random.fold_in(jax.random.fold_in(own_key, 6), axis_at), (parts,), jnp.float32, low / len(shards), top_value / len(shards))
        return jnp.repeat(jnp.exp(heights), shape[axis_at] // parts).reshape((-1,) + (1,) * (len(shape) - axis_at - 1))

    loudness = one(*shards[0])
    for cut in shards[1:]:
        loudness = loudness * one(*cut)
    return loudness


def scatter_about(key, shape, deviation, reach, shards=(), held_as=jnp.bfloat16):
    drawn = deviation * jax.random.normal(key, shape, jnp.float32)
    if shards:
        drawn = drawn * shard_levels(key, shape, shards, -0.22, 0.18)
    return jnp.clip(drawn, -reach, reach).astype(held_as)


def setup_inputs(seed: int = 0) -> dict:
    seeds = jax.random.split(jax.random.key(seed), 10)
    wavefunction = scatter_about(seeds[0], (M, M), 1.0, 6.0)
    left_blocks = scatter_about(seeds[1], (TERMS, NB, MAXB, MAXB), MAXB ** -0.5, 0.4375, ((0, 32), (1, 4)))
    right_blocks = scatter_about(seeds[2], (TERMS, NB, MAXB, MAXB), (MAXB * TERMS_DEV * N_OPS // 8) ** -0.5, 0.078125, ((0, 32), (1, 4)))
    left_sector = draw_left_sector(jax.random.fold_in(seeds[9], 71), 0)
    right_sector = draw_right_sector(jax.random.fold_in(seeds[9], 71), 0)
    term_count = draw_term_count(jax.random.fold_in(seeds[9], 71), 0)
    left_energy = jnp.clip(jax.random.uniform(seeds[6], (M,), jnp.float32, -1.0, 1.0), -1.0, 1.0)
    right_energy = jnp.clip(jax.random.uniform(seeds[7], (M,), jnp.float32, -1.0, 1.0), -1.0, 1.0)
    subspace = scatter_about(seeds[8], (SUB, NB, MAXB, M), (1.0 / M), 0.0078125, ((1, 4),))
    return {"wavefunction": wavefunction, "left_blocks": left_blocks, "right_blocks": right_blocks, "left_sector": left_sector, "right_sector": right_sector, "term_count": term_count, "left_energy": left_energy, "right_energy": right_energy, "subspace": subspace}


def sector_tables(sector_ids, sectors):
    labels = jnp.arange(sectors, dtype=jnp.int32)
    sector_starts = jnp.sum((sector_ids[None, :] < labels[:, None]).astype(jnp.int32), axis=1)
    sector_sizes = jnp.sum((sector_ids[None, :] == labels[:, None]).astype(jnp.int32), axis=1)
    return sector_starts.astype(jnp.int32), sector_sizes.astype(jnp.int32)


def reference(wavefunction, left_blocks, right_blocks, left_sector, right_sector, term_count, left_energy, right_energy, subspace):
    left_start, left_size = sector_tables(left_sector, NB)
    right_start, right_size = sector_tables(right_sector, NB)
    positions = jnp.arange(MAXB, dtype=jnp.int32)
    left_inside = positions[None, :] < left_size[:, None]
    right_inside = positions[None, :] < right_size[:, None]
    left_masks = left_inside[:, :, None] & left_inside[:, None, :]
    right_masks = right_inside[:, :, None] & right_inside[:, None, :]
    psi_padded = jnp.concatenate([wavefunction, jnp.zeros((MAXB, M), wavefunction.dtype)], axis=0)
    psi_slabs = jax.vmap(lambda row_start: lax.dynamic_slice_in_dim(psi_padded, row_start, MAXB, 0))(left_start)
    slab_values = psi_slabs.astype(jnp.float32)
    row_count = NB * MAXB

    def term_product(accum, term_idx):
        live = (term_idx % TERMS_DEV) < term_count[term_idx // TERMS_DEV]

        def apply_term(summed_in):
            blocks = jnp.where(left_masks, left_blocks[term_idx], jnp.zeros((), left_blocks.dtype)).astype(jnp.float32)
            left_image = jnp.einsum("qab,qbc->qac", blocks, slab_values, precision=lax.Precision.HIGHEST)
            rounded = lax.optimization_barrier(left_image.astype(jnp.bfloat16)).astype(jnp.float32)
            rounded = rounded.reshape(row_count, M)
            padded_image = jnp.concatenate([rounded, jnp.zeros((row_count, MAXB), jnp.float32)], axis=1)
            right_terms = jnp.where(right_masks, right_blocks[term_idx], jnp.zeros((), right_blocks.dtype)).astype(jnp.float32)

            def one_sector(sector, summed):
                col_start = right_start[sector]
                window = lax.dynamic_slice_in_dim(padded_image, col_start, MAXB, 1)
                added = jnp.dot(window, right_terms[sector].T, precision=lax.Precision.HIGHEST)
                previous = lax.dynamic_slice_in_dim(summed, col_start, MAXB, 1)
                return lax.dynamic_update_slice_in_dim(summed, previous + added, col_start, 1)

            return lax.fori_loop(0, NB, one_sector, summed_in)

        return lax.cond(live, apply_term, lambda kept: kept, accum), None

    terms_padded, ignored = lax.scan(term_product, jnp.zeros((row_count, M + MAXB), jnp.float32), jnp.arange(TERMS_DEV * N_OPS, dtype=jnp.int32))
    terms = terms_padded[:, :M].reshape(NB, MAXB, M)
    psi_rows = jnp.where(left_inside[:, :, None], slab_values, jnp.float32(0.0))
    energy_padded = jnp.concatenate([left_energy, jnp.zeros((MAXB,), jnp.float32)])
    energy_rows = jax.vmap(lambda row_start: lax.dynamic_slice_in_dim(energy_padded, row_start, MAXB, 0))(left_start)
    sigma_full = terms + (energy_rows[:, :, None] + right_energy[None, None, :]) * psi_rows
    projections = jnp.sum(subspace.astype(jnp.float32) * sigma_full[None], axis=(1, 2, 3))
    return sigma_full.astype(jnp.bfloat16), projections
```

```python
import functools

import jax
import jax.numpy as jnp
from jax import lax
from jax.experimental import pallas as pl
from jax.experimental.pallas import tpu as pltpu
from jax.sharding import Mesh
from jax.sharding import PartitionSpec as P


OPS = ("z", "y", "core")
CHUNK = 4
WIN_ROWS = 256
WIN_COLS = 384
SLOT_COLS = 256


def params():
    return pltpu.CompilerParams(vmem_limit_bytes=56 * 1024 * 1024)


def sector_tables(sector_ids, sectors):
    labels = jnp.arange(sectors, dtype=jnp.int32)
    starts = jnp.sum((sector_ids[None, :] < labels[:, None]).astype(jnp.int32), axis=1)
    sizes = jnp.sum((sector_ids[None, :] == labels[:, None]).astype(jnp.int32), axis=1)
    return starts, sizes


def pack_body(blocks, first, second):
    for half, out in ((0, first), (1, second)):
        out[0, 0] = blocks[0, 2 * half, :, :128]
        out[0, 1] = blocks[0, 2 * half + 1, :, :128]
        out[0, 2] = jnp.concatenate([blocks[0, 2 * half, :, 128:192], blocks[0, 2 * half + 1, :, 128:192]], axis=1)


def pack_right(blocks, chunk):
    spec = pl.BlockSpec((1, 3, 192, 128), lambda i: (i, 0, 0, 0))
    shape = jax.ShapeDtypeStruct((CHUNK, 3, 192, 128), jnp.bfloat16)
    return pl.pallas_call(
        pack_body,
        grid=(CHUNK,),
        in_specs=[pl.BlockSpec((1, 4, 192, 192), lambda i: (i + CHUNK * chunk, 0, 0, 0))],
        out_specs=[spec, spec],
        out_shape=[shape, shape],
        name="pack_right",
    )(blocks)


def rows_body(tables, psi, out):
    for within in range(4):
        start = tables[within]
        size = tables[4 + within]
        base = pl.multiple_of(jnp.minimum((start // 16) * 16, psi.shape[0] - WIN_ROWS), 16)
        shift = start - base
        row = lax.broadcasted_iota(jnp.int32, (192, WIN_ROWS), 0)
        col = lax.broadcasted_iota(jnp.int32, (192, WIN_ROWS), 1)
        pick = jnp.where((col == row + shift) & (row < size), 1.0, 0.0).astype(jnp.bfloat16)
        got = jnp.dot(pick, psi[pl.ds(base, WIN_ROWS), :], preferred_element_type=jnp.float32)
        out[pl.ds(within * 192, 192), :] = got.astype(jnp.bfloat16)


def cols_body(tables, rows, out):
    q = pl.program_id(0)
    start = tables[q]
    size = tables[16 + q]
    base = pl.multiple_of(jnp.minimum((start // 128) * 128, rows.shape[1] - WIN_COLS), 128)
    shift = start - base
    row = lax.broadcasted_iota(jnp.int32, (WIN_COLS, SLOT_COLS), 0)
    lane = lax.broadcasted_iota(jnp.int32, (WIN_COLS, SLOT_COLS), 1)
    odd = q % 2
    at = jnp.where(lane < 128, lane, lane - 64 * odd)
    valid = jnp.where(lane < 128, 1, jnp.where(odd == 1, (lane >= 192).astype(jnp.int32), (lane < 192).astype(jnp.int32)))
    pick = jnp.where((row == at + shift) & (at < size) & (valid == 1), 1.0, 0.0).astype(jnp.bfloat16)
    got = jnp.dot(rows[:, pl.ds(base, WIN_COLS)], pick, preferred_element_type=jnp.float32)
    out[0] = got.astype(jnp.bfloat16)


def select_rows(left_table, psi):
    return pl.pallas_call(
        rows_body,
        in_specs=[pl.BlockSpec(memory_space=pltpu.SMEM), pl.BlockSpec(memory_space=pltpu.VMEM)],
        out_specs=pl.BlockSpec(memory_space=pltpu.VMEM),
        out_shape=jax.ShapeDtypeStruct((768, psi.shape[1]), jnp.bfloat16),
        compiler_params=params(),
        name="select_rows",
    )(left_table, psi)


def select_cols(right_table, rows):
    return pl.pallas_call(
        cols_body,
        grid=(16,),
        in_specs=[
            pl.BlockSpec(memory_space=pltpu.SMEM),
            pl.BlockSpec((768, rows.shape[1]), lambda q: (0, 0)),
        ],
        out_specs=pl.BlockSpec((1, 768, SLOT_COLS), lambda q: (q, 0, 0)),
        out_shape=jax.ShapeDtypeStruct((16, 768, SLOT_COLS), jnp.bfloat16),
        compiler_params=params(),
        name="select_cols",
    )(right_table, rows)


def multiply_body(has_acc, scalars, left, right_a, right_b, psi, *rest):
    if has_acc:
        acc_in, out, image = rest
    else:
        out, image = rest
    live = scalars[1]
    if has_acc:
        out[...] = acc_in[...]
    else:
        out[...] = jnp.zeros(out.shape, jnp.float32)

    def pair(p, carry):
        for q in range(4):
            right = right_a if q < 2 else right_b
            total = None
            for u in range(2):
                t = 2 * p + u
                for within in range(4):
                    got = jnp.dot(
                        left[t, within], psi[q, pl.ds(within * 192, 192), :], preferred_element_type=jnp.float32
                    )
                    if u == 1:
                        got = jnp.where(t < live, got, 0.0)
                    image[u, pl.ds(within * 192, 192), :] = got.astype(jnp.bfloat16)
                block = jnp.concatenate([right[t, q % 2], right[t, 2]], axis=1)
                part = lax.dot_general(
                    image[u], block, (((1,), (1,)), ((), ())), preferred_element_type=jnp.float32
                )
                total = part if total is None else total + part
            out[:, q * SLOT_COLS : q * SLOT_COLS + 192] += total
        return carry

    lax.fori_loop(0, (live + 1) // 2, pair, 0)


def multiply(scalars, left, chunk, right_a, right_b, psi_cols, acc=None):
    has_acc = acc is not None
    grid_spec = pltpu.PrefetchScalarGridSpec(
        num_scalar_prefetch=1,
        grid=(1,),
        in_specs=[
            pl.BlockSpec((CHUNK, 4, 192, 192), lambda i, s: (chunk, 0, 0, 0)),
            pl.BlockSpec((CHUNK, 3, 192, 128), lambda i, s: (0, 0, 0, 0)),
            pl.BlockSpec((CHUNK, 3, 192, 128), lambda i, s: (0, 0, 0, 0)),
            pl.BlockSpec((4, 768, SLOT_COLS), lambda i, s: (s[0], 0, 0)),
        ]
        + ([pl.BlockSpec((768, 4 * SLOT_COLS), lambda i, s: (0, 0))] if has_acc else []),
        out_specs=pl.BlockSpec((768, 4 * SLOT_COLS), lambda i, s: (0, 0)),
        scratch_shapes=[pltpu.VMEM((2, 768, SLOT_COLS), jnp.bfloat16)],
    )
    args = (scalars, left, right_a, right_b, psi_cols) + ((acc,) if has_acc else ())
    return pl.pallas_call(
        functools.partial(multiply_body, has_acc),
        grid_spec=grid_spec,
        out_shape=jax.ShapeDtypeStruct((768, 4 * SLOT_COLS), jnp.float32),
        input_output_aliases={5: 0} if has_acc else {},
        compiler_params=params(),
        cost_estimate=pl.CostEstimate(flops=7 * 10**9, bytes_accessed=8 * 2**20, transcendentals=0),
        name="multiply",
    )(*args)


def finish_kernel(tables, acc0, acc1, acc2, acc3, rows, subspace, energies, right_energy, out, proj, total):
    within = pl.program_id(0)
    site = tables[36]
    diagonal_on = tables[37].astype(jnp.float32)
    width = out.shape[1]
    total[...] = (energies[...] + right_energy[...]) * rows[...].astype(jnp.float32) * diagonal_on
    lane = lax.broadcasted_iota(jnp.int32, (192, SLOT_COLS), 1)
    for rel, acc in enumerate((acc0, acc1, acc2, acc3)):
        for q in range(4):
            sector = ((site + rel) % 4) * 4 + q
            start = tables[sector]
            size = tables[16 + sector]
            base = pl.multiple_of(jnp.minimum((start // 128) * 128, width - WIN_COLS), 128)
            shift = start - base
            piece = jnp.where(lane < size, acc[:, q * SLOT_COLS : (q + 1) * SLOT_COLS], 0.0)
            piece = jnp.concatenate([piece, jnp.zeros((192, WIN_COLS - SLOT_COLS), jnp.float32)], axis=1)
            total[:, pl.ds(base, WIN_COLS)] += pltpu.roll(piece, shift, 1)
    row = lax.broadcasted_iota(jnp.int32, (192, width), 0)
    kept = jnp.where(row < tables[32 + within], total[...], 0.0)
    out[...] = kept.astype(jnp.bfloat16)
    for k in range(2):
        part = jnp.sum(subspace[k, 0].astype(jnp.float32) * kept, axis=0, keepdims=True)

        @pl.when(within == 0)
        def _():
            proj[k : k + 1, :] = part

        @pl.when(within > 0)
        def _():
            proj[k : k + 1, :] += part


def finish(tables, accs, rows, subspace, energies, right_energy):
    width = rows.shape[1]
    acc_spec = pl.BlockSpec((192, 4 * SLOT_COLS), lambda i: (i, 0))
    return pl.pallas_call(
        finish_kernel,
        grid=(4,),
        in_specs=[pl.BlockSpec(memory_space=pltpu.SMEM)]
        + [acc_spec] * 4
        + [
            pl.BlockSpec((192, width), lambda i: (i, 0)),
            pl.BlockSpec((2, 1, 192, width), lambda i: (0, i, 0, 0)),
            pl.BlockSpec((192, 1), lambda i: (i, 0)),
            pl.BlockSpec((1, width), lambda i: (0, 0)),
        ],
        out_specs=[pl.BlockSpec((192, width), lambda i: (i, 0)), pl.BlockSpec((2, width), lambda i: (0, 0))],
        out_shape=[
            jax.ShapeDtypeStruct((768, width), jnp.bfloat16),
            jax.ShapeDtypeStruct((2, width), jnp.float32),
        ],
        scratch_shapes=[pltpu.VMEM((192, width), jnp.float32)],
        compiler_params=params(),
        name="finish",
    )(tables, *accs, rows, subspace, energies, right_energy)


def shifted(value, axis, by):
    size = lax.axis_size(axis)
    return lax.ppermute(value, axis, [(i, (i + by) % size) for i in range(size)])


def small_sum(value, axis):
    size = lax.axis_size(axis)
    me = lax.axis_index(axis)
    got = jnp.stack([value] + [shifted(value, axis, k) for k in range(1, size)])
    order = (me - jnp.arange(size)) % size
    return jnp.take(got, order, axis=0).sum(axis=0)


def local(
    wavefunction,
    left_blocks,
    right_blocks,
    left_sector,
    right_sector,
    term_count,
    left_energy,
    right_energy,
    subspace,
):
    bond = wavefunction.shape[0]
    site = lax.axis_index("site")
    core = lax.axis_index("core")
    active = term_count[0]
    left_start, left_size = sector_tables(left_sector, 16)
    right_start, right_size = sector_tables(right_sector, 16)
    my_start = lax.dynamic_slice_in_dim(left_start, site * 4, 4)
    my_size = lax.dynamic_slice_in_dim(left_size, site * 4, 4)
    left_table = jnp.concatenate([my_start, my_size])
    right_table = jnp.concatenate([right_start, right_size])
    first_ops = (lax.axis_index(OPS) == 0).astype(jnp.int32)
    finish_table = jnp.concatenate([right_table, my_size, jnp.stack([site, first_ops])])
    energy_padded = jnp.concatenate([left_energy, jnp.zeros((192,), jnp.float32)])
    energies = jnp.concatenate(
        [lax.dynamic_slice_in_dim(energy_padded, my_start[w], 192) for w in range(4)]
    )[:, None]

    early = jnp.minimum(active, CHUNK)
    late = jnp.maximum(active - CHUNK, 0)

    def scalars(rel, live):
        return jnp.stack([(site + rel) % 4, live])

    first_a, second_a = pack_right(right_blocks, 0)
    first_b, second_b = pack_right(right_blocks, 1)

    prev_first = shifted(first_a, "site", 1)
    next_second = shifted(second_a, "site", -1)
    prev_second = shifted(second_a, "site", 1)
    next_first = shifted(first_a, "site", -1)

    rows = select_rows(left_table, wavefunction)
    psi_cols = select_cols(right_table, rows)

    own = multiply(scalars(0, early), left_blocks, 0, first_a, second_a, psi_cols)
    own = multiply(scalars(0, late), left_blocks, 1, first_b, second_b, psi_cols, own)

    def early_groups(prev_first, prev_second, next_first, next_second):
        far_first = shifted(prev_first, "site", 1)
        far_second = shifted(next_second, "site", -1)
        prev = multiply(scalars(3, early), left_blocks, 0, prev_first, prev_second, psi_cols)
        nxt = multiply(scalars(1, early), left_blocks, 0, next_first, next_second, psi_cols)
        far = multiply(scalars(2, early), left_blocks, 0, far_first, far_second, psi_cols)
        return nxt, far, prev

    def more(prev_first, prev_second, next_first, next_second):
        moved = []
        for by in (1, -1, 2):
            moved.append((shifted(first_b, "site", by), shifted(second_b, "site", by)))
        nxt, far, prev = early_groups(prev_first, prev_second, next_first, next_second)
        prev = multiply(scalars(3, late), left_blocks, 1, *moved[0], psi_cols, prev)
        nxt = multiply(scalars(1, late), left_blocks, 1, *moved[1], psi_cols, nxt)
        far = multiply(scalars(2, late), left_blocks, 1, *moved[2], psi_cols, far)
        return nxt, far, prev

    nxt, far, prev = lax.cond(
        late > 0, more, early_groups, prev_first, prev_second, next_first, next_second
    )

    part, proj = finish(
        finish_table, (own, nxt, far, prev), rows, subspace, energies, right_energy[None, :]
    )
    half = part.shape[0] // 2
    away = lax.ppermute(lax.dynamic_slice_in_dim(part, (1 - core) * half, half, 0), "core", [(0, 1), (1, 0)])
    mine = lax.dynamic_slice_in_dim(part, core * half, half, 0)
    both = (mine.astype(jnp.float32) + away.astype(jnp.float32)).astype(jnp.bfloat16)

    plane = lax.axis_size(("z", "y"))
    share = half // plane
    pieces = lax.all_to_all(both.reshape(plane, share, bond), ("z", "y"), 0, 0, tiled=True)
    summed = jnp.sum(pieces.astype(jnp.float32), axis=0).astype(jnp.bfloat16)
    gathered = lax.all_to_all(
        jnp.broadcast_to(summed[None], (plane, share, bond)), ("z", "y"), 0, 0, tiled=True
    ).reshape(half, bond)
    other = lax.ppermute(gathered, "core", [(0, 1), (1, 0)])
    sigma = jnp.concatenate(
        [jnp.where(core == 0, gathered, other), jnp.where(core == 0, other, gathered)], axis=0
    ).reshape(4, 192, bond)

    projections = jnp.broadcast_to(jnp.sum(proj, axis=1)[None, :], (8, 2))
    for axis in ("core", "y", "z", "site"):
        projections = small_sum(projections, axis)
    return sigma, projections[0]


def solution(mesh):
    shape = dict(mesh.shape)
    ops = shape["ops"]
    parts = Mesh(mesh.devices.reshape(4, ops // 8, 2, shape["site"]), ("z", "y", "core", "site"))
    in_specs = (
        P(),
        P(OPS, "site", None, None),
        P(OPS, "site", None, None),
        P(),
        P(),
        P(OPS),
        P(),
        P(),
        P(None, "site", None, None),
    )
    out_specs = (P("site", None, None), P())
    return jax.shard_map(local, mesh=parts, in_specs=in_specs, out_specs=out_specs, check_vma=False)
```

```python
import functools

import jax
import jax.numpy as jnp
from jax import lax
from jax.experimental import pallas as pl
from jax.experimental.pallas import tpu as pltpu
from jax.sharding import Mesh
from jax.sharding import PartitionSpec as P


OPS = ("z", "y", "core")
CHUNK = 4
WIN_ROWS = 256
WIN_COLS = 384
SLOT_COLS = 256
GROUP_COLS = 4 * SLOT_COLS
EXTRA = 128

MY_START, MY_SIZE, RIGHT_START, RIGHT_SIZE, SITE, CORE, FIRST_OPS, LIVE = 0, 4, 8, 24, 40, 41, 42, 43


def params():
    return pltpu.CompilerParams(vmem_limit_bytes=56 * 1024 * 1024)


def sector_tables(sector_ids, sectors):
    labels = jnp.arange(sectors, dtype=jnp.int32)
    starts = jnp.sum((sector_ids[None, :] < labels[:, None]).astype(jnp.int32), axis=1)
    sizes = jnp.sum((sector_ids[None, :] == labels[:, None]).astype(jnp.int32), axis=1)
    return starts, sizes


def pack_one(blocks, slot, half, out, index):
    out[index + (0,)] = blocks[slot, 2 * half, :, :128]
    out[index + (1,)] = blocks[slot, 2 * half + 1, :, :128]
    out[index + (2,)] = jnp.concatenate(
        [blocks[slot, 2 * half, :, 128:192], blocks[slot, 2 * half + 1, :, 128:192]], axis=1
    )


def pack_early_body(blocks, first, second):
    for slot in range(2):
        pack_one(blocks, slot, 0, first, (slot,))
        pack_one(blocks, slot, 1, second, (slot,))


def pack_late_body(blocks, out):
    for slot in range(2):
        for half in range(2):
            pack_one(blocks, slot, half, out, (0, slot, half))


def pack_early(blocks):
    spec = pl.BlockSpec((2, 3, 192, 128), lambda i: (i, 0, 0, 0))
    shape = jax.ShapeDtypeStruct((CHUNK, 3, 192, 128), jnp.bfloat16)
    return pl.pallas_call(
        pack_early_body,
        grid=(2,),
        in_specs=[pl.BlockSpec((2, 4, 192, 192), lambda i: (i, 0, 0, 0))],
        out_specs=[spec, spec],
        out_shape=[shape, shape],
        name="pack_early",
    )(blocks)


def pack_late(blocks):
    return pl.pallas_call(
        pack_late_body,
        grid=(2,),
        in_specs=[pl.BlockSpec((2, 4, 192, 192), lambda i: (i + 2, 0, 0, 0))],
        out_specs=pl.BlockSpec((1, 2, 2, 3, 192, 128), lambda i: (i, 0, 0, 0, 0, 0)),
        out_shape=jax.ShapeDtypeStruct((2, 2, 2, 3, 192, 128), jnp.bfloat16),
        name="pack_late",
    )(blocks)


def select_body(table, psi, rows, cols, window, sems):
    group = pl.program_id(0)

    @pl.when(group == 0)
    def _():
        copies = []
        shifts = []
        for within in range(4):
            start = table[MY_START + within]
            base = pl.multiple_of(jnp.minimum((start // 16) * 16, psi.shape[0] - WIN_ROWS), 16)
            shifts.append(start - base)
            copies.append(
                pltpu.make_async_copy(psi.at[pl.ds(base, WIN_ROWS), :], window.at[within], sems.at[within])
            )
        for copy in copies:
            copy.start()
        row = lax.broadcasted_iota(jnp.int32, (192, WIN_ROWS), 0)
        col = lax.broadcasted_iota(jnp.int32, (192, WIN_ROWS), 1)
        for within in range(4):
            copies[within].wait()
            kept = (col == row + shifts[within]) & (row < table[MY_SIZE + within])
            pick = jnp.where(kept, 1.0, 0.0).astype(jnp.bfloat16)
            got = jnp.dot(pick, window[within], preferred_element_type=jnp.float32)
            rows[pl.ds(within * 192, 192), :] = got.astype(jnp.bfloat16)

    row = lax.broadcasted_iota(jnp.int32, (WIN_COLS, SLOT_COLS), 0)
    lane = lax.broadcasted_iota(jnp.int32, (WIN_COLS, SLOT_COLS), 1)
    for q in range(4):
        start = table[RIGHT_START + 4 * group + q]
        size = table[RIGHT_SIZE + 4 * group + q]
        base = pl.multiple_of(jnp.minimum((start // 128) * 128, rows.shape[1] - WIN_COLS), 128)
        if q % 2:
            at = jnp.where(lane < 128, lane, jnp.where(lane < 192, size, lane - 64))
        else:
            at = lane
        kept = (row == at + (start - base)) & (at < size)
        pick = jnp.where(kept, 1.0, 0.0).astype(jnp.bfloat16)
        got = jnp.dot(rows[:, pl.ds(base, WIN_COLS)], pick, preferred_element_type=jnp.float32)
        cols[0, :, q * SLOT_COLS : (q + 1) * SLOT_COLS] = got.astype(jnp.bfloat16)


def select(table, psi):
    bond = psi.shape[1]
    return pl.pallas_call(
        select_body,
        grid=(4,),
        in_specs=[pl.BlockSpec(memory_space=pltpu.SMEM), pl.BlockSpec(memory_space=pltpu.HBM)],
        out_specs=[
            pl.BlockSpec((768, bond), lambda g: (0, 0)),
            pl.BlockSpec((1, 768, GROUP_COLS), lambda g: (g, 0, 0)),
        ],
        out_shape=[
            jax.ShapeDtypeStruct((768, bond), jnp.bfloat16),
            jax.ShapeDtypeStruct((4, 768, GROUP_COLS), jnp.bfloat16),
        ],
        scratch_shapes=[pltpu.VMEM((4, WIN_ROWS, bond), jnp.bfloat16), pltpu.SemaphoreType.DMA((4,))],
        compiler_params=params(),
        name="select",
    )(table, psi)


def products_body(rels, pairs, has_acc, table, left, left_late, psi, *rest):
    groups = len(rels)
    early = 0 in pairs
    late = 2 in pairs
    rest = list(rest)
    rights = []
    for _ in rels:
        one = {}
        if early:
            one["a"], one["b"] = rest.pop(0), rest.pop(0)
        if late:
            one["e"], one["f"] = rest.pop(0), rest.pop(0)
        rights.append(one)
    acc_in = rest.pop(0) if has_acc else None
    out, left_v, right_v, psi_v, acc_v, image, sem_left, sem_right, sem_psi, sem_acc = rest
    first = 0 if early else 2
    live_e = table[LIVE + 2] if late else None
    live_f = table[LIVE + 3] if late else None

    copies_left = []
    if early:
        copies_left.append((None, pltpu.make_async_copy(left.at[pl.ds(0, 4)], left_v.at[pl.ds(0, 4)], sem_left.at[0])))
    if late:
        at = 4 - 2 * first
        copies_left.append((live_e, pltpu.make_async_copy(left_late, left_v.at[pl.ds(at, 2)], sem_left.at[1])))
        copies_left.append(
            (live_f, pltpu.make_async_copy(left.at[pl.ds(6, 2)], left_v.at[pl.ds(at + 2, 2)], sem_left.at[2]))
        )

    def right_copies(i):
        found = []
        if early:
            found.append(
                (None, pltpu.make_async_copy(rights[i]["a"], right_v.at[i, 0, pl.ds(0, 4)], sem_right.at[i, 0]))
            )
            found.append(
                (None, pltpu.make_async_copy(rights[i]["b"], right_v.at[i, 1, pl.ds(0, 4)], sem_right.at[i, 1]))
            )
        if late:
            at = 4 - 2 * first
            for name, live, place, where in (("e", live_e, 2, at), ("f", live_f, 4, at + 2)):
                for half in range(2):
                    found.append(
                        (
                            live,
                            pltpu.make_async_copy(
                                rights[i][name].at[:, half],
                                right_v.at[i, half, pl.ds(where, 2)],
                                sem_right.at[i, place + half],
                            ),
                        )
                    )
        return found

    def act(copies, what):
        for live, copy in copies:
            if live is None:
                getattr(copy, what)()
            else:

                @pl.when(live > 0)
                def _():
                    getattr(copy, what)()

    site = table[SITE]
    psi_copies = [
        pltpu.make_async_copy(psi.at[(site + rels[i]) % 4], psi_v.at[i], sem_psi.at[i]) for i in range(groups)
    ]
    acc_copies = [
        pltpu.make_async_copy(acc_in.at[i], acc_v.at[i], sem_acc.at[i]) if has_acc else None for i in range(groups)
    ]
    out_copies = [pltpu.make_async_copy(acc_v.at[i], out.at[i], sem_acc.at[groups + i]) for i in range(groups)]
    all_right = [right_copies(i) for i in range(groups)]
    act(copies_left, "start")
    for i in range(groups):
        act(all_right[i], "start")
        psi_copies[i].start()
        if has_acc:
            acc_copies[i].start()
    act(copies_left, "wait")

    def one_group(i, carry):
        for j in range(groups):

            @pl.when(i == j)
            def _():
                act(all_right[j], "wait")
                psi_copies[j].wait()
                if has_acc:
                    acc_copies[j].wait()

        if not has_acc:
            acc_v[i] = jnp.zeros(acc_v.shape[1:], jnp.float32)

        def one_pair(p, inner):
            live = table[LIVE + first + p]

            @pl.when(live > 0)
            def _():
                for u in range(2):
                    for within in range(4):
                        got = jnp.dot(
                            left_v[2 * p + u, within],
                            psi_v[i, within * 192 : (within + 1) * 192, :],
                            preferred_element_type=jnp.float32,
                        )
                        if u == 1:
                            got = jnp.where(live > 1, got, 0.0)
                        image[u, within * 192 : (within + 1) * 192, :] = got.astype(jnp.bfloat16)
                for q in range(4):
                    parts = []
                    for u in range(2):
                        block = jnp.concatenate(
                            [right_v[i, q // 2, 2 * p + u, q % 2], right_v[i, q // 2, 2 * p + u, 2]], axis=1
                        )
                        block = jnp.concatenate([block, jnp.zeros((64, 256), jnp.bfloat16)], axis=0)
                        parts.append(
                            lax.dot_general(
                                image[u, :, q * SLOT_COLS : (q + 1) * SLOT_COLS],
                                block,
                                (((1,), (1,)), ((), ())),
                                preferred_element_type=jnp.float32,
                            )
                        )
                    acc_v[i, :, q * SLOT_COLS : (q + 1) * SLOT_COLS] += parts[0] + parts[1]

            return inner

        lax.fori_loop(0, len(pairs), one_pair, 0)
        for j in range(groups):

            @pl.when(i == j)
            def _():
                out_copies[j].start()

        return carry

    lax.fori_loop(0, groups, one_group, 0)
    for copy in out_copies:
        copy.wait()


def products(rels, pairs, table, left, left_late, psi, rights, acc=None):
    groups = len(rels)
    slots = 2 * len(pairs)
    flat = [one for several in rights for one in several]
    args = [table, left, left_late, psi] + flat + ([] if acc is None else [acc])
    hbm = pl.BlockSpec(memory_space=pltpu.HBM)
    flops = groups * 2 * 1024 * 768 * (192 + 256) * 4
    return pl.pallas_call(
        functools.partial(products_body, tuple(rels), tuple(pairs), acc is not None),
        in_specs=[pl.BlockSpec(memory_space=pltpu.SMEM)] + [hbm] * (len(args) - 1),
        out_specs=hbm,
        out_shape=jax.ShapeDtypeStruct((groups, 768, GROUP_COLS), jnp.float32),
        scratch_shapes=[
            pltpu.VMEM((slots, 4, 192, 192), jnp.bfloat16),
            pltpu.VMEM((groups, 2, slots, 3, 192, 128), jnp.bfloat16),
            pltpu.VMEM((groups, 768, GROUP_COLS), jnp.bfloat16),
            pltpu.VMEM((groups, 768, GROUP_COLS), jnp.float32),
            pltpu.VMEM((2, 768, GROUP_COLS), jnp.bfloat16),
            pltpu.SemaphoreType.DMA((3,)),
            pltpu.SemaphoreType.DMA((groups, 6)),
            pltpu.SemaphoreType.DMA((groups,)),
            pltpu.SemaphoreType.DMA((2 * groups,)),
        ],
        input_output_aliases={} if acc is None else {len(args) - 1: 0},
        compiler_params=params(),
        cost_estimate=pl.CostEstimate(flops=flops, bytes_accessed=8 * 2**20, transcendentals=0),
        name="products",
    )(*args)


def finish_body(table, own, others, rows, subspace, energies, right_energy, send, mine, total, proj):
    step = pl.program_id(0)
    core = table[CORE]
    within = 2 * jnp.where(step < 2, 1 - core, core) + step % 2
    site = table[SITE]
    diagonal_on = table[FIRST_OPS].astype(jnp.float32)
    width = rows.shape[1]
    total[...] = (energies[...] + right_energy[...]) * rows[...].astype(jnp.float32) * diagonal_on
    lane = lax.broadcasted_iota(jnp.int32, (192, SLOT_COLS), 1)
    for rel in range(4):
        for q in range(4):
            sector = ((site + rel) % 4) * 4 + q
            start = table[RIGHT_START + sector]
            size = table[RIGHT_SIZE + sector]
            base = pl.multiple_of(jnp.minimum((start // 128) * 128, width - WIN_COLS), 128)
            acc = own[0] if rel == 0 else others[rel - 1]
            piece = jnp.where(lane < size, acc[:, q * SLOT_COLS : (q + 1) * SLOT_COLS], 0.0)
            piece = jnp.concatenate([piece, jnp.zeros((192, WIN_COLS - SLOT_COLS), jnp.float32)], axis=1)
            total[:, pl.ds(base, WIN_COLS)] += pltpu.roll(piece, start - base, 1)
    row = lax.broadcasted_iota(jnp.int32, (192, width), 0)
    kept = jnp.where(row < table[MY_SIZE + within], total[...], 0.0)

    @pl.when(step == 0)
    def _():
        proj[...] = jnp.zeros(proj.shape, jnp.float32)

    for k in range(2):
        part = subspace[k, 0].astype(jnp.float32) * kept
        proj[k] += jnp.sum(part.reshape(24, 8, width), axis=0)

    @pl.when(step < 2)
    def _():
        send[...] = kept.astype(jnp.bfloat16)

    @pl.when(step >= 2)
    def _():
        mine[...] = kept.astype(jnp.bfloat16)


def finish(table, own, others, rows, subspace, energies, right_energy):
    width = rows.shape[1]

    def place(i, table):
        core = table[CORE]
        return 2 * jnp.where(i < 2, 1 - core, core) + i % 2

    half = jax.ShapeDtypeStruct((384, width), jnp.bfloat16)
    grid_spec = pltpu.PrefetchScalarGridSpec(
        num_scalar_prefetch=1,
        grid=(4,),
        in_specs=[
            pl.BlockSpec((1, 192, GROUP_COLS), lambda i, t: (0, place(i, t), 0)),
            pl.BlockSpec((3, 192, GROUP_COLS), lambda i, t: (0, place(i, t), 0)),
            pl.BlockSpec((192, width), lambda i, t: (place(i, t), 0)),
            pl.BlockSpec((2, 1, 192, width), lambda i, t: (0, place(i, t), 0, 0)),
            pl.BlockSpec((192, 1), lambda i, t: (place(i, t), 0)),
            pl.BlockSpec((1, width), lambda i, t: (0, 0)),
        ],
        out_specs=[
            pl.BlockSpec((192, width), lambda i, t: (jnp.minimum(i, 1), 0)),
            pl.BlockSpec((192, width), lambda i, t: (jnp.maximum(i - 2, 0), 0)),
            pl.BlockSpec((2, 8, width), lambda i, t: (0, 0, 0)),
        ],
        scratch_shapes=[pltpu.VMEM((192, width), jnp.float32)],
    )

    def body(table, own, others, rows, subspace, energies, right_energy, send, mine, proj, total):
        finish_body(table, own, others, rows, subspace, energies, right_energy, send, mine, total, proj)

    return pl.pallas_call(
        body,
        grid_spec=grid_spec,
        out_shape=[half, half, jax.ShapeDtypeStruct((2, 8, width), jnp.float32)],
        compiler_params=params(),
        name="finish",
    )(table, own, others, rows, subspace, energies, right_energy)


def shifted(value, axis, by):
    size = lax.axis_size(axis)
    return lax.ppermute(value, axis, [(i, (i + by) % size) for i in range(size)])


def small_sum(value, axis):
    size = lax.axis_size(axis)
    me = lax.axis_index(axis)
    got = jnp.stack([value] + [shifted(value, axis, k) for k in range(1, size)])
    order = (me - jnp.arange(size)) % size
    return jnp.take(got, order, axis=0).sum(axis=0)


def local(
    wavefunction,
    left_blocks,
    right_blocks,
    left_sector,
    right_sector,
    term_count,
    left_energy,
    right_energy,
    subspace,
):
    bond = wavefunction.shape[0]
    site = lax.axis_index("site")
    core = lax.axis_index("core")
    first_a, second_a = pack_early(right_blocks)
    prev_first = shifted(first_a, "site", 1)
    next_second = shifted(second_a, "site", -1)
    prev_second = shifted(second_a, "site", 1)
    next_first = shifted(first_a, "site", -1)

    left_start, left_size = sector_tables(left_sector, 16)
    right_start, right_size = sector_tables(right_sector, 16)
    my_start = lax.dynamic_slice_in_dim(left_start, site * 4, 4)
    my_size = lax.dynamic_slice_in_dim(left_size, site * 4, 4)
    active = term_count[0]
    beside = shifted(term_count, "core", 1)[0]
    heavy = active > CHUNK
    heavy_beside = beside > CHUNK
    live_e = jnp.where(heavy, jnp.clip(active - 4, 0, 2), jnp.clip(beside - 6, 0, 2))
    live_f = jnp.where(heavy & heavy_beside, jnp.clip(active - 6, 0, 2), 0)
    few = jnp.stack(
        [
            site,
            core,
            (lax.axis_index(OPS) == 0).astype(jnp.int32),
            jnp.minimum(active, 2),
            jnp.clip(active - 2, 0, 2),
            live_e,
            live_f,
        ]
    )
    table = jnp.concatenate([my_start, my_size, right_start, right_size, few])
    energy_padded = jnp.concatenate([left_energy, jnp.zeros((192,), jnp.float32)])
    energies = jnp.concatenate(
        [lax.dynamic_slice_in_dim(energy_padded, my_start[w], 192) for w in range(4)]
    )[:, None]

    rows, psi = select(table, wavefunction)
    late = pack_late(right_blocks)
    right_e = jnp.where(heavy, late[0], shifted(late[1], "core", 1))
    right_f = late[1]
    left_e = jnp.where(heavy, left_blocks[4:6], shifted(left_blocks[6:8], "core", 1))

    own = products(
        (0,), (0, 1, 2, 3), table, left_blocks, left_e, psi, [(first_a, second_a, right_e, right_f)]
    )

    def early_groups(prev_first, prev_second, next_first, next_second):
        far_first = shifted(prev_first, "site", 1)
        far_second = shifted(next_second, "site", -1)
        return products(
            (1, 2, 3),
            (0, 1),
            table,
            left_blocks,
            left_e,
            psi,
            [(next_first, next_second), (far_first, far_second), (prev_first, prev_second)],
        )

    def more(prev_first, prev_second, next_first, next_second):
        moved_e = [shifted(right_e, "site", by) for by in (-1, 2, 1)]
        others = early_groups(prev_first, prev_second, next_first, next_second)
        moved_f = lax.cond(
            heavy & heavy_beside,
            lambda right: [shifted(right, "site", by) for by in (-1, 2, 1)],
            lambda right: [right, right, right],
            right_f,
        )
        return products(
            (1, 2, 3), (2, 3), table, left_blocks, left_e, psi, list(zip(moved_e, moved_f, strict=True)), others
        )

    others = lax.cond(
        heavy | heavy_beside, more, early_groups, prev_first, prev_second, next_first, next_second
    )

    send, mine, proj = finish(table, own, others, rows, subspace, energies, right_energy[None, :])
    proj = jnp.sum(proj, axis=(1, 2))
    swap = [(0, 1), (1, 0)]
    away = lax.ppermute(send, "core", swap)
    proj = proj + lax.ppermute(jnp.broadcast_to(proj[None, :], (8, 2)), "core", swap)[0]
    both = (mine.astype(jnp.float32) + away.astype(jnp.float32)).astype(jnp.bfloat16)

    high = lax.reduce_precision(proj, 8, 7)
    middle = lax.reduce_precision(proj - high, 8, 7)
    thirds = jnp.concatenate([high, middle, proj - high - middle]).astype(jnp.bfloat16)
    plane = lax.axis_size(("z", "y"))
    half = both.shape[0]
    share = half // plane
    extra = jnp.broadcast_to(jnp.pad(thirds, (0, EXTRA - 6))[None, :], (half, EXTRA))
    both = jnp.concatenate([both, extra], axis=1)

    pieces = lax.all_to_all(both.reshape(plane, share, bond + EXTRA), ("z", "y"), 0, 0, tiled=True)
    added = jnp.sum(pieces.astype(jnp.float32), axis=0)
    summed = added[:, :bond].astype(jnp.bfloat16)
    gathered = lax.all_to_all(
        jnp.broadcast_to(summed[None], (plane, share, bond)), ("z", "y"), 0, 0, tiled=True
    ).reshape(half, bond)
    whole = added[:8, bond : bond + 2] + added[:8, bond + 2 : bond + 4] + added[:8, bond + 4 : bond + 6]
    projections = small_sum(whole, "site")
    other = lax.ppermute(gathered, "core", swap)
    sigma = jnp.concatenate(
        [jnp.where(core == 0, gathered, other), jnp.where(core == 0, other, gathered)], axis=0
    ).reshape(4, 192, bond)
    return sigma, projections[0]


def solution(mesh):
    shape = dict(mesh.shape)
    ops = shape["ops"]
    parts = Mesh(mesh.devices.reshape(4, ops // 8, 2, shape["site"]), ("z", "y", "core", "site"))
    in_specs = (
        P(),
        P(OPS, "site", None, None),
        P(OPS, "site", None, None),
        P(),
        P(),
        P(OPS),
        P(),
        P(),
        P(None, "site", None, None),
    )
    out_specs = (P("site", None, None), P())
    return jax.shard_map(local, mesh=parts, in_specs=in_specs, out_specs=out_specs, check_vma=False)
```

```python
import functools

import jax
import jax.numpy as jnp
from jax import lax
from jax.experimental import pallas as pl
from jax.experimental.pallas import tpu as pltpu
from jax.sharding import Mesh
from jax.sharding import PartitionSpec as P


OPS = ("z", "y", "core")
CHUNK = 4
WIN_ROWS = 256
WIN_COLS = 384
SLOT_COLS = 256
GROUP_COLS = 4 * SLOT_COLS
EXTRA = 128

MY_START, MY_SIZE, RIGHT_START, RIGHT_SIZE = 0, 4, 8, 24
SITE, CORE, FIRST_OPS = 0, 1, 2


def params():
    return pltpu.CompilerParams(vmem_limit_bytes=56 * 1024 * 1024)


def pack_one(blocks, slot, half, out, index):
    out[index + (0,)] = blocks[slot, 2 * half, :, :128]
    out[index + (1,)] = blocks[slot, 2 * half + 1, :, :128]
    out[index + (2,)] = jnp.concatenate(
        [blocks[slot, 2 * half, :, 128:192], blocks[slot, 2 * half + 1, :, 128:192]], axis=1
    )


def pack_early_body(blocks, first, second):
    for slot in range(2):
        pack_one(blocks, slot, 0, first, (slot,))
        pack_one(blocks, slot, 1, second, (slot,))


def pack_late_body(blocks, out):
    for slot in range(2):
        for half in range(2):
            pack_one(blocks, slot, half, out, (0, slot, half))


def pack_early(blocks):
    spec = pl.BlockSpec((2, 3, 192, 128), lambda i: (i, 0, 0, 0))
    shape = jax.ShapeDtypeStruct((CHUNK, 3, 192, 128), jnp.bfloat16)
    return pl.pallas_call(
        pack_early_body,
        grid=(2,),
        in_specs=[pl.BlockSpec((2, 4, 192, 192), lambda i: (i, 0, 0, 0))],
        out_specs=[spec, spec],
        out_shape=[shape, shape],
        name="pack_early",
    )(blocks)


def pack_late(blocks):
    return pl.pallas_call(
        pack_late_body,
        grid=(2,),
        in_specs=[pl.BlockSpec((2, 4, 192, 192), lambda i: (i + 2, 0, 0, 0))],
        out_specs=pl.BlockSpec((1, 2, 2, 3, 192, 128), lambda i: (i, 0, 0, 0, 0, 0)),
        out_shape=jax.ShapeDtypeStruct((2, 2, 2, 3, 192, 128), jnp.bfloat16),
        name="pack_late",
    )(blocks)


def select_body(where, left_sector, right_sector, left_energy, psi, table, rows, cols, energies, window, sems):
    group = pl.program_id(0)

    @pl.when(group == 0)
    def _():
        site = where[SITE]
        left_ids = left_sector[...]
        right_ids = right_sector[...]
        for within in range(4):
            sector = 4 * site + within
            table[MY_START + within] = jnp.sum((left_ids < sector).astype(jnp.int32))
            table[MY_SIZE + within] = jnp.sum((left_ids == sector).astype(jnp.int32))
        before = jnp.int32(0)
        for sector in range(16):
            size = jnp.sum((right_ids == sector).astype(jnp.int32))
            table[RIGHT_START + sector] = before
            table[RIGHT_SIZE + sector] = size
            before = before + size
        copies = []
        shifts = []
        for within in range(4):
            start = table[MY_START + within]
            base = pl.multiple_of(jnp.minimum((start // 16) * 16, psi.shape[0] - WIN_ROWS), 16)
            shifts.append(start - base)
            copies.append(
                pltpu.make_async_copy(psi.at[pl.ds(base, WIN_ROWS), :], window.at[within], sems.at[within])
            )
        for copy in copies:
            copy.start()
        row = lax.broadcasted_iota(jnp.int32, (192, WIN_ROWS), 0)
        col = lax.broadcasted_iota(jnp.int32, (192, WIN_ROWS), 1)
        wide_row = lax.broadcasted_iota(jnp.int32, (192, WIN_COLS), 0)
        wide_col = lax.broadcasted_iota(jnp.int32, (192, WIN_COLS), 1)
        for within in range(4):
            start = table[MY_START + within]
            size = table[MY_SIZE + within]
            base = pl.multiple_of(jnp.minimum((start // 128) * 128, psi.shape[0] - WIN_COLS), 128)
            kept = (wide_col == wide_row + (start - base)) & (wide_row < size)
            near = jnp.where(kept, left_energy[:, pl.ds(base, WIN_COLS)], 0.0)
            energies[pl.ds(within * 192, 192), :] = jnp.sum(near, axis=1, keepdims=True)
        for within in range(4):
            copies[within].wait()
            kept = (col == row + shifts[within]) & (row < table[MY_SIZE + within])
            pick = jnp.where(kept, 1.0, 0.0).astype(jnp.bfloat16)
            got = jnp.dot(pick, window[within], preferred_element_type=jnp.float32)
            rows[pl.ds(within * 192, 192), :] = got.astype(jnp.bfloat16)

    row = lax.broadcasted_iota(jnp.int32, (WIN_COLS, SLOT_COLS), 0)
    lane = lax.broadcasted_iota(jnp.int32, (WIN_COLS, SLOT_COLS), 1)
    for q in range(4):
        start = table[RIGHT_START + 4 * group + q]
        size = table[RIGHT_SIZE + 4 * group + q]
        base = pl.multiple_of(jnp.minimum((start // 128) * 128, rows.shape[1] - WIN_COLS), 128)
        if q % 2:
            at = jnp.where(lane < 128, lane, jnp.where(lane < 192, size, lane - 64))
        else:
            at = lane
        kept = (row == at + (start - base)) & (at < size)
        pick = jnp.where(kept, 1.0, 0.0).astype(jnp.bfloat16)
        got = jnp.dot(rows[:, pl.ds(base, WIN_COLS)], pick, preferred_element_type=jnp.float32)
        cols[0, :, q * SLOT_COLS : (q + 1) * SLOT_COLS] = got.astype(jnp.bfloat16)


def select(where, left_sector, right_sector, left_energy, psi):
    bond = psi.shape[1]
    smem = pl.BlockSpec(memory_space=pltpu.SMEM)
    ids = pl.BlockSpec((bond // 128, 128), lambda g: (0, 0))
    return pl.pallas_call(
        select_body,
        grid=(4,),
        in_specs=[smem, ids, ids, pl.BlockSpec((1, bond), lambda g: (0, 0)), pl.BlockSpec(memory_space=pltpu.HBM)],
        out_specs=[
            smem,
            pl.BlockSpec((768, bond), lambda g: (0, 0)),
            pl.BlockSpec((1, 768, GROUP_COLS), lambda g: (g, 0, 0)),
            pl.BlockSpec((768, 1), lambda g: (0, 0)),
        ],
        out_shape=[
            jax.ShapeDtypeStruct((40,), jnp.int32),
            jax.ShapeDtypeStruct((768, bond), jnp.bfloat16),
            jax.ShapeDtypeStruct((4, 768, GROUP_COLS), jnp.bfloat16),
            jax.ShapeDtypeStruct((768, 1), jnp.float32),
        ],
        scratch_shapes=[pltpu.VMEM((4, WIN_ROWS, bond), jnp.bfloat16), pltpu.SemaphoreType.DMA((4,))],
        compiler_params=params(),
        name="select",
    )(
        where,
        left_sector.reshape(bond // 128, 128),
        right_sector.reshape(bond // 128, 128),
        left_energy[None, :],
        psi,
    )


def act(copies, what):
    for live, copy in copies:
        if live is None:
            getattr(copy, what)()
        else:

            @pl.when(live > 0)
            def _():
                getattr(copy, what)()


class Products:
    def __init__(self, rels, pairs, refs):
        self.rels, self.pairs = rels, pairs
        self.early, self.late = 0 in pairs, 2 in pairs
        self.first = 0 if self.early else 2
        self.where, self.live, left, left_late, psi = refs[:5]
        refs = list(refs[5:])
        self.rights = []
        for _ in rels:
            one = {}
            if self.early:
                one["a"], one["b"] = refs.pop(0), refs.pop(0)
            if self.late:
                one["e"], one["f"] = refs.pop(0), refs.pop(0)
            self.rights.append(one)
        self.left, self.left_late, self.psi = left, left_late, psi

    def taken(rels, pairs):
        return 5 + len(rels) * 2 * ((0 in pairs) + (2 in pairs))

    def scratch(rels, pairs):
        slots = 2 * len(pairs)
        groups = len(rels)
        return [
            pltpu.VMEM((slots, 4, 192, 192), jnp.bfloat16),
            pltpu.VMEM((groups, 2, slots, 3, 192, 128), jnp.bfloat16),
            pltpu.VMEM((groups, 768, GROUP_COLS), jnp.bfloat16),
            pltpu.VMEM((2, 768, GROUP_COLS), jnp.bfloat16),
            pltpu.SemaphoreType.DMA((3,)),
            pltpu.SemaphoreType.DMA((groups, 6)),
            pltpu.SemaphoreType.DMA((groups,)),
        ]

    def prepare(self, scratch):
        self.left_v, self.right_v, self.psi_v, self.image, sem_left, sem_right, sem_psi = scratch
        live_e = self.live[2] if self.late else None
        live_f = self.live[3] if self.late else None
        late_at = 4 - 2 * self.first
        self.copies_left = []
        if self.early:
            self.copies_left.append(
                (
                    None,
                    pltpu.make_async_copy(
                        self.left.at[pl.ds(0, 4)], self.left_v.at[pl.ds(0, 4)], sem_left.at[0]
                    ),
                )
            )
        if self.late:
            for live, source, at, sem in (
                (live_e, self.left_late, late_at, 1),
                (live_f, self.left.at[pl.ds(6, 2)], late_at + 2, 2),
            ):
                self.copies_left.append(
                    (live, pltpu.make_async_copy(source, self.left_v.at[pl.ds(at, 2)], sem_left.at[sem]))
                )
        self.copies = []
        for i, right in enumerate(self.rights):
            found = []
            if self.early:
                for half, name in enumerate("ab"):
                    found.append(
                        (
                            None,
                            pltpu.make_async_copy(
                                right[name], self.right_v.at[i, half, pl.ds(0, 4)], sem_right.at[i, half]
                            ),
                        )
                    )
            if self.late:
                for name, live, place, at in (("e", live_e, 2, late_at), ("f", live_f, 4, late_at + 2)):
                    for half in range(2):
                        found.append(
                            (
                                live,
                                pltpu.make_async_copy(
                                    right[name].at[:, half],
                                    self.right_v.at[i, half, pl.ds(at, 2)],
                                    sem_right.at[i, place + half],
                                ),
                            )
                        )
            site = (self.where[SITE] + self.rels[i]) % 4
            found.append((None, pltpu.make_async_copy(self.psi.at[site], self.psi_v.at[i], sem_psi.at[i])))
            self.copies.append(found)

    def multiply(self, i, acc):
        left_v, right_v, psi_v, image = self.left_v, self.right_v, self.psi_v, self.image

        def one_pair(p, inner):
            live = self.live[self.first + p]

            @pl.when(live > 0)
            def _():
                for u in range(2):
                    for within in range(4):
                        got = jnp.dot(
                            left_v[2 * p + u, within],
                            psi_v[i, within * 192 : (within + 1) * 192, :],
                            preferred_element_type=jnp.float32,
                        )
                        if u == 1:
                            got = jnp.where(live > 1, got, 0.0)
                        image[u, within * 192 : (within + 1) * 192, :] = got.astype(jnp.bfloat16)
                for q in range(4):
                    parts = []
                    for u in range(2):
                        block = jnp.concatenate(
                            [right_v[i, q // 2, 2 * p + u, q % 2], right_v[i, q // 2, 2 * p + u, 2]], axis=1
                        )
                        block = jnp.concatenate([block, jnp.zeros((64, 256), jnp.bfloat16)], axis=0)
                        parts.append(
                            lax.dot_general(
                                image[u, :, q * SLOT_COLS : (q + 1) * SLOT_COLS],
                                block,
                                (((1,), (1,)), ((), ())),
                                preferred_element_type=jnp.float32,
                            )
                        )
                    acc[:, q * SLOT_COLS : (q + 1) * SLOT_COLS] += parts[0] + parts[1]

            return inner

        lax.fori_loop(0, len(self.pairs), one_pair, 0)


def products_body(rels, pairs, *refs):
    groups = len(rels)
    taken = Products.taken(rels, pairs)
    work = Products(rels, pairs, refs[:taken])
    out, *rest = refs[taken:]
    acc_v, sem_out = rest[-2:]
    work.prepare(rest[:-2])
    act(work.copies_left, "start")
    for found in work.copies:
        act(found, "start")
    act(work.copies_left, "wait")
    out_copies = [pltpu.make_async_copy(acc_v.at[i], out.at[i], sem_out.at[i]) for i in range(groups)]

    def one_group(i, carry):
        for j in range(groups):

            @pl.when(i == j)
            def _():
                act(work.copies[j], "wait")

        acc_v[i] = jnp.zeros(acc_v.shape[1:], jnp.float32)
        work.multiply(i, acc_v.at[i])
        for j in range(groups):

            @pl.when(i == j)
            def _():
                out_copies[j].start()

        return carry

    lax.fori_loop(0, groups, one_group, 0)
    for copy in out_copies:
        copy.wait()


def operands(where, live, left, left_late, psi, rights):
    args = [where, live, left, left_late, psi] + [one for several in rights for one in several]
    smem = pl.BlockSpec(memory_space=pltpu.SMEM)
    hbm = pl.BlockSpec(memory_space=pltpu.HBM)
    return args, [smem, smem] + [hbm] * (len(args) - 2)


def products(rels, pairs, where, live, left, left_late, psi, rights):
    groups = len(rels)
    args, specs = operands(where, live, left, left_late, psi, rights)
    flops = groups * 2 * 1024 * 768 * (192 + 256) * 4
    return pl.pallas_call(
        functools.partial(products_body, tuple(rels), tuple(pairs)),
        in_specs=specs,
        out_specs=pl.BlockSpec(memory_space=pltpu.HBM),
        out_shape=jax.ShapeDtypeStruct((groups, 768, GROUP_COLS), jnp.float32),
        scratch_shapes=Products.scratch(rels, pairs)
        + [pltpu.VMEM((groups, 768, GROUP_COLS), jnp.float32), pltpu.SemaphoreType.DMA((groups,))],
        compiler_params=params(),
        cost_estimate=pl.CostEstimate(flops=flops, bytes_accessed=8 * 2**20, transcendentals=0),
        name="products",
    )(*args)


def finish_body(rels, pairs, *refs):
    taken = Products.taken(rels, pairs) if pairs else 1
    where = refs[0]
    work = Products(rels, pairs, refs[:taken]) if pairs else None
    table, own, others, rows, subspace, energies, right_energy, send, mine, proj = refs[taken : taken + 10]
    rest = refs[taken + 10 :]
    acc_v, rows_v, sub_v, total, staged, sem_acc, sem_in, sem_out = rest[-8:]
    width = rows.shape[1]
    acc_copies = [
        pltpu.make_async_copy(own.at[0] if i == 0 else others.at[i - 1], acc_v.at[i], sem_acc.at[i])
        for i in range(4)
    ]
    more_copies = [
        pltpu.make_async_copy(rows, rows_v, sem_in.at[0]),
        pltpu.make_async_copy(subspace, sub_v, sem_in.at[1]),
    ]
    if work is not None:
        work.prepare(rest[:-8])
        act(work.copies_left, "start")
        for i in range(3):
            act(work.copies[i], "start")
            acc_copies[i + 1].start()
        acc_copies[0].start()
        for copy in more_copies:
            copy.start()
        act(work.copies_left, "wait")

        def one_group(i, carry):
            for j in range(3):

                @pl.when(i == j)
                def _():
                    act(work.copies[j], "wait")
                    acc_copies[j + 1].wait()

            work.multiply(i, acc_v.at[i + 1])
            return carry

        lax.fori_loop(0, 3, one_group, 0)
        acc_copies[0].wait()
    else:
        for copy in acc_copies:
            copy.start()
        for copy in more_copies:
            copy.start()
        for copy in acc_copies:
            copy.wait()
    for copy in more_copies:
        copy.wait()

    core = where[CORE]
    site = where[SITE]
    diagonal_on = where[FIRST_OPS].astype(jnp.float32)
    lane = lax.broadcasted_iota(jnp.int32, (192, 128), 1)
    row = lax.broadcasted_iota(jnp.int32, (192, width), 0)
    proj[...] = jnp.zeros(proj.shape, jnp.float32)

    def out_copy(step):
        out = send if step < 2 else mine
        return pltpu.make_async_copy(staged.at[step], out.at[pl.ds(192 * (step % 2), 192)], sem_out.at[step])

    def one_block(step, carry):
        within = 2 * jnp.where(step < 2, 1 - core, core) + step % 2
        at = pl.multiple_of(192 * within, 192)
        mine_rows = pl.ds(at, 192)
        total[:, :width] = (
            (energies[mine_rows, :] + right_energy[...]) * rows_v[mine_rows, :].astype(jnp.float32) * diagonal_on
        )
        total[:, width:] = jnp.zeros((192, total.shape[1] - width), jnp.float32)
        for rel in range(4):
            for q in range(4):
                sector = ((site + rel) % 4) * 4 + q
                start = table[RIGHT_START + sector]
                size = table[RIGHT_SIZE + sector]
                base = pl.multiple_of((start // 128) * 128, 128)
                shift = start - base
                first = jnp.where(lane < size, acc_v[rel, mine_rows, q * SLOT_COLS : q * SLOT_COLS + 128], 0.0)
                second = jnp.where(
                    lane < size - 128, acc_v[rel, mine_rows, q * SLOT_COLS + 128 : (q + 1) * SLOT_COLS], 0.0
                )
                first = pltpu.roll(first, shift, 1)
                second = pltpu.roll(second, shift, 1)
                low = lane < shift
                total[:, pl.ds(base, 128)] += jnp.where(low, 0.0, first)
                total[:, pl.ds(base + 128, 128)] += jnp.where(low, first, second)
                total[:, pl.ds(base + 256, 128)] += jnp.where(low, second, 0.0)
        kept = jnp.where(row < table[MY_SIZE + within], total[:, :width], 0.0)
        for k in range(2):
            part = sub_v[k, within].astype(jnp.float32) * kept
            proj[k] += jnp.sum(part.reshape(24, 8, width), axis=0)
        staged[step] = kept.astype(jnp.bfloat16)
        for j in range(4):

            @pl.when(step == j)
            def _():
                out_copy(j).start()

        return carry

    lax.fori_loop(0, 4, one_block, 0)
    for j in range(4):
        out_copy(j).wait()


def finish(rels, pairs, first_args, first_specs, table, own, others, rows, subspace, energies, right_energy):
    width = rows.shape[1]
    smem = pl.BlockSpec(memory_space=pltpu.SMEM)
    hbm = pl.BlockSpec(memory_space=pltpu.HBM)
    vmem = pl.BlockSpec(memory_space=pltpu.VMEM)
    half = jax.ShapeDtypeStruct((384, width), jnp.bfloat16)
    flops = len(pairs) * 3 * 2 * 2 * 1024 * 768 * (192 + 256) + 10**9
    return pl.pallas_call(
        functools.partial(finish_body, tuple(rels), tuple(pairs)),
        in_specs=first_specs + [smem, hbm, hbm, hbm, hbm, vmem, vmem],
        out_specs=[hbm, hbm, vmem],
        out_shape=[half, half, jax.ShapeDtypeStruct((2, 8, width), jnp.float32)],
        scratch_shapes=(Products.scratch(rels, pairs) if pairs else [])
        + [
            pltpu.VMEM((4, 768, GROUP_COLS), jnp.float32),
            pltpu.VMEM((768, width), jnp.bfloat16),
            pltpu.VMEM((2, 4, 192, width), jnp.bfloat16),
            pltpu.VMEM((192, width + 256), jnp.float32),
            pltpu.VMEM((4, 192, width), jnp.bfloat16),
            pltpu.SemaphoreType.DMA((4,)),
            pltpu.SemaphoreType.DMA((2,)),
            pltpu.SemaphoreType.DMA((4,)),
        ],
        compiler_params=params(),
        cost_estimate=pl.CostEstimate(flops=flops, bytes_accessed=30 * 2**20, transcendentals=0),
        name="finish",
    )(*first_args, table, own, others, rows, subspace, energies, right_energy)


def place_body(which, where, half, *rest):
    out, sem = rest[-2:]
    core = where[CORE] if which == 0 else 1 - where[CORE]
    copy = pltpu.make_async_copy(half, out.at[pl.ds(2 * core, 2)], sem)
    copy.start()
    copy.wait()


def place(which, where, half, whole=None):
    hbm = pl.BlockSpec(memory_space=pltpu.HBM)
    args = (where, half) if whole is None else (where, half, whole)
    return pl.pallas_call(
        functools.partial(place_body, which),
        in_specs=[pl.BlockSpec(memory_space=pltpu.SMEM)] + [hbm] * (len(args) - 1),
        out_specs=hbm,
        out_shape=jax.ShapeDtypeStruct((4,) + half.shape[1:], half.dtype),
        scratch_shapes=[pltpu.SemaphoreType.DMA(())],
        input_output_aliases={} if whole is None else {2: 0},
        name="place",
    )(*args)


def shifted(value, axis, by):
    size = lax.axis_size(axis)
    return lax.ppermute(value, axis, [(i, (i + by) % size) for i in range(size)])


def small_sum(value, axis):
    size = lax.axis_size(axis)
    me = lax.axis_index(axis)
    got = jnp.stack([value] + [shifted(value, axis, k) for k in range(1, size)])
    order = (me - jnp.arange(size)) % size
    return jnp.take(got, order, axis=0).sum(axis=0)


def local(
    wavefunction,
    left_blocks,
    right_blocks,
    left_sector,
    right_sector,
    term_count,
    left_energy,
    right_energy,
    subspace,
):
    bond = wavefunction.shape[0]
    site = lax.axis_index("site")
    core = lax.axis_index("core")
    first_a, second_a = pack_early(right_blocks)
    prev_first = shifted(first_a, "site", 1)
    next_second = shifted(second_a, "site", -1)
    prev_second = shifted(second_a, "site", 1)
    next_first = shifted(first_a, "site", -1)
    left_later, right_later, _ = lax.optimization_barrier((left_blocks, right_blocks, first_a))

    active = term_count[0]
    beside = shifted(term_count, "core", 1)[0]
    heavy = active > CHUNK
    heavy_beside = beside > CHUNK
    where = jnp.stack([site, core, (lax.axis_index(OPS) == 0).astype(jnp.int32)])
    live = jnp.stack(
        [
            jnp.minimum(active, 2),
            jnp.clip(active - 2, 0, 2),
            jnp.where(heavy, jnp.clip(active - 4, 0, 2), jnp.clip(beside - 6, 0, 2)),
            jnp.where(heavy & heavy_beside, jnp.clip(active - 6, 0, 2), 0),
        ]
    )
    table, rows, psi, energies = select(where, left_sector, right_sector, left_energy, wavefunction)
    late = pack_late(right_later)
    right_e = jnp.where(heavy, late[0], shifted(late[1], "core", 1))
    right_f = late[1]
    left_e = jnp.where(heavy, left_later[4:6], shifted(left_later[6:8], "core", 1))

    own = products(
        (0,), (0, 1, 2, 3), where, live, left_blocks, left_e, psi, [(first_a, second_a, right_e, right_f)]
    )
    rels = (1, 2, 3)
    last = (table, own)
    more_last = (rows, subspace, energies, right_energy[None, :])
    smem = pl.BlockSpec(memory_space=pltpu.SMEM)

    def early_groups(prev_first, prev_second, next_first, next_second):
        far_first = shifted(prev_first, "site", 1)
        far_second = shifted(next_second, "site", -1)
        rights = [(next_first, next_second), (far_first, far_second), (prev_first, prev_second)]
        return products(rels, (0, 1), where, live, left_blocks, left_e, psi, rights)

    def no_more(*moved):
        return tuple(finish(rels, (), [where], [smem], *last, early_groups(*moved), *more_last))

    def more(*moved):
        moved_e = [shifted(right_e, "site", by) for by in (-1, 2, 1)]
        others = early_groups(*moved)
        moved_f = lax.cond(
            heavy & heavy_beside,
            lambda right: [shifted(right, "site", by) for by in (-1, 2, 1)],
            lambda right: [right, right, right],
            right_f,
        )
        rights = list(zip(moved_e, moved_f, strict=True))
        args, specs = operands(where, live, left_blocks, left_e, psi, rights)
        return tuple(finish(rels, (2, 3), args, specs, *last, others, *more_last))

    send, mine, proj = lax.cond(
        heavy | heavy_beside, more, no_more, prev_first, prev_second, next_first, next_second
    )
    proj = jnp.sum(proj, axis=(1, 2))
    swap = [(0, 1), (1, 0)]
    away = lax.ppermute(send, "core", swap)
    proj = proj + lax.ppermute(jnp.broadcast_to(proj[None, :], (8, 2)), "core", swap)[0]
    both = (mine.astype(jnp.float32) + away.astype(jnp.float32)).astype(jnp.bfloat16)

    high = lax.reduce_precision(proj, 8, 7)
    middle = lax.reduce_precision(proj - high, 8, 7)
    thirds = jnp.concatenate([high, middle, proj - high - middle]).astype(jnp.bfloat16)
    plane = lax.axis_size(("z", "y"))
    half = both.shape[0]
    share = half // plane
    extra = jnp.broadcast_to(jnp.pad(thirds, (0, EXTRA - 6))[None, :], (half, EXTRA))
    both = jnp.concatenate([both, extra], axis=1)

    pieces = lax.all_to_all(both.reshape(plane, share, bond + EXTRA), ("z", "y"), 0, 0, tiled=True)
    added = jnp.sum(pieces.astype(jnp.float32), axis=0)
    summed = added[:, :bond].astype(jnp.bfloat16)
    gathered = lax.all_to_all(
        jnp.broadcast_to(summed[None], (plane, share, bond)), ("z", "y"), 0, 0, tiled=True
    ).reshape(half, bond)
    whole = added[:8, bond : bond + 2] + added[:8, bond + 2 : bond + 4] + added[:8, bond + 4 : bond + 6]
    projections = small_sum(whole, "site")
    gathered = gathered.reshape(2, 192, bond)
    other = lax.ppermute(gathered, "core", swap)
    sigma = place(1, where, other, place(0, where, gathered))
    return sigma, projections[0]


def solution(mesh):
    shape = dict(mesh.shape)
    ops = shape["ops"]
    parts = Mesh(mesh.devices.reshape(4, ops // 8, 2, shape["site"]), ("z", "y", "core", "site"))
    in_specs = (
        P(),
        P(OPS, "site", None, None),
        P(OPS, "site", None, None),
        P(),
        P(),
        P(OPS),
        P(),
        P(),
        P(None, "site", None, None),
    )
    out_specs = (P("site", None, None), P())
    return jax.shard_map(local, mesh=parts, in_specs=in_specs, out_specs=out_specs, check_vma=False)
```

```python
import functools

import jax
import jax.numpy as jnp
from jax import lax
from jax.experimental import pallas as pl
from jax.experimental.pallas import tpu as pltpu
from jax.sharding import Mesh
from jax.sharding import PartitionSpec as P


OPS = ("z", "y", "core")
CHUNK = 4
WIN_ROWS = 256
WIN_COLS = 384
SLOT_COLS = 256
GROUP_COLS = 4 * SLOT_COLS
EXTRA = 128

MY_START, MY_SIZE, RIGHT_START, RIGHT_SIZE = 0, 4, 8, 24
SITE, CORE, FIRST_OPS = 0, 1, 2


def params():
    return pltpu.CompilerParams(vmem_limit_bytes=56 * 1024 * 1024)


def pack_one(blocks, slot, half, out, index, at=0):
    out[index + (at,)] = blocks[slot, 2 * half, :, :128]
    out[index + (at + 1,)] = blocks[slot, 2 * half + 1, :, :128]
    out[index + (at + 2,)] = jnp.concatenate(
        [blocks[slot, 2 * half, :, 128:192], blocks[slot, 2 * half + 1, :, 128:192]], axis=1
    )


def pack_early_body(blocks, first, second):
    for slot in range(2):
        pack_one(blocks, slot, 0, first, (slot,))
        pack_one(blocks, slot, 1, second, (slot,))


def pack_late_body(count, left, right, *outs):
    for k in range(4):

        @pl.when(pl.program_id(0) == k)
        def _():
            for half in range(2):
                pack_one(left, 0, half, outs[k], (), 3 * half)
                pack_one(right, 0, half, outs[k], (), 6 + 3 * half)
            outs[k][12] = jnp.full((192, 128), count[0].astype(jnp.float32)).astype(jnp.bfloat16)


def pack_early(blocks):
    spec = pl.BlockSpec((2, 3, 192, 128), lambda i: (i, 0, 0, 0))
    shape = jax.ShapeDtypeStruct((CHUNK, 3, 192, 128), jnp.bfloat16)
    return pl.pallas_call(
        pack_early_body,
        grid=(2,),
        in_specs=[pl.BlockSpec((2, 4, 192, 192), lambda i: (i, 0, 0, 0))],
        out_specs=[spec, spec],
        out_shape=[shape, shape],
        name="pack_early",
    )(blocks)


def pack_late(count, left, right):
    block = pl.BlockSpec((1, 4, 192, 192), lambda i: (i + CHUNK, 0, 0, 0))
    return pl.pallas_call(
        pack_late_body,
        grid=(4,),
        in_specs=[pl.BlockSpec(memory_space=pltpu.SMEM), block, block],
        out_specs=[pl.BlockSpec((13, 192, 128), lambda i: (0, 0, 0))] * 4,
        out_shape=[jax.ShapeDtypeStruct((13, 192, 128), jnp.bfloat16)] * 4,
        name="pack_late",
    )(count, left, right)


def select_body(where, left_sector, right_sector, left_energy, psi, table, rows, cols, energies, window, sems):
    group = pl.program_id(0)

    @pl.when(group == 0)
    def _():
        site = where[SITE]
        left_ids = left_sector[...]
        right_ids = right_sector[...]
        for within in range(4):
            sector = 4 * site + within
            table[MY_START + within] = jnp.sum((left_ids < sector).astype(jnp.int32))
            table[MY_SIZE + within] = jnp.sum((left_ids == sector).astype(jnp.int32))
        before = jnp.int32(0)
        for sector in range(16):
            size = jnp.sum((right_ids == sector).astype(jnp.int32))
            table[RIGHT_START + sector] = before
            table[RIGHT_SIZE + sector] = size
            before = before + size
        copies = []
        shifts = []
        for within in range(4):
            start = table[MY_START + within]
            base = pl.multiple_of(jnp.minimum((start // 16) * 16, psi.shape[0] - WIN_ROWS), 16)
            shifts.append(start - base)
            copies.append(
                pltpu.make_async_copy(psi.at[pl.ds(base, WIN_ROWS), :], window.at[within], sems.at[within])
            )
        for copy in copies:
            copy.start()
        row = lax.broadcasted_iota(jnp.int32, (192, WIN_ROWS), 0)
        col = lax.broadcasted_iota(jnp.int32, (192, WIN_ROWS), 1)
        wide_row = lax.broadcasted_iota(jnp.int32, (192, WIN_COLS), 0)
        wide_col = lax.broadcasted_iota(jnp.int32, (192, WIN_COLS), 1)
        for within in range(4):
            start = table[MY_START + within]
            size = table[MY_SIZE + within]
            base = pl.multiple_of(jnp.minimum((start // 128) * 128, psi.shape[0] - WIN_COLS), 128)
            kept = (wide_col == wide_row + (start - base)) & (wide_row < size)
            near = jnp.where(kept, left_energy[:, pl.ds(base, WIN_COLS)], 0.0)
            energies[pl.ds(within * 192, 192), :] = jnp.sum(near, axis=1, keepdims=True)
        for within in range(4):
            copies[within].wait()
            kept = (col == row + shifts[within]) & (row < table[MY_SIZE + within])
            pick = jnp.where(kept, 1.0, 0.0).astype(jnp.bfloat16)
            got = jnp.dot(pick, window[within], preferred_element_type=jnp.float32)
            rows[pl.ds(within * 192, 192), :] = got.astype(jnp.bfloat16)

    row = lax.broadcasted_iota(jnp.int32, (WIN_COLS, SLOT_COLS), 0)
    lane = lax.broadcasted_iota(jnp.int32, (WIN_COLS, SLOT_COLS), 1)
    for q in range(4):
        start = table[RIGHT_START + 4 * group + q]
        size = table[RIGHT_SIZE + 4 * group + q]
        base = pl.multiple_of(jnp.minimum((start // 128) * 128, rows.shape[1] - WIN_COLS), 128)
        if q % 2:
            at = jnp.where(lane < 128, lane, jnp.where(lane < 192, size, lane - 64))
        else:
            at = lane
        kept = (row == at + (start - base)) & (at < size)
        pick = jnp.where(kept, 1.0, 0.0).astype(jnp.bfloat16)
        got = jnp.dot(rows[:, pl.ds(base, WIN_COLS)], pick, preferred_element_type=jnp.float32)
        cols[0, :, q * SLOT_COLS : (q + 1) * SLOT_COLS] = got.astype(jnp.bfloat16)


def select(where, left_sector, right_sector, left_energy, psi):
    bond = psi.shape[1]
    smem = pl.BlockSpec(memory_space=pltpu.SMEM)
    ids = pl.BlockSpec((bond // 128, 128), lambda g: (0, 0))
    return pl.pallas_call(
        select_body,
        grid=(4,),
        in_specs=[smem, ids, ids, pl.BlockSpec((1, bond), lambda g: (0, 0)), pl.BlockSpec(memory_space=pltpu.HBM)],
        out_specs=[
            smem,
            pl.BlockSpec((768, bond), lambda g: (0, 0)),
            pl.BlockSpec((1, 768, GROUP_COLS), lambda g: (g, 0, 0)),
            pl.BlockSpec((768, 1), lambda g: (0, 0)),
        ],
        out_shape=[
            jax.ShapeDtypeStruct((40,), jnp.int32),
            jax.ShapeDtypeStruct((768, bond), jnp.bfloat16),
            jax.ShapeDtypeStruct((4, 768, GROUP_COLS), jnp.bfloat16),
            jax.ShapeDtypeStruct((768, 1), jnp.float32),
        ],
        scratch_shapes=[pltpu.VMEM((4, WIN_ROWS, bond), jnp.bfloat16), pltpu.SemaphoreType.DMA((4,))],
        compiler_params=params(),
        name="select",
    )(
        where,
        left_sector.reshape(bond // 128, 128),
        right_sector.reshape(bond // 128, 128),
        left_energy[None, :],
        psi,
    )


def multiply_slots(lefts, rights, psi, image, acc, last_live):
    count = len(lefts)
    for u in range(count):
        for within in range(4):
            got = jnp.dot(
                lefts[u](within), psi[within * 192 : (within + 1) * 192, :], preferred_element_type=jnp.float32
            )
            if u == 1:
                got = jnp.where(last_live, got, 0.0)
            image[u, within * 192 : (within + 1) * 192, :] = got.astype(jnp.bfloat16)
    for q in range(4):
        parts = None
        for u in range(count):
            block = jnp.concatenate([rights[u](q), jnp.zeros((64, 256), jnp.bfloat16)], axis=0)
            part = lax.dot_general(
                image[u, :, q * SLOT_COLS : (q + 1) * SLOT_COLS],
                block,
                (((1,), (1,)), ((), ())),
                preferred_element_type=jnp.float32,
            )
            parts = part if parts is None else parts + part
        acc[:, q * SLOT_COLS : (q + 1) * SLOT_COLS] += parts


def products_body(rels, where, live, left, psi, *refs):
    groups = len(rels)
    rights = [refs[2 * i : 2 * i + 2] for i in range(groups)]
    out, left_v, right_v, psi_v, image, acc_v, sem_left, sem_right, sem_psi, sem_out = refs[2 * groups :]
    site = where[SITE]
    left_copies = [
        pltpu.make_async_copy(left.at[pl.ds(2 * p, 2)], left_v.at[pl.ds(2 * p, 2)], sem_left.at[p])
        for p in range(2)
    ]
    copies = []
    for i in range(groups):
        copies.append(
            [
                pltpu.make_async_copy(rights[i][half], right_v.at[i, half], sem_right.at[i, half])
                for half in range(2)
            ]
            + [pltpu.make_async_copy(psi.at[(site + rels[i]) % 4], psi_v.at[i], sem_psi.at[i])]
        )
    out_copies = [pltpu.make_async_copy(acc_v.at[i], out.at[i], sem_out.at[i]) for i in range(groups)]
    for copy in left_copies:
        copy.start()
    for found in copies:
        for copy in found:
            copy.start()
    for copy in left_copies:
        copy.wait()

    def one_group(i, carry):
        for j in range(groups):

            @pl.when(i == j)
            def _():
                for copy in copies[j]:
                    copy.wait()

        acc_v[i] = jnp.zeros(acc_v.shape[1:], jnp.float32)

        def one_pair(p, inner):
            lefts = [lambda within, u=u: left_v[2 * p + u, within] for u in range(2)]
            block = [
                lambda q, u=u: jnp.concatenate(
                    [right_v[i, q // 2, 2 * p + u, q % 2], right_v[i, q // 2, 2 * p + u, 2]], axis=1
                )
                for u in range(2)
            ]
            multiply_slots(lefts, block, psi_v.at[i], image, acc_v.at[i], 2 * p + 1 < live[0])
            return inner

        lax.fori_loop(0, (live[0] + 1) // 2, one_pair, 0)
        for j in range(groups):

            @pl.when(i == j)
            def _():
                out_copies[j].start()

        return carry

    lax.fori_loop(0, groups, one_group, 0)
    for copy in out_copies:
        copy.wait()


def products(rels, where, live, left, psi, rights):
    groups = len(rels)
    smem = pl.BlockSpec(memory_space=pltpu.SMEM)
    hbm = pl.BlockSpec(memory_space=pltpu.HBM)
    flops = groups * 2 * 1024 * 768 * (192 + 256) * 4
    return pl.pallas_call(
        functools.partial(products_body, tuple(rels)),
        in_specs=[smem, smem, hbm, hbm] + [hbm] * (2 * groups),
        out_specs=hbm,
        out_shape=jax.ShapeDtypeStruct((groups, 768, GROUP_COLS), jnp.float32),
        scratch_shapes=[
            pltpu.VMEM((CHUNK, 4, 192, 192), jnp.bfloat16),
            pltpu.VMEM((groups, 2, CHUNK, 3, 192, 128), jnp.bfloat16),
            pltpu.VMEM((groups, 768, GROUP_COLS), jnp.bfloat16),
            pltpu.VMEM((2, 768, GROUP_COLS), jnp.bfloat16),
            pltpu.VMEM((groups, 768, GROUP_COLS), jnp.float32),
            pltpu.SemaphoreType.DMA((2,)),
            pltpu.SemaphoreType.DMA((groups, 2)),
            pltpu.SemaphoreType.DMA((groups,)),
            pltpu.SemaphoreType.DMA((groups,)),
        ],
        compiler_params=params(),
        cost_estimate=pl.CostEstimate(flops=flops, bytes_accessed=8 * 2**20, transcendentals=0),
        name="products",
    )(where, live, left, psi, *[one for several in rights for one in several])


def finish_body(slots, where, live, table, own, others, rows, subspace, energies, right_energy, *refs):
    refs = list(refs)
    if slots:
        psi, extra = refs[:2]
        moved = refs[2:5]
        refs = refs[5:]
    send, mine, proj, acc_v, rows_v, sub_v, total, staged, sem_acc, sem_in, sem_out = refs[:11]
    width = rows.shape[1]
    core = where[CORE]
    site = where[SITE]
    acc_copies = [
        pltpu.make_async_copy(own.at[0] if i == 0 else others.at[i - 1], acc_v.at[i], sem_acc.at[i])
        for i in range(4)
    ]

    def block_copies(step):
        within = 2 * ((1 - core) if step < 2 else core) + step % 2
        part = pl.ds(pl.multiple_of(192 * within, 192), 192)
        return [
            pltpu.make_async_copy(rows.at[part], rows_v.at[step], sem_in.at[step, 0]),
            pltpu.make_async_copy(subspace.at[0, within], sub_v.at[step, 0], sem_in.at[step, 1]),
            pltpu.make_async_copy(subspace.at[1, within], sub_v.at[step, 1], sem_in.at[step, 2]),
        ]

    if slots:
        extra_v, moved_v, psi_v, image, sem_extra, sem_psi = refs[11:]
        extra_copy = pltpu.make_async_copy(extra.at[:, pl.ds(0, 12)], extra_v, sem_extra.at[0])
        moved_copies = [
            pltpu.make_async_copy(moved[i], moved_v.at[i], sem_extra.at[1 + i]) for i in range(3)
        ]
        psi_copies = [
            pltpu.make_async_copy(psi.at[(site + i) % 4], psi_v.at[i], sem_psi.at[i]) for i in range(4)
        ]
        extra_copy.start()
        for i in range(4):
            psi_copies[i].start()
            acc_copies[i].start()
            if i:
                moved_copies[i - 1].start()
    else:
        for copy in acc_copies:
            copy.start()
    for step in range(4):
        for copy in block_copies(step):
            copy.start()

    if slots:
        extra_copy.wait()

        def one_group(i, carry):
            for j in range(4):

                @pl.when(i == j)
                def _():
                    psi_copies[j].wait()
                    acc_copies[j].wait()
                    if j:
                        moved_copies[j - 1].wait()
                    else:
                        moved_v[3] = extra_v[:, 6:12]

            place_of = (i + 3) % 4

            def one_slot(n, inner):
                @pl.when(live[1 + n] > 0)
                def _():
                    def left_block(within):
                        at = 3 * (within // 2)
                        lane = 64 * (within % 2)
                        high = extra_v[n, at + 2]
                        return jnp.concatenate(
                            [extra_v[n, at + within % 2], high[:, lane : lane + 64]], axis=1
                        )

                    def right_block(q):
                        at = 3 * (q // 2)
                        return jnp.concatenate(
                            [moved_v[place_of, n, at + q % 2], moved_v[place_of, n, at + 2]], axis=1
                        )

                    multiply_slots([left_block], [right_block], psi_v.at[i], image, acc_v.at[i], None)

                return inner

            lax.fori_loop(0, slots, one_slot, 0)
            return carry

        lax.fori_loop(0, 4, one_group, 0)
    else:
        for copy in acc_copies:
            copy.wait()

    diagonal_on = where[FIRST_OPS].astype(jnp.float32)
    lane = lax.broadcasted_iota(jnp.int32, (192, 128), 1)
    row = lax.broadcasted_iota(jnp.int32, (192, width), 0)
    proj[...] = jnp.zeros(proj.shape, jnp.float32)

    def out_copy(step):
        out = send if step < 2 else mine
        return pltpu.make_async_copy(staged.at[step], out.at[pl.ds(192 * (step % 2), 192)], sem_out.at[step])

    def one_block(step, carry):
        for j in range(4):

            @pl.when(step == j)
            def _():
                for copy in block_copies(j):
                    copy.wait()

        within = 2 * jnp.where(step < 2, 1 - core, core) + step % 2
        at = pl.multiple_of(192 * within, 192)
        mine_rows = pl.ds(at, 192)
        total[:, :width] = (
            (energies[mine_rows, :] + right_energy[...]) * rows_v[step].astype(jnp.float32) * diagonal_on
        )
        total[:, width:] = jnp.zeros((192, total.shape[1] - width), jnp.float32)
        for rel in range(4):
            for q in range(4):
                sector = ((site + rel) % 4) * 4 + q
                start = table[RIGHT_START + sector]
                size = table[RIGHT_SIZE + sector]
                base = pl.multiple_of((start // 128) * 128, 128)
                shift = start - base
                first = jnp.where(lane < size, acc_v[rel, mine_rows, q * SLOT_COLS : q * SLOT_COLS + 128], 0.0)
                second = jnp.where(
                    lane < size - 128, acc_v[rel, mine_rows, q * SLOT_COLS + 128 : (q + 1) * SLOT_COLS], 0.0
                )
                first = pltpu.roll(first, shift, 1)
                second = pltpu.roll(second, shift, 1)
                low = lane < shift
                total[:, pl.ds(base, 128)] += jnp.where(low, 0.0, first)
                total[:, pl.ds(base + 128, 128)] += jnp.where(low, first, second)
                total[:, pl.ds(base + 256, 128)] += jnp.where(low, second, 0.0)
        kept = jnp.where(row < table[MY_SIZE + within], total[:, :width], 0.0)
        for k in range(2):
            part = sub_v[step, k].astype(jnp.float32) * kept
            proj[k] += jnp.sum(part.reshape(24, 8, width), axis=0)
        staged[step] = kept.astype(jnp.bfloat16)
        for j in range(4):

            @pl.when(step == j)
            def _():
                out_copy(j).start()

        return carry

    lax.fori_loop(0, 4, one_block, 0)
    for j in range(4):
        out_copy(j).wait()


def finish(slots, where, live, table, own, others, rows, subspace, energies, right_energy, late=()):
    width = rows.shape[1]
    smem = pl.BlockSpec(memory_space=pltpu.SMEM)
    hbm = pl.BlockSpec(memory_space=pltpu.HBM)
    vmem = pl.BlockSpec(memory_space=pltpu.VMEM)
    half = jax.ShapeDtypeStruct((384, width), jnp.bfloat16)
    scratch = [
        pltpu.VMEM((4, 768, GROUP_COLS), jnp.float32),
        pltpu.VMEM((4, 192, width), jnp.bfloat16),
        pltpu.VMEM((4, 2, 192, width), jnp.bfloat16),
        pltpu.VMEM((192, width + 256), jnp.float32),
        pltpu.VMEM((4, 192, width), jnp.bfloat16),
        pltpu.SemaphoreType.DMA((4,)),
        pltpu.SemaphoreType.DMA((4, 3)),
        pltpu.SemaphoreType.DMA((4,)),
    ]
    if slots:
        scratch += [
            pltpu.VMEM((slots, 12, 192, 128), jnp.bfloat16),
            pltpu.VMEM((4, slots, 6, 192, 128), jnp.bfloat16),
            pltpu.VMEM((4, 768, GROUP_COLS), jnp.bfloat16),
            pltpu.VMEM((1, 768, GROUP_COLS), jnp.bfloat16),
            pltpu.SemaphoreType.DMA((4,)),
            pltpu.SemaphoreType.DMA((4,)),
        ]
    return pl.pallas_call(
        functools.partial(finish_body, slots),
        in_specs=[smem, smem, smem, hbm, hbm, hbm, hbm, vmem, vmem] + [hbm] * len(late),
        out_specs=[hbm, hbm, vmem],
        out_shape=[half, half, jax.ShapeDtypeStruct((2, 8, width), jnp.float32)],
        scratch_shapes=scratch,
        compiler_params=params(),
        cost_estimate=pl.CostEstimate(flops=8 * 10**9, bytes_accessed=30 * 2**20, transcendentals=0),
        name="finish",
    )(where, live, table, own, others, rows, subspace, energies, right_energy, *late)


def place_body(where, half, *rest):
    rest[-1][...] = half[...]


def place(which, where, half, whole=None):
    def at(i, where):
        core = where[CORE] if which == 0 else 1 - where[CORE]
        return (2 * core + i, 0, 0)

    args = (where, half) if whole is None else (where, half, whole)
    block = (1,) + half.shape[1:]
    return pl.pallas_call(
        place_body,
        grid_spec=pltpu.PrefetchScalarGridSpec(
            num_scalar_prefetch=1,
            grid=(2,),
            in_specs=[pl.BlockSpec(block, lambda i, w: (i, 0, 0))]
            + ([] if whole is None else [pl.BlockSpec(memory_space=pltpu.HBM)]),
            out_specs=pl.BlockSpec(block, at),
        ),
        out_shape=jax.ShapeDtypeStruct((4,) + half.shape[1:], half.dtype),
        input_output_aliases={} if whole is None else {2: 0},
        name="place",
    )(*args)


def shifted(value, axis, by):
    size = lax.axis_size(axis)
    return lax.ppermute(value, axis, [(i, (i + by) % size) for i in range(size)])


def small_sum(value, axis):
    size = lax.axis_size(axis)
    me = lax.axis_index(axis)
    got = jnp.stack([value] + [shifted(value, axis, k) for k in range(1, size)])
    order = (me - jnp.arange(size)) % size
    return jnp.take(got, order, axis=0).sum(axis=0)


def local(
    wavefunction,
    left_blocks,
    right_blocks,
    left_sector,
    right_sector,
    term_count,
    left_energy,
    right_energy,
    subspace,
):
    bond = wavefunction.shape[0]
    site = lax.axis_index("site")
    core = lax.axis_index("core")
    first_a, second_a = pack_early(right_blocks)
    prev_first = shifted(first_a, "site", 1)
    next_second = shifted(second_a, "site", -1)
    prev_second = shifted(second_a, "site", 1)
    next_first = shifted(first_a, "site", -1)
    left_later, right_later, _ = lax.optimization_barrier((left_blocks, right_blocks, first_a))

    where = jnp.stack([site, core, (lax.axis_index(OPS) == 0).astype(jnp.int32)])
    table, rows, psi, energies = select(where, left_sector, right_sector, left_energy, wavefunction)

    late = pack_late(term_count, left_later, right_later)
    extras = [
        shifted(late[k], axis, by) for k, (axis, by) in enumerate((("y", 1), ("y", -1), ("z", 1), ("z", -1)))
    ]
    counts = jnp.stack([one[12, 0, 0] for one in extras]).astype(jnp.int32)
    there = counts > CHUNK + jnp.arange(4, dtype=jnp.int32)
    number = jnp.sum(there.astype(jnp.int32))
    live = jnp.concatenate([jnp.minimum(term_count, CHUNK), there.astype(jnp.int32)])
    live_one = jnp.concatenate([jnp.minimum(term_count, CHUNK), jnp.ones((1,), jnp.int32)])

    own = products((0,), where, live_one, left_blocks, psi, [(first_a, second_a)])
    others_of = (rows, subspace, energies, right_energy[None, :])

    def early_groups(prev_first, prev_second, next_first, next_second):
        far_first = shifted(prev_first, "site", 1)
        far_second = shifted(next_second, "site", -1)
        rights = [(next_first, next_second), (far_first, far_second), (prev_first, prev_second)]
        return products((1, 2, 3), where, live_one, left_blocks, psi, rights)

    def none(*moved):
        return tuple(finish(0, where, live_one, table, own, early_groups(*moved), *others_of))

    def with_extra(slots, extra, which, moved):
        going = extra[:, 6:12]
        arrived = [shifted(going, "site", by) for by in (-1, 2, 1)]
        others = early_groups(*moved)
        return tuple(finish(slots, where, which, table, own, others, *others_of, late=(psi, extra, *arrived)))

    def one(*moved):
        extra = extras[3]
        for k in (2, 1, 0):
            extra = jnp.where(there[k], extras[k], extra)
        return with_extra(1, extra[None], live_one, moved)

    def many(*moved):
        return with_extra(4, jnp.stack(extras), live, moved)

    send, mine, proj = lax.switch(
        jnp.minimum(number, 2), [none, one, many], prev_first, prev_second, next_first, next_second
    )
    proj = jnp.sum(proj, axis=(1, 2))
    swap = [(0, 1), (1, 0)]
    away = lax.ppermute(send, "core", swap)
    proj = proj + lax.ppermute(jnp.broadcast_to(proj[None, :], (8, 2)), "core", swap)[0]
    both = (mine.astype(jnp.float32) + away.astype(jnp.float32)).astype(jnp.bfloat16)

    high = lax.reduce_precision(proj, 8, 7)
    middle = lax.reduce_precision(proj - high, 8, 7)
    thirds = jnp.concatenate([high, middle, proj - high - middle]).astype(jnp.bfloat16)
    plane = lax.axis_size(("z", "y"))
    half = both.shape[0]
    share = half // plane
    extra = jnp.broadcast_to(jnp.pad(thirds, (0, EXTRA - 6))[None, :], (half, EXTRA))
    both = jnp.concatenate([both, extra], axis=1)

    pieces = lax.all_to_all(both.reshape(plane, share, bond + EXTRA), ("z", "y"), 0, 0, tiled=True)
    added = jnp.sum(pieces.astype(jnp.float32), axis=0)
    summed = added[:, :bond].astype(jnp.bfloat16)
    gathered = lax.all_to_all(
        jnp.broadcast_to(summed[None], (plane, share, bond)), ("z", "y"), 0, 0, tiled=True
    ).reshape(half, bond)
    whole = added[:8, bond : bond + 2] + added[:8, bond + 2 : bond + 4] + added[:8, bond + 4 : bond + 6]
    projections = small_sum(whole, "site")
    gathered = gathered.reshape(2, 192, bond)
    other = lax.ppermute(gathered, "core", swap)
    sigma = place(1, where, other, place(0, where, gathered))
    return sigma, projections[0]


def solution(mesh):
    shape = dict(mesh.shape)
    ops = shape["ops"]
    parts = Mesh(mesh.devices.reshape(4, ops // 8, 2, shape["site"]), ("z", "y", "core", "site"))
    in_specs = (
        P(),
        P(OPS, "site", None, None),
        P(OPS, "site", None, None),
        P(),
        P(),
        P(OPS),
        P(),
        P(),
        P(None, "site", None, None),
    )
    out_specs = (P("site", None, None), P())
    return jax.shard_map(local, mesh=parts, in_specs=in_specs, out_specs=out_specs, check_vma=False)
```

```python
import functools

import jax
import jax.numpy as jnp
from jax import lax
from jax.experimental import pallas as pl
from jax.experimental.pallas import tpu as pltpu
from jax.sharding import Mesh
from jax.sharding import PartitionSpec as P


OPS = ("z", "y", "core")
CHUNK = 4
WIN_ROWS = 256
WIN_COLS = 384
SLOT_COLS = 256
GROUP_COLS = 4 * SLOT_COLS
EXTRA = 128

MY_START, MY_SIZE, RIGHT_START, RIGHT_SIZE = 0, 4, 8, 24
SITE, CORE, MEMBER = 0, 1, 2
DIAGONAL_ROWS = 32


def params():
    return pltpu.CompilerParams(vmem_limit_bytes=56 * 1024 * 1024)


def pack_one(blocks, slot, half, out, index, at=0):
    out[index + (at,)] = blocks[slot, 2 * half, :, :128]
    out[index + (at + 1,)] = blocks[slot, 2 * half + 1, :, :128]
    out[index + (at + 2,)] = jnp.concatenate(
        [blocks[slot, 2 * half, :, 128:192], blocks[slot, 2 * half + 1, :, 128:192]], axis=1
    )


def pack_early_body(blocks, first, second):
    for slot in range(2):
        pack_one(blocks, slot, 0, first, (slot,))
        pack_one(blocks, slot, 1, second, (slot,))


def pack_late_body(left, right, *outs):
    for k in range(4):

        @pl.when(pl.program_id(0) == k)
        def _():
            for half in range(2):
                pack_one(left, 0, half, outs[k], (), 3 * half)
                pack_one(right, 0, half, outs[k], (), 6 + 3 * half)


def pack_early(blocks):
    spec = pl.BlockSpec((2, 3, 192, 128), lambda i: (i, 0, 0, 0))
    shape = jax.ShapeDtypeStruct((CHUNK, 3, 192, 128), jnp.bfloat16)
    return pl.pallas_call(
        pack_early_body,
        grid=(2,),
        in_specs=[pl.BlockSpec((2, 4, 192, 192), lambda i: (i, 0, 0, 0))],
        out_specs=[spec, spec],
        out_shape=[shape, shape],
        name="pack_early",
    )(blocks)


def pack_late(left, right):
    block = pl.BlockSpec((1, 4, 192, 192), lambda i: (i + CHUNK, 0, 0, 0))
    return pl.pallas_call(
        pack_late_body,
        grid=(4,),
        in_specs=[block, block],
        out_specs=[pl.BlockSpec((12, 192, 128), lambda i: (0, 0, 0))] * 4,
        out_shape=[jax.ShapeDtypeStruct((12, 192, 128), jnp.bfloat16)] * 4,
        name="pack_late",
    )(left, right)


def select_body(where, left_sector, right_sector, left_energy, psi, table, rows, cols, energies, window, wide, sems):
    group = pl.program_id(0)

    @pl.when(group == 0)
    def _():
        site = where[SITE]
        left_ids = left_sector[...]
        right_ids = right_sector[...]
        for within in range(4):
            sector = 4 * site + within
            table[MY_START + within] = jnp.sum((left_ids < sector).astype(jnp.int32))
            table[MY_SIZE + within] = jnp.sum((left_ids == sector).astype(jnp.int32))
        before = jnp.int32(0)
        for sector in range(16):
            size = jnp.sum((right_ids == sector).astype(jnp.int32))
            table[RIGHT_START + sector] = before
            table[RIGHT_SIZE + sector] = size
            before = before + size
        copies = []
        shifts = []
        for within in range(4):
            start = table[MY_START + within]
            base = pl.multiple_of(jnp.minimum((start // 16) * 16, psi.shape[0] - WIN_ROWS), 16)
            shifts.append(start - base)
            copies.append(
                pltpu.make_async_copy(psi.at[pl.ds(base, WIN_ROWS), :], window.at[within], sems.at[within])
            )
        for copy in copies:
            copy.start()
        row = lax.broadcasted_iota(jnp.int32, (192, WIN_ROWS), 0)
        col = lax.broadcasted_iota(jnp.int32, (192, WIN_ROWS), 1)
        wide_row = lax.broadcasted_iota(jnp.int32, (192, WIN_COLS), 0)
        wide_col = lax.broadcasted_iota(jnp.int32, (192, WIN_COLS), 1)
        for within in range(4):
            start = table[MY_START + within]
            size = table[MY_SIZE + within]
            base = pl.multiple_of(jnp.minimum((start // 128) * 128, psi.shape[0] - WIN_COLS), 128)
            kept = (wide_col == wide_row + (start - base)) & (wide_row < size)
            near = jnp.where(kept, left_energy[:, pl.ds(base, WIN_COLS)], 0.0)
            energies[pl.ds(within * 192, 192), :] = jnp.sum(near, axis=1, keepdims=True)
        for within in range(4):
            copies[within].wait()
            kept = (col == row + shifts[within]) & (row < table[MY_SIZE + within])
            pick = jnp.where(kept, 1.0, 0.0).astype(jnp.bfloat16)
            got = jnp.dot(pick, window[within], preferred_element_type=jnp.float32)
            rows[pl.ds(within * 192, 192), :] = got.astype(jnp.bfloat16)
            wide[pl.ds(within * 192, 192), : rows.shape[1]] = got

    lane = lax.broadcasted_iota(jnp.int32, (96, 128), 1)

    def one_part(part, carry):
        here = pl.ds(pl.multiple_of(96 * part, 96), 96)
        for q in range(4):
            start = table[RIGHT_START + 4 * group + q]
            size = table[RIGHT_SIZE + 4 * group + q]
            base = pl.multiple_of((start // 128) * 128, 128)
            left_over = 128 - (start - base)
            turned = [pltpu.roll(wide[here, pl.ds(base + 128 * j, 128)], left_over % 128, 1) for j in range(3)]
            low = lane < left_over
            first = jnp.where(lane < size, jnp.where(low, turned[0], turned[1]), 0.0)
            second = jnp.where(lane < size - 128, jnp.where(low, turned[1], turned[2]), 0.0)
            if q % 2:
                second = pltpu.roll(second, 64, 1)
            cols[0, here, q * SLOT_COLS : q * SLOT_COLS + 128] = first.astype(jnp.bfloat16)
            cols[0, here, q * SLOT_COLS + 128 : (q + 1) * SLOT_COLS] = second.astype(jnp.bfloat16)
        return carry

    lax.fori_loop(0, 8, one_part, 0)


def select(where, left_sector, right_sector, left_energy, psi):
    bond = psi.shape[1]
    smem = pl.BlockSpec(memory_space=pltpu.SMEM)
    ids = pl.BlockSpec((bond // 128, 128), lambda g: (0, 0))
    return pl.pallas_call(
        select_body,
        grid=(4,),
        in_specs=[smem, ids, ids, pl.BlockSpec((1, bond), lambda g: (0, 0)), pl.BlockSpec(memory_space=pltpu.HBM)],
        out_specs=[
            smem,
            pl.BlockSpec((768, bond), lambda g: (0, 0)),
            pl.BlockSpec((1, 768, GROUP_COLS), lambda g: (g, 0, 0)),
            pl.BlockSpec((768, 1), lambda g: (0, 0)),
        ],
        out_shape=[
            jax.ShapeDtypeStruct((40,), jnp.int32),
            jax.ShapeDtypeStruct((768, bond), jnp.bfloat16),
            jax.ShapeDtypeStruct((4, 768, GROUP_COLS), jnp.bfloat16),
            jax.ShapeDtypeStruct((768, 1), jnp.float32),
        ],
        scratch_shapes=[
            pltpu.VMEM((4, WIN_ROWS, bond), jnp.bfloat16),
            pltpu.VMEM((768, bond + 256), jnp.float32),
            pltpu.SemaphoreType.DMA((4,)),
        ],
        compiler_params=params(),
        name="select",
    )(
        where,
        left_sector.reshape(bond // 128, 128),
        right_sector.reshape(bond // 128, 128),
        left_energy[None, :],
        psi,
    )


def multiply_slots(lefts, rights, psi, image, acc, last_live):
    count = len(lefts)
    for u in range(count):
        for within in range(4):
            got = jnp.dot(
                lefts[u](within), psi[within * 192 : (within + 1) * 192, :], preferred_element_type=jnp.float32
            )
            if u == 1:
                got = jnp.where(last_live, got, 0.0)
            image[u, within * 192 : (within + 1) * 192, :] = got.astype(jnp.bfloat16)
    for q in range(4):
        parts = None
        for u in range(count):
            block = jnp.concatenate([rights[u](q), jnp.zeros((64, 256), jnp.bfloat16)], axis=0)
            part = lax.dot_general(
                image[u, :, q * SLOT_COLS : (q + 1) * SLOT_COLS],
                block,
                (((1,), (1,)), ((), ())),
                preferred_element_type=jnp.float32,
            )
            parts = part if parts is None else parts + part
        acc[:, q * SLOT_COLS : (q + 1) * SLOT_COLS] += parts


def products_body(rels, where, live, left, psi, *refs):
    groups = len(rels)
    rights = [refs[2 * i : 2 * i + 2] for i in range(groups)]
    out, left_v, right_v, psi_v, image, acc_v, sem_left, sem_right, sem_psi, sem_out = refs[2 * groups :]
    site = where[SITE]
    left_copies = [
        pltpu.make_async_copy(left.at[pl.ds(2 * p, 2)], left_v.at[pl.ds(2 * p, 2)], sem_left.at[p])
        for p in range(2)
    ]
    copies = []
    for i in range(groups):
        copies.append(
            [
                pltpu.make_async_copy(rights[i][half], right_v.at[i, half], sem_right.at[i, half])
                for half in range(2)
            ]
            + [pltpu.make_async_copy(psi.at[(site + rels[i]) % 4], psi_v.at[i], sem_psi.at[i])]
        )
    out_copies = [
        [
            pltpu.make_async_copy(
                acc_v.at[i, pl.ds(192 * w, 192)], out.at[i, pl.ds(192 * w, 192)], sem_out.at[i, w]
            )
            for w in range(4)
        ]
        for i in range(groups)
    ]
    for copy in left_copies:
        copy.start()
    for found in copies:
        for copy in found:
            copy.start()
    for copy in left_copies:
        copy.wait()

    def one_group(i, carry):
        for j in range(groups):

            @pl.when(i == j)
            def _():
                for copy in copies[j]:
                    copy.wait()

        acc_v[i] = jnp.zeros(acc_v.shape[1:], jnp.float32)

        def one_pair(p, inner):
            lefts = [lambda within, u=u: left_v[2 * p + u, within] for u in range(2)]
            block = [
                lambda q, u=u: jnp.concatenate(
                    [right_v[i, q // 2, 2 * p + u, q % 2], right_v[i, q // 2, 2 * p + u, 2]], axis=1
                )
                for u in range(2)
            ]
            multiply_slots(lefts, block, psi_v.at[i], image, acc_v.at[i], 2 * p + 1 < live[0])
            return inner

        lax.fori_loop(0, (live[0] + 1) // 2, one_pair, 0)
        for j in range(groups):

            @pl.when(i == j)
            def _():
                for copy in out_copies[j]:
                    copy.start()

        return carry

    lax.fori_loop(0, groups, one_group, 0)
    for found in out_copies:
        for copy in found:
            copy.wait()


def products(rels, where, live, left, psi, rights):
    groups = len(rels)
    smem = pl.BlockSpec(memory_space=pltpu.SMEM)
    hbm = pl.BlockSpec(memory_space=pltpu.HBM)
    flops = groups * 2 * 1024 * 768 * (192 + 256) * 4
    return pl.pallas_call(
        functools.partial(products_body, tuple(rels)),
        in_specs=[smem, smem, hbm, hbm] + [hbm] * (2 * groups),
        out_specs=hbm,
        out_shape=jax.ShapeDtypeStruct((groups, 768, GROUP_COLS), jnp.float32),
        scratch_shapes=[
            pltpu.VMEM((CHUNK, 4, 192, 192), jnp.bfloat16),
            pltpu.VMEM((groups, 2, CHUNK, 3, 192, 128), jnp.bfloat16),
            pltpu.VMEM((groups, 768, GROUP_COLS), jnp.bfloat16),
            pltpu.VMEM((2, 768, GROUP_COLS), jnp.bfloat16),
            pltpu.VMEM((groups, 768, GROUP_COLS), jnp.float32),
            pltpu.SemaphoreType.DMA((2,)),
            pltpu.SemaphoreType.DMA((groups, 2)),
            pltpu.SemaphoreType.DMA((groups,)),
            pltpu.SemaphoreType.DMA((groups, 4)),
        ],
        compiler_params=params(),
        cost_estimate=pl.CostEstimate(flops=flops, bytes_accessed=8 * 2**20, transcendentals=0),
        name="products",
    )(where, live, left, psi, *[one for several in rights for one in several])


def finish_body(slots, where, live, table, own, near, far_a, far_b, left, psi, *refs):
    rows, subspace, energies, right_energy = refs[:4]
    refs = list(refs[4:])
    if slots:
        extras, moved = refs[:4], refs[4:7]
        refs = refs[7:]
    send, mine, proj, left_v, right_v, psi_v, image, acc_v, rows_v, sub_v, total, staged, sums = refs[:13]
    sem_left, sem_right, sem_psi, sem_acc, sem_rows, sem_sub, sem_out = refs[13:20]
    width = subspace.shape[3]
    core = where[CORE]
    site = where[SITE]
    member = where[MEMBER]

    left_copies = [
        pltpu.make_async_copy(left.at[pl.ds(2 * p, 2)], left_v.at[pl.ds(2 * p, 2)], sem_left.at[p])
        for p in range(2)
    ]
    far_copies = [
        pltpu.make_async_copy(far_a, right_v.at[0], sem_right.at[0]),
        pltpu.make_async_copy(far_b, right_v.at[1], sem_right.at[1]),
    ]
    psi_copies = {
        i: pltpu.make_async_copy(psi.at[(site + i) % 4], psi_v.at[i], sem_psi.at[i])
        for i in ((2, 0, 1, 3) if slots else (2,))
    }
    acc_copies = [
        pltpu.make_async_copy(source, acc_v.at[rel], sem_acc.at[rel])
        for rel, source in ((0, own.at[0]), (1, near.at[0]), (3, near.at[1]))
    ]
    their = jnp.minimum(member, 768 // DIAGONAL_ROWS - 1)
    rows_copy = pltpu.make_async_copy(
        rows.at[pl.ds(pl.multiple_of(DIAGONAL_ROWS * their, DIAGONAL_ROWS), DIAGONAL_ROWS)],
        rows_v,
        sem_rows,
    )

    def sub_copies(step):
        within = 2 * ((1 - core) if step < 2 else core) + step % 2
        return [
            pltpu.make_async_copy(subspace.at[k, within], sub_v.at[step, k], sem_sub.at[step, k]) for k in range(2)
        ]

    for copy in left_copies + far_copies:
        copy.start()
    psi_copies[2].start()
    if slots:
        extra_v, moved_v, sem_extra, sem_moved = refs[20:]
        extra_copies = []
        for k in range(4):
            if slots == 1:
                extra_copies.append((live[1] == k, pltpu.make_async_copy(extras[k], extra_v.at[0], sem_extra.at[0])))
            else:
                extra_copies.append((True, pltpu.make_async_copy(extras[k], extra_v.at[k], sem_extra.at[k])))
        moved_copies = [
            pltpu.make_async_copy(moved[i], moved_v.at[i + 1], sem_moved.at[i]) for i in range(3)
        ]
        for wanted, copy in extra_copies:

            @pl.when(wanted)
            def _():
                copy.start()

        for i in (0, 1, 3):
            psi_copies[i].start()
        for copy in moved_copies:
            copy.start()
    for copy in acc_copies:
        copy.start()
    rows_copy.start()
    for step in range(4):
        for copy in sub_copies(step):
            copy.start()

    acc_v[2] = jnp.zeros(acc_v.shape[1:], jnp.float32)
    for copy in left_copies + far_copies:
        copy.wait()
    psi_copies[2].wait()

    def one_pair(p, inner):
        lefts = [lambda within, u=u: left_v[2 * p + u, within] for u in range(2)]
        blocks = [
            lambda q, u=u: jnp.concatenate(
                [right_v[q // 2, 2 * p + u, q % 2], right_v[q // 2, 2 * p + u, 2]], axis=1
            )
            for u in range(2)
        ]
        multiply_slots(lefts, blocks, psi_v.at[2], image, acc_v.at[2], 2 * p + 1 < live[0])
        return inner

    lax.fori_loop(0, (live[0] + 1) // 2, one_pair, 0)
    for copy in acc_copies:
        copy.wait()
    if slots:
        for wanted, copy in extra_copies:

            @pl.when(wanted)
            def _():
                copy.wait()

        for i in (0, 1, 3):
            psi_copies[i].wait()
        for copy in moved_copies:
            copy.wait()
        moved_v[0] = extra_v[:, 6:12]

        def one_group(i, carry):
            def one_slot(n, inner):
                @pl.when((slots == 1) | (live[1 + n] > 0))
                def _():
                    def left_block(within):
                        at = 3 * (within // 2)
                        lane = 64 * (within % 2)
                        high = extra_v[n, at + 2]
                        return jnp.concatenate([extra_v[n, at + within % 2], high[:, lane : lane + 64]], axis=1)

                    def right_block(q):
                        at = 3 * (q // 2)
                        return jnp.concatenate([moved_v[i, n, at + q % 2], moved_v[i, n, at + 2]], axis=1)

                    multiply_slots([left_block], [right_block], psi_v.at[i], image, acc_v.at[i], None)

                return inner

            lax.fori_loop(0, slots, one_slot, 0)
            return carry

        lax.fori_loop(0, 4, one_group, 0)
    rows_copy.wait()

    lane = lax.broadcasted_iota(jnp.int32, (192, 128), 1)
    row = lax.broadcasted_iota(jnp.int32, (192, width), 0)
    sums[...] = jnp.zeros(sums.shape, jnp.float32)

    def out_copy(step):
        out = send if step < 2 else mine
        return pltpu.make_async_copy(staged.at[step], out.at[pl.ds(192 * (step % 2), 192)], sem_out.at[step])

    def one_block(step, carry):
        for j in range(4):

            @pl.when(step == j)
            def _():
                for copy in sub_copies(j):
                    copy.wait()

        within = 2 * jnp.where(step < 2, 1 - core, core) + step % 2
        here = pl.ds(pl.multiple_of(192 * within, 192), 192)

        def one_site(i, inner):
            rel = (i + 4 - site) % 4
            for q in range(4):
                start = table[RIGHT_START + 4 * i + q]
                base = pl.multiple_of((start // 128) * 128, 128)
                shift = start - base
                first = pltpu.roll(acc_v[rel, here, q * SLOT_COLS : q * SLOT_COLS + 128], shift, 1)
                second = pltpu.roll(acc_v[rel, here, q * SLOT_COLS + 128 : (q + 1) * SLOT_COLS], shift, 1)
                low = lane < shift
                total[:, pl.ds(base, 128)] = jnp.where(low, total[:, pl.ds(base, 128)], first)
                total[:, pl.ds(base + 128, 128)] = jnp.where(low, first, second)
                total[:, pl.ds(base + 256, 128)] = second
            return inner

        lax.fori_loop(0, 4, one_site, 0)
        per = 192 // DIAGONAL_ROWS

        @pl.when(member // per == within)
        def _():
            at = pl.multiple_of(DIAGONAL_ROWS * (member % per), DIAGONAL_ROWS)
            part = pl.ds(at, DIAGONAL_ROWS)
            energy = energies[pl.ds(pl.multiple_of(192 * within + at, DIAGONAL_ROWS), DIAGONAL_ROWS), :]
            total[part, :width] += (energy + right_energy[...]) * rows_v[...].astype(jnp.float32)

        kept = jnp.where(row < table[MY_SIZE + within], total[:, :width], 0.0)
        for k in range(2):
            part = sub_v[step, k].astype(jnp.float32) * kept
            sums[k] += jnp.sum(part.reshape(24, 8, width), axis=0)
        staged[step] = kept.astype(jnp.bfloat16)
        for j in range(4):

            @pl.when(step == j)
            def _():
                out_copy(j).start()

        return carry

    lax.fori_loop(0, 4, one_block, 0)
    for k in range(2):
        added = sums[k, :, :128]
        for j in range(1, width // 128):
            added = added + sums[k, :, 128 * j : 128 * (j + 1)]
        proj[k] = added
    for j in range(4):
        out_copy(j).wait()


def finish(slots, where, live, table, own, near, far, left, psi, rows, subspace, energies, right_energy, late=()):
    width = rows.shape[1]
    smem = pl.BlockSpec(memory_space=pltpu.SMEM)
    hbm = pl.BlockSpec(memory_space=pltpu.HBM)
    vmem = pl.BlockSpec(memory_space=pltpu.VMEM)
    half = jax.ShapeDtypeStruct((384, width), jnp.bfloat16)
    scratch = [
        pltpu.VMEM((CHUNK, 4, 192, 192), jnp.bfloat16),
        pltpu.VMEM((2, CHUNK, 3, 192, 128), jnp.bfloat16),
        pltpu.VMEM((4, 768, GROUP_COLS), jnp.bfloat16),
        pltpu.VMEM((2, 768, GROUP_COLS), jnp.bfloat16),
        pltpu.VMEM((4, 768, GROUP_COLS), jnp.float32),
        pltpu.VMEM((DIAGONAL_ROWS, width), jnp.bfloat16),
        pltpu.VMEM((4, 2, 192, width), jnp.bfloat16),
        pltpu.VMEM((192, width + 256), jnp.float32),
        pltpu.VMEM((4, 192, width), jnp.bfloat16),
        pltpu.VMEM((2, 8, width), jnp.float32),
        pltpu.SemaphoreType.DMA((2,)),
        pltpu.SemaphoreType.DMA((2,)),
        pltpu.SemaphoreType.DMA((4,)),
        pltpu.SemaphoreType.DMA((4,)),
        pltpu.SemaphoreType.DMA(()),
        pltpu.SemaphoreType.DMA((4, 2)),
        pltpu.SemaphoreType.DMA((4,)),
    ]
    if slots:
        scratch += [
            pltpu.VMEM((slots, 12, 192, 128), jnp.bfloat16),
            pltpu.VMEM((4, slots, 6, 192, 128), jnp.bfloat16),
            pltpu.SemaphoreType.DMA((4,)),
            pltpu.SemaphoreType.DMA((3,)),
        ]
    return pl.pallas_call(
        functools.partial(finish_body, slots),
        in_specs=[smem] * 3 + [hbm] * 8 + [vmem, vmem] + [hbm] * len(late),
        out_specs=[hbm, hbm, vmem],
        out_shape=[half, half, jax.ShapeDtypeStruct((2, 8, 128), jnp.float32)],
        scratch_shapes=scratch,
        compiler_params=params(),
        cost_estimate=pl.CostEstimate(flops=8 * 10**9, bytes_accessed=30 * 2**20, transcendentals=0),
        name="finish",
    )(where, live, table, own, near, *far, left, psi, rows, subspace, energies, right_energy, *late)


def place_body(where, half, *rest):
    rest[-1][...] = half[...]


def place(which, where, half, whole=None):
    def at(i, j, where):
        core = where[CORE] if which == 0 else 1 - where[CORE]
        return (2 * core + i, j, 0)

    args = (where, half) if whole is None else (where, half, whole)
    block = (1, 96) + half.shape[2:]
    return pl.pallas_call(
        place_body,
        grid_spec=pltpu.PrefetchScalarGridSpec(
            num_scalar_prefetch=1,
            grid=(2, 2),
            in_specs=[pl.BlockSpec(block, lambda i, j, w: (i, j, 0))]
            + ([] if whole is None else [pl.BlockSpec(memory_space=pltpu.HBM)]),
            out_specs=pl.BlockSpec(block, at),
        ),
        out_shape=jax.ShapeDtypeStruct((4,) + half.shape[1:], half.dtype),
        input_output_aliases={} if whole is None else {2: 0},
        name="place",
    )(*args)


def shifted(value, axis, by):
    size = lax.axis_size(axis)
    return lax.ppermute(value, axis, [(i, (i + by) % size) for i in range(size)])


def small_sum(value, axis):
    size = lax.axis_size(axis)
    me = lax.axis_index(axis)
    got = [value] + [shifted(value, axis, k) for k in range(1, size)]
    total = None
    for source in range(size):
        one = sum(jnp.where((me - source) % size == k, got[k], 0.0) for k in range(size))
        total = one if total is None else total + one
    return total


def local(
    wavefunction,
    left_blocks,
    right_blocks,
    left_sector,
    right_sector,
    term_count,
    left_energy,
    right_energy,
    subspace,
):
    bond = wavefunction.shape[0]
    site = lax.axis_index("site")
    core = lax.axis_index("core")
    first_a, second_a = pack_early(right_blocks)
    prev_first = shifted(first_a, "site", 1)
    next_second = shifted(second_a, "site", -1)
    prev_second = shifted(second_a, "site", 1)
    next_first = shifted(first_a, "site", -1)
    left_later, right_later, _ = lax.optimization_barrier((left_blocks, right_blocks, first_a))

    ways = (("y", 1), ("y", -1), ("z", 1), ("z", -1))
    counts = jnp.concatenate([shifted(term_count, axis, by) for axis, by in ways])
    late = pack_late(left_later, right_later)
    extras = [shifted(late[k], axis, by) for k, (axis, by) in enumerate(ways)]
    places = jnp.arange(4, dtype=jnp.int32)
    there = counts > CHUNK + places
    number = jnp.sum(there.astype(jnp.int32))
    mine_live = jnp.minimum(term_count, CHUNK)
    first_there = jnp.min(jnp.where(there, places, 3))
    live_one = jnp.concatenate([mine_live, first_there[None]])
    live_many = jnp.concatenate([mine_live, there.astype(jnp.int32)])

    where = jnp.stack([site, core, lax.axis_index(OPS)])
    table, rows, psi, energies = select(where, left_sector, right_sector, left_energy, wavefunction)
    own = products((0,), where, live_one, left_blocks, psi, [(first_a, second_a)])

    def rest(slots, live, moved, late):
        prev_first, prev_second, next_first, next_second = moved
        far = (shifted(prev_first, "site", 1), shifted(next_second, "site", -1))
        arrived = []
        if slots:
            extras, going = late
            arrived = [*extras] + [shifted(going, "site", by) for by in (-1, 2, 1)]
        near = products((1, 3), where, live, left_blocks, psi, [(next_first, next_second), (prev_first, prev_second)])
        return tuple(
            finish(
                slots,
                where,
                live,
                table,
                own,
                near,
                far,
                left_blocks,
                psi,
                rows,
                subspace,
                energies,
                right_energy[None, :],
                late=arrived,
            )
        )

    def none(*moved):
        return rest(0, live_one, moved, None)

    def one(*moved):
        going = extras[3][6:12]
        for k in (2, 1, 0):
            going = jnp.where(first_there == k, extras[k][6:12], going)
        return rest(1, live_one, moved, (extras, going[None]))

    def many(*moved):
        return rest(4, live_many, moved, (extras, jnp.stack([one[6:12] for one in extras])))

    send, mine, proj = lax.switch(
        jnp.minimum(number, 2), [none, one, many], prev_first, prev_second, next_first, next_second
    )
    swap = [(0, 1), (1, 0)]
    away = lax.ppermute(send, "core", swap)
    proj = small_sum(jnp.broadcast_to(jnp.sum(proj, axis=(1, 2))[None, :], (8, 2)), "site")[0]
    both = (mine.astype(jnp.float32) + away.astype(jnp.float32)).astype(jnp.bfloat16)

    high = lax.reduce_precision(proj, 8, 7)
    middle = lax.reduce_precision(proj - high, 8, 7)
    thirds = jnp.concatenate([high, middle, proj - high - middle]).astype(jnp.bfloat16)
    plane = lax.axis_size(("z", "y"))
    half = both.shape[0]
    share = half // plane
    extra = jnp.broadcast_to(jnp.pad(thirds, (0, EXTRA - 6))[None, :], (half, EXTRA))
    both = jnp.concatenate([both, extra], axis=1)

    pieces = lax.all_to_all(both.reshape(plane, share, bond + EXTRA), ("z", "y"), 0, 0, tiled=True)
    added = jnp.sum(pieces.astype(jnp.float32), axis=0)
    summed = added[:, :bond].astype(jnp.bfloat16)
    gathered = lax.all_to_all(
        jnp.broadcast_to(summed[None], (plane, share, bond)), ("z", "y"), 0, 0, tiled=True
    ).reshape(half, bond)
    whole = added[:8, bond : bond + 2] + added[:8, bond + 2 : bond + 4] + added[:8, bond + 4 : bond + 6]
    gathered = gathered.reshape(2, 192, bond)
    other = lax.ppermute(gathered, "core", swap)
    projections = whole + lax.ppermute(whole, "core", swap)
    sigma = place(1, where, other, place(0, where, gathered))
    return sigma, projections[0]


def solution(mesh):
    shape = dict(mesh.shape)
    ops = shape["ops"]
    parts = Mesh(mesh.devices.reshape(4, ops // 8, 2, shape["site"]), ("z", "y", "core", "site"))
    in_specs = (
        P(),
        P(OPS, "site", None, None),
        P(OPS, "site", None, None),
        P(),
        P(),
        P(OPS),
        P(),
        P(),
        P(None, "site", None, None),
    )
    out_specs = (P("site", None, None), P())
    return jax.shard_map(local, mesh=parts, in_specs=in_specs, out_specs=out_specs, check_vma=False)
```

```python
import functools

import jax
import jax.numpy as jnp
from jax import lax
from jax.experimental import pallas as pl
from jax.experimental.pallas import tpu as pltpu
from jax.sharding import Mesh
from jax.sharding import PartitionSpec as P


OPS = ("z", "y", "core")
CHUNK = 4
WIN_ROWS = 256
WIN_COLS = 384
SLOT_COLS = 256
GROUP_COLS = 4 * SLOT_COLS
EXTRA = 128

MY_START, MY_SIZE, RIGHT_START, RIGHT_SIZE = 0, 4, 8, 24
SITE, CORE, MEMBER = 0, 1, 2
DIAGONAL_ROWS = 32


def params():
    return pltpu.CompilerParams(vmem_limit_bytes=56 * 1024 * 1024)


def pack_one(blocks, slot, half, out, index, at=0):
    out[index + (at,)] = blocks[slot, 2 * half, :, :128]
    out[index + (at + 1,)] = blocks[slot, 2 * half + 1, :, :128]
    out[index + (at + 2,)] = jnp.concatenate(
        [blocks[slot, 2 * half, :, 128:192], blocks[slot, 2 * half + 1, :, 128:192]], axis=1
    )


def pack_early_body(blocks, out):
    for slot in range(2):
        for half in range(2):
            pack_one(blocks, slot, half, out, (half, slot))


def pack_late_body(left, right, *outs):
    for k in range(4):

        @pl.when(pl.program_id(0) == k)
        def _():
            for half in range(2):
                pack_one(left, 0, half, outs[k], (), 3 * half)
                pack_one(right, 0, half, outs[k], (), 6 + 3 * half)


def pack_early(blocks):
    return pl.pallas_call(
        pack_early_body,
        grid=(2,),
        in_specs=[pl.BlockSpec((2, 4, 192, 192), lambda i: (i, 0, 0, 0))],
        out_specs=pl.BlockSpec((2, 2, 3, 192, 128), lambda i: (0, i, 0, 0, 0)),
        out_shape=jax.ShapeDtypeStruct((2, CHUNK, 3, 192, 128), jnp.bfloat16),
        name="pack_early",
    )(blocks)


def pack_late(left, right):
    block = pl.BlockSpec((1, 4, 192, 192), lambda i: (i + CHUNK, 0, 0, 0))
    return pl.pallas_call(
        pack_late_body,
        grid=(4,),
        in_specs=[block, block],
        out_specs=[pl.BlockSpec((12, 192, 128), lambda i: (0, 0, 0))] * 4,
        out_shape=[jax.ShapeDtypeStruct((12, 192, 128), jnp.bfloat16)] * 4,
        cost_estimate=pl.CostEstimate(flops=2 * 10**9, bytes_accessed=2**22, transcendentals=0),
        name="pack_late",
    )(left, right)


def select_body(where, left_sector, right_sector, left_energy, psi, table, rows, cols, energies, window, sems):
    group = pl.program_id(0)

    @pl.when(group == 0)
    def _():
        site = where[SITE]
        left_ids = left_sector[...]
        right_ids = right_sector[...]
        for within in range(4):
            sector = 4 * site + within
            table[MY_START + within] = jnp.sum((left_ids < sector).astype(jnp.int32))
            table[MY_SIZE + within] = jnp.sum((left_ids == sector).astype(jnp.int32))
        before = jnp.int32(0)
        for sector in range(16):
            size = jnp.sum((right_ids == sector).astype(jnp.int32))
            table[RIGHT_START + sector] = before
            table[RIGHT_SIZE + sector] = size
            before = before + size
        copies = []
        shifts = []
        for within in range(4):
            start = table[MY_START + within]
            base = pl.multiple_of(jnp.minimum((start // 16) * 16, psi.shape[0] - WIN_ROWS), 16)
            shifts.append(start - base)
            copies.append(
                pltpu.make_async_copy(psi.at[pl.ds(base, WIN_ROWS), :], window.at[within], sems.at[within])
            )
        for copy in copies:
            copy.start()
        row = lax.broadcasted_iota(jnp.int32, (192, WIN_ROWS), 0)
        col = lax.broadcasted_iota(jnp.int32, (192, WIN_ROWS), 1)
        wide_row = lax.broadcasted_iota(jnp.int32, (192, WIN_COLS), 0)
        wide_col = lax.broadcasted_iota(jnp.int32, (192, WIN_COLS), 1)
        for within in range(4):
            start = table[MY_START + within]
            size = table[MY_SIZE + within]
            base = pl.multiple_of(jnp.minimum((start // 128) * 128, psi.shape[0] - WIN_COLS), 128)
            kept = (wide_col == wide_row + (start - base)) & (wide_row < size)
            near = jnp.where(kept, left_energy[:, pl.ds(base, WIN_COLS)], 0.0)
            energies[pl.ds(within * 192, 192), :] = jnp.sum(near, axis=1, keepdims=True)
        for within in range(4):
            copies[within].wait()
            kept = (col == row + shifts[within]) & (row < table[MY_SIZE + within])
            pick = jnp.where(kept, 1.0, 0.0).astype(jnp.bfloat16)
            got = jnp.dot(pick, window[within], preferred_element_type=jnp.float32)
            rows[pl.ds(within * 192, 192), :] = got.astype(jnp.bfloat16)

    row = lax.broadcasted_iota(jnp.int32, (WIN_COLS, SLOT_COLS), 0)
    lane = lax.broadcasted_iota(jnp.int32, (WIN_COLS, SLOT_COLS), 1)
    for q in range(4):
        start = table[RIGHT_START + 4 * group + q]
        size = table[RIGHT_SIZE + 4 * group + q]
        base = pl.multiple_of(jnp.minimum((start // 128) * 128, rows.shape[1] - WIN_COLS), 128)
        if q % 2:
            at = jnp.where(lane < 128, lane, jnp.where(lane < 192, size, lane - 64))
        else:
            at = lane
        kept = (row == at + (start - base)) & (at < size)
        pick = jnp.where(kept, 1.0, 0.0).astype(jnp.bfloat16)
        got = jnp.dot(rows[:, pl.ds(base, WIN_COLS)], pick, preferred_element_type=jnp.float32)
        cols[0, :, q * SLOT_COLS : (q + 1) * SLOT_COLS] = got.astype(jnp.bfloat16)


def select(where, left_sector, right_sector, left_energy, psi):
    bond = psi.shape[1]
    smem = pl.BlockSpec(memory_space=pltpu.SMEM)
    ids = pl.BlockSpec((bond // 128, 128), lambda g: (0, 0))
    return pl.pallas_call(
        select_body,
        grid=(4,),
        in_specs=[smem, ids, ids, pl.BlockSpec((1, bond), lambda g: (0, 0)), pl.BlockSpec(memory_space=pltpu.HBM)],
        out_specs=[
            smem,
            pl.BlockSpec((768, bond), lambda g: (0, 0)),
            pl.BlockSpec((1, 768, GROUP_COLS), lambda g: (g, 0, 0)),
            pl.BlockSpec((768, 1), lambda g: (0, 0)),
        ],
        out_shape=[
            jax.ShapeDtypeStruct((40,), jnp.int32),
            jax.ShapeDtypeStruct((768, bond), jnp.bfloat16),
            jax.ShapeDtypeStruct((4, 768, GROUP_COLS), jnp.bfloat16),
            jax.ShapeDtypeStruct((768, 1), jnp.float32),
        ],
        scratch_shapes=[
            pltpu.VMEM((4, WIN_ROWS, bond), jnp.bfloat16),
            pltpu.SemaphoreType.DMA((4,)),
        ],
        compiler_params=params(),
        cost_estimate=pl.CostEstimate(flops=5 * 10**9, bytes_accessed=2**24, transcendentals=0),
        name="select",
    )(
        where,
        left_sector.reshape(bond // 128, 128),
        right_sector.reshape(bond // 128, 128),
        left_energy[None, :],
        psi,
    )


def multiply_slots(lefts, rights, psi, image, acc, last_live):
    count = len(lefts)
    for u in range(count):
        for within in range(4):
            got = jnp.dot(
                lefts[u](within), psi[within * 192 : (within + 1) * 192, :], preferred_element_type=jnp.float32
            )
            if u == 1:
                got = jnp.where(last_live, got, 0.0)
            image[u, within * 192 : (within + 1) * 192, :] = got.astype(jnp.bfloat16)
    for q in range(4):
        parts = None
        for u in range(count):
            block = jnp.concatenate([rights[u](q), jnp.zeros((64, 256), jnp.bfloat16)], axis=0)
            part = lax.dot_general(
                image[u, :, q * SLOT_COLS : (q + 1) * SLOT_COLS],
                block,
                (((1,), (1,)), ((), ())),
                preferred_element_type=jnp.float32,
            )
            parts = part if parts is None else parts + part
        acc[:, q * SLOT_COLS : (q + 1) * SLOT_COLS] += parts


def products_body(rels, where, count, left, psi, *refs):
    groups = len(rels)
    live = jnp.minimum(count[0], CHUNK)
    rights = refs[:groups]
    out, left_v, right_v, psi_v, image, acc_v, sem_left, sem_right, sem_psi, sem_out = refs[groups:]
    site = where[SITE]
    left_copies = [
        pltpu.make_async_copy(left.at[pl.ds(2 * p, 2)], left_v.at[pl.ds(2 * p, 2)], sem_left.at[p])
        for p in range(2)
    ]
    copies = []
    for i in range(groups):
        copies.append(
            [
                pltpu.make_async_copy(rights[i], right_v.at[i], sem_right.at[i]),
                pltpu.make_async_copy(psi.at[(site + rels[i]) % 4], psi_v.at[i], sem_psi.at[i]),
            ]
        )
    out_copies = [
        [
            pltpu.make_async_copy(
                acc_v.at[i, pl.ds(192 * w, 192)], out.at[i, pl.ds(192 * w, 192)], sem_out.at[i, w]
            )
            for w in range(4)
        ]
        for i in range(groups)
    ]
    for copy in left_copies + copies[0]:
        copy.start()
    acc_v[0] = jnp.zeros(acc_v.shape[1:], jnp.float32)
    for copy in left_copies:
        copy.wait()

    def one_group(i, carry):
        for j in range(groups):

            @pl.when(i == j)
            def _():
                for copy in copies[j]:
                    copy.wait()
                if j + 1 < groups:
                    for copy in copies[j + 1]:
                        copy.start()
                    acc_v[j + 1] = jnp.zeros(acc_v.shape[1:], jnp.float32)

        def one_pair(p, inner):
            lefts = [lambda within, u=u: left_v[2 * p + u, within] for u in range(2)]
            block = [
                lambda q, u=u: jnp.concatenate(
                    [right_v[i, q // 2, 2 * p + u, q % 2], right_v[i, q // 2, 2 * p + u, 2]], axis=1
                )
                for u in range(2)
            ]
            multiply_slots(lefts, block, psi_v.at[i], image, acc_v.at[i], 2 * p + 1 < live)
            return inner

        lax.fori_loop(0, (live + 1) // 2, one_pair, 0)
        for j in range(groups):

            @pl.when(i == j)
            def _():
                for copy in out_copies[j]:
                    copy.start()

        return carry

    lax.fori_loop(0, groups, one_group, 0)
    for found in out_copies:
        for copy in found:
            copy.wait()


def products(rels, where, count, left, psi, rights):
    groups = len(rels)
    smem = pl.BlockSpec(memory_space=pltpu.SMEM)
    hbm = pl.BlockSpec(memory_space=pltpu.HBM)
    flops = groups * 2 * 1024 * 768 * (192 + 256) * 4
    return pl.pallas_call(
        functools.partial(products_body, tuple(rels)),
        in_specs=[smem, smem, hbm, hbm] + [hbm] * groups,
        out_specs=hbm,
        out_shape=jax.ShapeDtypeStruct((groups, 768, GROUP_COLS), jnp.float32),
        scratch_shapes=[
            pltpu.VMEM((CHUNK, 4, 192, 192), jnp.bfloat16),
            pltpu.VMEM((groups, 2, CHUNK, 3, 192, 128), jnp.bfloat16),
            pltpu.VMEM((groups, 768, GROUP_COLS), jnp.bfloat16),
            pltpu.VMEM((2, 768, GROUP_COLS), jnp.bfloat16),
            pltpu.VMEM((groups, 768, GROUP_COLS), jnp.float32),
            pltpu.SemaphoreType.DMA((2,)),
            pltpu.SemaphoreType.DMA((groups,)),
            pltpu.SemaphoreType.DMA((groups,)),
            pltpu.SemaphoreType.DMA((groups, 4)),
        ],
        compiler_params=params(),
        cost_estimate=pl.CostEstimate(flops=flops, bytes_accessed=8 * 2**20, transcendentals=0),
        name="products",
    )(where, count, left, psi, *rights)


def finish_body(slots, where, count, table, own, near, far_a, far_b, left, psi, *refs):
    live = jnp.minimum(count[0], CHUNK)
    rows, subspace, energies, right_energy = refs[:4]
    refs = list(refs[4:])
    if slots:
        counts, extras, moved = refs[:4], refs[4:8], refs[8:11]
        there = [counts[k][0] > CHUNK + k for k in range(4)]
        refs = refs[11:]
    send, mine, proj, left_v, right_v, psi_v, image, acc_v, rows_v, sub_v, total, staged, sums = refs[:13]
    sem_left, sem_right, sem_psi, sem_acc, sem_rows, sem_sub, sem_out = refs[13:20]
    width = subspace.shape[3]
    core = where[CORE]
    site = where[SITE]
    member = where[MEMBER]

    left_copies = [
        pltpu.make_async_copy(left.at[pl.ds(2 * p, 2)], left_v.at[pl.ds(2 * p, 2)], sem_left.at[p])
        for p in range(2)
    ]
    far_copies = [
        pltpu.make_async_copy(far_a, right_v.at[0], sem_right.at[0]),
        pltpu.make_async_copy(far_b, right_v.at[1], sem_right.at[1]),
    ]
    psi_copies = {
        i: pltpu.make_async_copy(psi.at[(site + i) % 4], psi_v.at[i], sem_psi.at[i])
        for i in ((2, 0, 1, 3) if slots else (2,))
    }
    acc_copies = [
        pltpu.make_async_copy(source, acc_v.at[rel], sem_acc.at[rel])
        for rel, source in ((0, own.at[0]), (1, near.at[0]), (3, near.at[1]))
    ]
    their = jnp.minimum(member, 768 // DIAGONAL_ROWS - 1)
    rows_copy = pltpu.make_async_copy(
        rows.at[pl.ds(pl.multiple_of(DIAGONAL_ROWS * their, DIAGONAL_ROWS), DIAGONAL_ROWS)],
        rows_v,
        sem_rows,
    )

    def sub_copies(step):
        within = 2 * ((1 - core) if step < 2 else core) + step % 2
        return [
            pltpu.make_async_copy(subspace.at[k, within], sub_v.at[step, k], sem_sub.at[step, k]) for k in range(2)
        ]

    for copy in left_copies + far_copies:
        copy.start()
    psi_copies[2].start()
    if slots:
        extra_v, moved_v, sem_extra, sem_moved = refs[20:]
        extra_copies = []
        taken = False
        for k in range(4):
            place = 0 if slots == 1 else k
            copy = pltpu.make_async_copy(extras[k], extra_v.at[place], sem_extra.at[place])
            extra_copies.append((there[k] & jnp.logical_not(taken) if slots == 1 else there[k], copy))
            taken = there[k] | taken
        moved_copies = [
            pltpu.make_async_copy(moved[i], moved_v.at[i + 1], sem_moved.at[i]) for i in range(3)
        ]
    acc_v[2] = jnp.zeros(acc_v.shape[1:], jnp.float32)
    for copy in left_copies + far_copies:
        copy.wait()
    psi_copies[2].wait()

    for copy in acc_copies:
        copy.start()
    if slots:
        for wanted, copy in extra_copies:

            @pl.when(wanted)
            def _():
                copy.start()

        for i in (0, 1, 3):
            psi_copies[i].start()
        for copy in moved_copies:
            copy.start()
    else:
        rows_copy.start()
        for step in range(4):
            for copy in sub_copies(step):
                copy.start()

    def one_pair(p, inner):
        lefts = [lambda within, u=u: left_v[2 * p + u, within] for u in range(2)]
        blocks = [
            lambda q, u=u: jnp.concatenate(
                [right_v[q // 2, 2 * p + u, q % 2], right_v[q // 2, 2 * p + u, 2]], axis=1
            )
            for u in range(2)
        ]
        multiply_slots(lefts, blocks, psi_v.at[2], image, acc_v.at[2], 2 * p + 1 < live)
        return inner

    lax.fori_loop(0, (live + 1) // 2, one_pair, 0)
    for copy in acc_copies:
        copy.wait()
    if slots:
        for wanted, copy in extra_copies:

            @pl.when(wanted)
            def _():
                copy.wait()

        for i in (0, 1, 3):
            psi_copies[i].wait()
        for copy in moved_copies:
            copy.wait()
        rows_copy.start()
        for step in range(4):
            for copy in sub_copies(step):
                copy.start()
        moved_v[0] = extra_v[:, 6:12]
        alive = [jnp.int32(1)] if slots == 1 else [one.astype(jnp.int32) for one in there]

        def one_group(i, carry):
            def one_slot(n, inner):
                wanted = alive[0]
                for k in range(1, slots):
                    wanted = jnp.where(n == k, alive[k], wanted)

                @pl.when(wanted > 0)
                def _():
                    def left_block(within):
                        at = 3 * (within // 2)
                        lane = 64 * (within % 2)
                        high = extra_v[n, at + 2]
                        return jnp.concatenate([extra_v[n, at + within % 2], high[:, lane : lane + 64]], axis=1)

                    def right_block(q):
                        at = 3 * (q // 2)
                        return jnp.concatenate([moved_v[i, n, at + q % 2], moved_v[i, n, at + 2]], axis=1)

                    multiply_slots([left_block], [right_block], psi_v.at[i], image, acc_v.at[i], None)

                return inner

            lax.fori_loop(0, slots, one_slot, 0)
            return carry

        lax.fori_loop(0, 4, one_group, 0)
    rows_copy.wait()

    lane = lax.broadcasted_iota(jnp.int32, (192, 128), 1)
    row = lax.broadcasted_iota(jnp.int32, (192, width), 0)
    sums[...] = jnp.zeros(sums.shape, jnp.float32)

    def out_copy(step):
        out = send if step < 2 else mine
        return pltpu.make_async_copy(staged.at[step], out.at[pl.ds(192 * (step % 2), 192)], sem_out.at[step])

    def one_block(step, carry):
        for j in range(4):

            @pl.when(step == j)
            def _():
                for copy in sub_copies(j):
                    copy.wait()

        within = 2 * jnp.where(step < 2, 1 - core, core) + step % 2
        here = pl.ds(pl.multiple_of(192 * within, 192), 192)

        def one_site(i, inner):
            rel = (i + 4 - site) % 4
            for q in range(4):
                start = table[RIGHT_START + 4 * i + q]
                base = pl.multiple_of((start // 128) * 128, 128)
                shift = start - base
                first = pltpu.roll(acc_v[rel, here, q * SLOT_COLS : q * SLOT_COLS + 128], shift, 1)
                second = pltpu.roll(acc_v[rel, here, q * SLOT_COLS + 128 : (q + 1) * SLOT_COLS], shift, 1)
                low = lane < shift
                total[:, pl.ds(base, 128)] = jnp.where(low, total[:, pl.ds(base, 128)], first)
                total[:, pl.ds(base + 128, 128)] = jnp.where(low, first, second)
                total[:, pl.ds(base + 256, 128)] = second
            return inner

        lax.fori_loop(0, 4, one_site, 0)
        per = 192 // DIAGONAL_ROWS

        @pl.when(member // per == within)
        def _():
            at = pl.multiple_of(DIAGONAL_ROWS * (member % per), DIAGONAL_ROWS)
            part = pl.ds(at, DIAGONAL_ROWS)
            energy = energies[pl.ds(pl.multiple_of(192 * within + at, DIAGONAL_ROWS), DIAGONAL_ROWS), :]
            total[part, :width] += (energy + right_energy[...]) * rows_v[...].astype(jnp.float32)

        kept = jnp.where(row < table[MY_SIZE + within], total[:, :width], 0.0)
        for k in range(2):
            part = sub_v[step, k].astype(jnp.float32) * kept
            sums[k] += jnp.sum(part.reshape(24, 8, width), axis=0)
        staged[step] = kept.astype(jnp.bfloat16)
        for j in range(4):

            @pl.when(step == j)
            def _():
                out_copy(j).start()

        return carry

    lax.fori_loop(0, 4, one_block, 0)
    for k in range(2):
        added = sums[k, :, :128]
        for j in range(1, width // 128):
            added = added + sums[k, :, 128 * j : 128 * (j + 1)]
        proj[k] = added
    for j in range(4):
        out_copy(j).wait()


def finish(slots, where, count, table, own, near, far, left, psi, rows, subspace, energies, right_energy, late=()):
    width = rows.shape[1]
    smem = pl.BlockSpec(memory_space=pltpu.SMEM)
    hbm = pl.BlockSpec(memory_space=pltpu.HBM)
    vmem = pl.BlockSpec(memory_space=pltpu.VMEM)
    half = jax.ShapeDtypeStruct((384, width), jnp.bfloat16)
    scratch = [
        pltpu.VMEM((CHUNK, 4, 192, 192), jnp.bfloat16),
        pltpu.VMEM((2, CHUNK, 3, 192, 128), jnp.bfloat16),
        pltpu.VMEM((4, 768, GROUP_COLS), jnp.bfloat16),
        pltpu.VMEM((2, 768, GROUP_COLS), jnp.bfloat16),
        pltpu.VMEM((4, 768, GROUP_COLS), jnp.float32),
        pltpu.VMEM((DIAGONAL_ROWS, width), jnp.bfloat16),
        pltpu.VMEM((4, 2, 192, width), jnp.bfloat16),
        pltpu.VMEM((192, width + 256), jnp.float32),
        pltpu.VMEM((4, 192, width), jnp.bfloat16),
        pltpu.VMEM((2, 8, width), jnp.float32),
        pltpu.SemaphoreType.DMA((2,)),
        pltpu.SemaphoreType.DMA((2,)),
        pltpu.SemaphoreType.DMA((4,)),
        pltpu.SemaphoreType.DMA((4,)),
        pltpu.SemaphoreType.DMA(()),
        pltpu.SemaphoreType.DMA((4, 2)),
        pltpu.SemaphoreType.DMA((4,)),
    ]
    if slots:
        scratch += [
            pltpu.VMEM((slots, 12, 192, 128), jnp.bfloat16),
            pltpu.VMEM((4, slots, 6, 192, 128), jnp.bfloat16),
            pltpu.SemaphoreType.DMA((4,)),
            pltpu.SemaphoreType.DMA((3,)),
        ]
    return pl.pallas_call(
        functools.partial(finish_body, slots),
        in_specs=[smem] * 3 + [hbm] * 8 + [vmem, vmem] + ([smem] * 4 + [hbm] * 7 if slots else []),
        out_specs=[hbm, hbm, vmem],
        out_shape=[half, half, jax.ShapeDtypeStruct((2, 8, 128), jnp.float32)],
        scratch_shapes=scratch,
        compiler_params=params(),
        cost_estimate=pl.CostEstimate(flops=8 * 10**9, bytes_accessed=30 * 2**20, transcendentals=0),
        name="finish",
    )(where, count, table, own, near, *far, left, psi, rows, subspace, energies, right_energy, *late)


def place_body(which, where, half, *rest):
    out, held, sem_in, sem_out = rest[-4:]
    core = where[CORE] if which == 0 else 1 - where[CORE]
    parts = [(i, pl.ds(96 * j, 96)) for i in range(2) for j in range(2)]
    inward = [
        pltpu.make_async_copy(half.at[i, part], held.at[i, part], sem_in.at[n]) for n, (i, part) in enumerate(parts)
    ]
    outward = [
        pltpu.make_async_copy(held.at[i, part], out.at[2 * core + i, part], sem_out.at[n])
        for n, (i, part) in enumerate(parts)
    ]
    for copy in inward:
        copy.start()
    for came, goes in zip(inward, outward, strict=True):
        came.wait()
        goes.start()
    for copy in outward:
        copy.wait()


def place(which, where, half, whole=None):
    hbm = pl.BlockSpec(memory_space=pltpu.HBM)
    args = (where, half) if whole is None else (where, half, whole)
    return pl.pallas_call(
        functools.partial(place_body, which),
        in_specs=[pl.BlockSpec(memory_space=pltpu.SMEM)] + [hbm] * (len(args) - 1),
        out_specs=hbm,
        out_shape=jax.ShapeDtypeStruct((4,) + half.shape[1:], half.dtype),
        scratch_shapes=[
            pltpu.VMEM(half.shape, half.dtype),
            pltpu.SemaphoreType.DMA((4,)),
            pltpu.SemaphoreType.DMA((4,)),
        ],
        input_output_aliases={} if whole is None else {2: 0},
        cost_estimate=pl.CostEstimate(flops=10**9, bytes_accessed=2**22, transcendentals=0),
        name="place",
    )(*args)


def shifted(value, axis, by):
    size = lax.axis_size(axis)
    return lax.ppermute(value, axis, [(i, (i + by) % size) for i in range(size)])


def small_sum(value, axis):
    size = lax.axis_size(axis)
    me = lax.axis_index(axis)
    got = [value] + [shifted(value, axis, k) for k in range(1, size)]
    total = None
    for source in range(size):
        one = sum(jnp.where((me - source) % size == k, got[k], 0.0) for k in range(size))
        total = one if total is None else total + one
    return total


def local(
    wavefunction,
    left_blocks,
    right_blocks,
    left_sector,
    right_sector,
    term_count,
    left_energy,
    right_energy,
    subspace,
):
    bond = wavefunction.shape[0]
    site = lax.axis_index("site")
    core = lax.axis_index("core")
    mine_early = pack_early(right_blocks)
    prev = shifted(mine_early, "site", 1)
    following = shifted(mine_early, "site", -1)
    left_later, right_later, count_later, _ = lax.optimization_barrier(
        (left_blocks, right_blocks, term_count, mine_early)
    )

    ways = (("y", 1), ("y", -1), ("z", 1), ("z", -1))
    late = pack_late(left_later, right_later)
    extras = [shifted(late[k], axis, by) for k, (axis, by) in enumerate(ways)]
    counts = [shifted(count_later, axis, by) for axis, by in ways]
    there = [counts[k][0] > CHUNK + k for k in range(4)]
    number = sum(one.astype(jnp.int32) for one in there)

    where = jnp.stack([site, core, lax.axis_index(OPS)])
    table, rows, psi, energies = select(where, left_sector, right_sector, left_energy, wavefunction)
    own = products((0,), where, term_count, left_blocks, psi, [mine_early])

    def rest(slots, going, prev, following):
        far = (shifted(prev[0], "site", 1), shifted(following[1], "site", -1))
        arrived = []
        if slots:
            arrived = [*counts, *extras] + [shifted(going, "site", by) for by in (-1, 2, 1)]
        near = products((1, 3), where, term_count, left_blocks, psi, [following, prev])
        return tuple(
            finish(
                slots,
                where,
                term_count,
                table,
                own,
                near,
                far,
                left_blocks,
                psi,
                rows,
                subspace,
                energies,
                right_energy[None, :],
                late=arrived,
            )
        )

    def none(*moved):
        return rest(0, None, *moved)

    def one(*moved):
        going = extras[3][6:12]
        for k in (2, 1, 0):
            going = jnp.where(there[k], extras[k][6:12], going)
        return rest(1, going[None], *moved)

    def many(*moved):
        return rest(4, jnp.stack([one[6:12] for one in extras]), *moved)

    send, mine, proj = lax.switch(jnp.minimum(number, 2), [none, one, many], prev, following)
    swap = [(0, 1), (1, 0)]
    away = lax.ppermute(send, "core", swap)
    proj = small_sum(jnp.broadcast_to(jnp.sum(proj, axis=(1, 2))[None, :], (8, 2)), "site")[0]
    both = (mine.astype(jnp.float32) + away.astype(jnp.float32)).astype(jnp.bfloat16)

    high = lax.reduce_precision(proj, 8, 7)
    middle = lax.reduce_precision(proj - high, 8, 7)
    thirds = jnp.concatenate([high, middle, proj - high - middle]).astype(jnp.bfloat16)
    plane = lax.axis_size(("z", "y"))
    half = both.shape[0]
    share = half // plane
    extra = jnp.broadcast_to(jnp.pad(thirds, (0, EXTRA - 6))[None, :], (half, EXTRA))
    both = jnp.concatenate([both, extra], axis=1)

    pieces = lax.all_to_all(both.reshape(plane, share, bond + EXTRA), ("z", "y"), 0, 0, tiled=True)
    added = jnp.sum(pieces.astype(jnp.float32), axis=0)
    summed = added[:, :bond].astype(jnp.bfloat16)
    gathered = lax.all_to_all(
        jnp.broadcast_to(summed[None], (plane, share, bond)), ("z", "y"), 0, 0, tiled=True
    ).reshape(half, bond)
    whole = added[:8, bond : bond + 2] + added[:8, bond + 2 : bond + 4] + added[:8, bond + 4 : bond + 6]
    gathered = gathered.reshape(2, 192, bond)
    other = lax.ppermute(gathered, "core", swap)
    projections = whole + lax.ppermute(whole, "core", swap)
    sigma = place(1, where, other, place(0, where, gathered))
    return sigma, projections[0]


def solution(mesh):
    shape = dict(mesh.shape)
    ops = shape["ops"]
    parts = Mesh(mesh.devices.reshape(4, ops // 8, 2, shape["site"]), ("z", "y", "core", "site"))
    in_specs = (
        P(),
        P(OPS, "site", None, None),
        P(OPS, "site", None, None),
        P(),
        P(),
        P(OPS),
        P(),
        P(),
        P(None, "site", None, None),
    )
    out_specs = (P("site", None, None), P())
    return jax.shard_map(local, mesh=parts, in_specs=in_specs, out_specs=out_specs, check_vma=False)
```

```python
import functools

import jax
import jax.numpy as jnp
from jax import lax
from jax.experimental import pallas as pl
from jax.experimental.pallas import tpu as pltpu
from jax.sharding import Mesh
from jax.sharding import PartitionSpec as P


OPS = ("z", "y", "core")
CHUNK = 4
WIN_ROWS = 256
WIN_COLS = 384
SLOT_COLS = 256
GROUP_COLS = 4 * SLOT_COLS
EXTRA = 128

MY_START, MY_SIZE, RIGHT_START, RIGHT_SIZE = 0, 4, 8, 24
SITE, CORE, MEMBER = 0, 1, 2
DIAGONAL_ROWS = 32


def params():
    return pltpu.CompilerParams(vmem_limit_bytes=56 * 1024 * 1024)


def pack_one(blocks, slot, half, out, index, at=0):
    out[index + (at,)] = blocks[slot, 2 * half, :, :128]
    out[index + (at + 1,)] = blocks[slot, 2 * half + 1, :, :128]
    out[index + (at + 2,)] = jnp.concatenate(
        [blocks[slot, 2 * half, :, 128:192], blocks[slot, 2 * half + 1, :, 128:192]], axis=1
    )


def pack_early_body(blocks, first, second):
    for slot in range(2):
        pack_one(blocks, slot, 0, first, (slot,))
        pack_one(blocks, slot, 1, second, (slot,))


def pack_late_body(left, right, *outs):
    for k in range(4):

        @pl.when(pl.program_id(0) == k)
        def _():
            for half in range(2):
                pack_one(left, 0, half, outs[k], (), 3 * half)
                pack_one(right, 0, half, outs[k], (), 6 + 3 * half)


def pack_early(blocks):
    spec = pl.BlockSpec((2, 3, 192, 128), lambda i: (i, 0, 0, 0))
    shape = jax.ShapeDtypeStruct((CHUNK, 3, 192, 128), jnp.bfloat16)
    return pl.pallas_call(
        pack_early_body,
        grid=(2,),
        in_specs=[pl.BlockSpec((2, 4, 192, 192), lambda i: (i, 0, 0, 0))],
        out_specs=[spec, spec],
        out_shape=[shape, shape],
        name="pack_early",
    )(blocks)


def pack_late(left, right):
    block = pl.BlockSpec((1, 4, 192, 192), lambda i: (i + CHUNK, 0, 0, 0))
    return pl.pallas_call(
        pack_late_body,
        grid=(4,),
        in_specs=[block, block],
        out_specs=[pl.BlockSpec((12, 192, 128), lambda i: (0, 0, 0))] * 4,
        out_shape=[jax.ShapeDtypeStruct((12, 192, 128), jnp.bfloat16)] * 4,
        cost_estimate=pl.CostEstimate(flops=2 * 10**9, bytes_accessed=2**22, transcendentals=0),
        name="pack_late",
    )(left, right)


def select_body(where, left_sector, right_sector, left_energy, psi, table, rows, cols, energies, window, sems):
    group = pl.program_id(0)

    @pl.when(group == 0)
    def _():
        site = where[SITE]
        left_ids = left_sector[...]
        right_ids = right_sector[...]
        for within in range(4):
            sector = 4 * site + within
            table[MY_START + within] = jnp.sum((left_ids < sector).astype(jnp.int32))
            table[MY_SIZE + within] = jnp.sum((left_ids == sector).astype(jnp.int32))
        before = jnp.int32(0)
        for sector in range(16):
            size = jnp.sum((right_ids == sector).astype(jnp.int32))
            table[RIGHT_START + sector] = before
            table[RIGHT_SIZE + sector] = size
            before = before + size
        copies = []
        shifts = []
        for within in range(4):
            start = table[MY_START + within]
            base = pl.multiple_of(jnp.minimum((start // 16) * 16, psi.shape[0] - WIN_ROWS), 16)
            shifts.append(start - base)
            copies.append(
                pltpu.make_async_copy(psi.at[pl.ds(base, WIN_ROWS), :], window.at[within], sems.at[within])
            )
        for copy in copies:
            copy.start()
        row = lax.broadcasted_iota(jnp.int32, (192, WIN_ROWS), 0)
        col = lax.broadcasted_iota(jnp.int32, (192, WIN_ROWS), 1)
        wide_row = lax.broadcasted_iota(jnp.int32, (192, WIN_COLS), 0)
        wide_col = lax.broadcasted_iota(jnp.int32, (192, WIN_COLS), 1)
        for within in range(4):
            start = table[MY_START + within]
            size = table[MY_SIZE + within]
            base = pl.multiple_of(jnp.minimum((start // 128) * 128, psi.shape[0] - WIN_COLS), 128)
            kept = (wide_col == wide_row + (start - base)) & (wide_row < size)
            near = jnp.where(kept, left_energy[:, pl.ds(base, WIN_COLS)], 0.0)
            energies[pl.ds(within * 192, 192), :] = jnp.sum(near, axis=1, keepdims=True)
        for within in range(4):
            copies[within].wait()
            kept = (col == row + shifts[within]) & (row < table[MY_SIZE + within])
            pick = jnp.where(kept, 1.0, 0.0).astype(jnp.bfloat16)
            got = jnp.dot(pick, window[within], preferred_element_type=jnp.float32)
            rows[pl.ds(within * 192, 192), :] = got.astype(jnp.bfloat16)

    row = lax.broadcasted_iota(jnp.int32, (WIN_COLS, SLOT_COLS), 0)
    lane = lax.broadcasted_iota(jnp.int32, (WIN_COLS, SLOT_COLS), 1)

    def two_sectors(half, carry):
        for odd in range(2):
            start = table[RIGHT_START + 4 * group + 2 * half + odd]
            size = table[RIGHT_SIZE + 4 * group + 2 * half + odd]
            base = pl.multiple_of(jnp.minimum((start // 128) * 128, rows.shape[1] - WIN_COLS), 128)
            at = jnp.where(lane < 128, lane, jnp.where(lane < 192, size, lane - 64)) if odd else lane
            kept = (row == at + (start - base)) & (at < size)
            pick = jnp.where(kept, 1.0, 0.0).astype(jnp.bfloat16)
            got = jnp.dot(rows[:, pl.ds(base, WIN_COLS)], pick, preferred_element_type=jnp.float32)
            where_to = pl.multiple_of(SLOT_COLS * (2 * half + odd), SLOT_COLS)
            cols[0, :, pl.ds(where_to, SLOT_COLS)] = got.astype(jnp.bfloat16)
        return carry

    lax.fori_loop(0, 2, two_sectors, 0)


def select(where, left_sector, right_sector, left_energy, psi):
    bond = psi.shape[1]
    smem = pl.BlockSpec(memory_space=pltpu.SMEM)
    ids = pl.BlockSpec((bond // 128, 128), lambda g: (0, 0))
    return pl.pallas_call(
        select_body,
        grid=(4,),
        in_specs=[smem, ids, ids, pl.BlockSpec((1, bond), lambda g: (0, 0)), pl.BlockSpec(memory_space=pltpu.HBM)],
        out_specs=[
            smem,
            pl.BlockSpec((768, bond), lambda g: (0, 0)),
            pl.BlockSpec((1, 768, GROUP_COLS), lambda g: (g, 0, 0)),
            pl.BlockSpec((768, 1), lambda g: (0, 0)),
        ],
        out_shape=[
            jax.ShapeDtypeStruct((40,), jnp.int32),
            jax.ShapeDtypeStruct((768, bond), jnp.bfloat16),
            jax.ShapeDtypeStruct((4, 768, GROUP_COLS), jnp.bfloat16),
            jax.ShapeDtypeStruct((768, 1), jnp.float32),
        ],
        scratch_shapes=[
            pltpu.VMEM((4, WIN_ROWS, bond), jnp.bfloat16),
            pltpu.SemaphoreType.DMA((4,)),
        ],
        compiler_params=params(),
        cost_estimate=pl.CostEstimate(flops=5 * 10**9, bytes_accessed=2**24, transcendentals=0),
        name="select",
    )(
        where,
        left_sector.reshape(bond // 128, 128),
        right_sector.reshape(bond // 128, 128),
        left_energy[None, :],
        psi,
    )


def multiply_slots(lefts, rights, psi, image, acc, last_live):
    count = len(lefts)
    for u in range(count):
        for within in range(4):
            got = jnp.dot(
                lefts[u](within), psi[within * 192 : (within + 1) * 192, :], preferred_element_type=jnp.float32
            )
            if u == 1:
                got = jnp.where(last_live, got, 0.0)
            image[u, within * 192 : (within + 1) * 192, :] = got.astype(jnp.bfloat16)
    for q in range(4):
        parts = None
        for u in range(count):
            block = jnp.concatenate([rights[u](q), jnp.zeros((64, 256), jnp.bfloat16)], axis=0)
            part = lax.dot_general(
                image[u, :, q * SLOT_COLS : (q + 1) * SLOT_COLS],
                block,
                (((1,), (1,)), ((), ())),
                preferred_element_type=jnp.float32,
            )
            parts = part if parts is None else parts + part
        acc[:, q * SLOT_COLS : (q + 1) * SLOT_COLS] += parts


def products_body(rels, where, count, left, psi, *refs):
    groups = len(rels)
    live = jnp.minimum(count[0], CHUNK)
    rights = [refs[2 * i : 2 * i + 2] for i in range(groups)]
    out, left_v, right_v, psi_v, image, acc_v, sem_left, sem_right, sem_psi, sem_out = refs[2 * groups :]
    site = where[SITE]
    left_copies = [
        pltpu.make_async_copy(left.at[pl.ds(2 * p, 2)], left_v.at[pl.ds(2 * p, 2)], sem_left.at[p])
        for p in range(2)
    ]
    copies = []
    for i in range(groups):
        copies.append(
            [
                pltpu.make_async_copy(rights[i][0], right_v.at[i, 0], sem_right.at[i, 0]),
                pltpu.make_async_copy(rights[i][1], right_v.at[i, 1], sem_right.at[i, 1]),
                pltpu.make_async_copy(psi.at[(site + rels[i]) % 4], psi_v.at[i], sem_psi.at[i]),
            ]
        )
    out_copies = [
        [
            pltpu.make_async_copy(
                acc_v.at[i, pl.ds(192 * w, 192)], out.at[i, pl.ds(192 * w, 192)], sem_out.at[i, w]
            )
            for w in range(4)
        ]
        for i in range(groups)
    ]
    for copy in left_copies + copies[0]:
        copy.start()
    acc_v[0] = jnp.zeros(acc_v.shape[1:], jnp.float32)
    for copy in left_copies:
        copy.wait()

    def one_group(i, carry):
        for j in range(groups):

            @pl.when(i == j)
            def _():
                for copy in copies[j]:
                    copy.wait()
                if j + 1 < groups:
                    for copy in copies[j + 1]:
                        copy.start()
                    acc_v[j + 1] = jnp.zeros(acc_v.shape[1:], jnp.float32)

        def one_pair(p, inner):
            lefts = [lambda within, u=u: left_v[2 * p + u, within] for u in range(2)]
            block = [
                lambda q, u=u: jnp.concatenate(
                    [right_v[i, q // 2, 2 * p + u, q % 2], right_v[i, q // 2, 2 * p + u, 2]], axis=1
                )
                for u in range(2)
            ]
            multiply_slots(lefts, block, psi_v.at[i], image, acc_v.at[i], 2 * p + 1 < live)
            return inner

        lax.fori_loop(0, (live + 1) // 2, one_pair, 0)
        for j in range(groups):

            @pl.when(i == j)
            def _():
                for copy in out_copies[j]:
                    copy.start()

        return carry

    lax.fori_loop(0, groups, one_group, 0)
    for found in out_copies:
        for copy in found:
            copy.wait()


def products(rels, where, count, left, psi, rights):
    groups = len(rels)
    smem = pl.BlockSpec(memory_space=pltpu.SMEM)
    hbm = pl.BlockSpec(memory_space=pltpu.HBM)
    flops = groups * 2 * 1024 * 768 * (192 + 256) * 4
    return pl.pallas_call(
        functools.partial(products_body, tuple(rels)),
        in_specs=[smem, smem, hbm, hbm] + [hbm] * (2 * groups),
        out_specs=hbm,
        out_shape=jax.ShapeDtypeStruct((groups, 768, GROUP_COLS), jnp.float32),
        scratch_shapes=[
            pltpu.VMEM((CHUNK, 4, 192, 192), jnp.bfloat16),
            pltpu.VMEM((groups, 2, CHUNK, 3, 192, 128), jnp.bfloat16),
            pltpu.VMEM((groups, 768, GROUP_COLS), jnp.bfloat16),
            pltpu.VMEM((2, 768, GROUP_COLS), jnp.bfloat16),
            pltpu.VMEM((groups, 768, GROUP_COLS), jnp.float32),
            pltpu.SemaphoreType.DMA((2,)),
            pltpu.SemaphoreType.DMA((groups, 2)),
            pltpu.SemaphoreType.DMA((groups,)),
            pltpu.SemaphoreType.DMA((groups, 4)),
        ],
        compiler_params=params(),
        cost_estimate=pl.CostEstimate(flops=flops, bytes_accessed=8 * 2**20, transcendentals=0),
        name="products",
    )(where, count, left, psi, *[half for halves in rights for half in halves])


def finish_body(slots, where, count, table, own, near, far_a, far_b, left, psi, *refs):
    live = jnp.minimum(count[0], CHUNK)
    rows, subspace, energies, right_energy = refs[:4]
    refs = list(refs[4:])
    if slots:
        counts, extras, moved = refs[:4], refs[4:8], refs[8:11]
        there = [counts[k][0] > CHUNK + k for k in range(4)]
        refs = refs[11:]
    send, mine, proj, left_v, right_v, psi_v, image, acc_v, rows_v, sub_v, total, staged, sums = refs[:13]
    sem_left, sem_right, sem_psi, sem_acc, sem_rows, sem_sub, sem_out = refs[13:20]
    width = subspace.shape[3]
    core = where[CORE]
    site = where[SITE]
    member = where[MEMBER]

    left_copies = [
        pltpu.make_async_copy(left.at[pl.ds(2 * p, 2)], left_v.at[pl.ds(2 * p, 2)], sem_left.at[p])
        for p in range(2)
    ]
    far_copies = [
        pltpu.make_async_copy(far_a, right_v.at[0], sem_right.at[0]),
        pltpu.make_async_copy(far_b, right_v.at[1], sem_right.at[1]),
    ]
    psi_copies = {
        i: pltpu.make_async_copy(psi.at[(site + i) % 4], psi_v.at[i], sem_psi.at[i])
        for i in ((2, 0, 1, 3) if slots else (2,))
    }
    acc_copies = [
        pltpu.make_async_copy(source, acc_v.at[rel], sem_acc.at[rel])
        for rel, source in ((0, own.at[0]), (1, near.at[0]), (3, near.at[1]))
    ]
    their = jnp.minimum(member, 768 // DIAGONAL_ROWS - 1)
    rows_copy = pltpu.make_async_copy(
        rows.at[pl.ds(pl.multiple_of(DIAGONAL_ROWS * their, DIAGONAL_ROWS), DIAGONAL_ROWS)],
        rows_v,
        sem_rows,
    )

    def sub_copies(step):
        within = 2 * ((1 - core) if step < 2 else core) + step % 2
        return [
            pltpu.make_async_copy(subspace.at[k, within], sub_v.at[step, k], sem_sub.at[step, k]) for k in range(2)
        ]

    for copy in left_copies + far_copies:
        copy.start()
    psi_copies[2].start()
    if slots:
        extra_v, moved_v, sem_extra, sem_moved = refs[20:]
        extra_copies = []
        taken = False
        for k in range(4):
            place = 0 if slots == 1 else k
            copy = pltpu.make_async_copy(extras[k], extra_v.at[place], sem_extra.at[place])
            extra_copies.append((there[k] & jnp.logical_not(taken) if slots == 1 else there[k], copy))
            taken = there[k] | taken
        moved_copies = [
            pltpu.make_async_copy(moved[i], moved_v.at[i + 1], sem_moved.at[i]) for i in range(3)
        ]
    acc_v[2] = jnp.zeros(acc_v.shape[1:], jnp.float32)
    for copy in left_copies + far_copies:
        copy.wait()
    psi_copies[2].wait()

    for copy in acc_copies:
        copy.start()
    if slots:
        for wanted, copy in extra_copies:

            @pl.when(wanted)
            def _():
                copy.start()

        for i in (0, 1, 3):
            psi_copies[i].start()
        for copy in moved_copies:
            copy.start()
    else:
        rows_copy.start()
        for step in range(4):
            for copy in sub_copies(step):
                copy.start()

    def one_pair(p, inner):
        lefts = [lambda within, u=u: left_v[2 * p + u, within] for u in range(2)]
        blocks = [
            lambda q, u=u: jnp.concatenate(
                [right_v[q // 2, 2 * p + u, q % 2], right_v[q // 2, 2 * p + u, 2]], axis=1
            )
            for u in range(2)
        ]
        multiply_slots(lefts, blocks, psi_v.at[2], image, acc_v.at[2], 2 * p + 1 < live)
        return inner

    lax.fori_loop(0, (live + 1) // 2, one_pair, 0)
    for copy in acc_copies:
        copy.wait()
    if slots:
        for wanted, copy in extra_copies:

            @pl.when(wanted)
            def _():
                copy.wait()

        for i in (0, 1, 3):
            psi_copies[i].wait()
        for copy in moved_copies:
            copy.wait()
        rows_copy.start()
        for step in range(4):
            for copy in sub_copies(step):
                copy.start()
        moved_v[0] = extra_v[:, 6:12]
        alive = [jnp.int32(1)] if slots == 1 else [one.astype(jnp.int32) for one in there]

        def one_group(i, carry):
            def one_slot(n, inner):
                wanted = alive[0]
                for k in range(1, slots):
                    wanted = jnp.where(n == k, alive[k], wanted)

                @pl.when(wanted > 0)
                def _():
                    def left_block(within):
                        at = 3 * (within // 2)
                        lane = 64 * (within % 2)
                        high = extra_v[n, at + 2]
                        return jnp.concatenate([extra_v[n, at + within % 2], high[:, lane : lane + 64]], axis=1)

                    def right_block(q):
                        at = 3 * (q // 2)
                        return jnp.concatenate([moved_v[i, n, at + q % 2], moved_v[i, n, at + 2]], axis=1)

                    multiply_slots([left_block], [right_block], psi_v.at[i], image, acc_v.at[i], None)

                return inner

            lax.fori_loop(0, slots, one_slot, 0)
            return carry

        lax.fori_loop(0, 4, one_group, 0)
    rows_copy.wait()

    lane = lax.broadcasted_iota(jnp.int32, (192, 128), 1)
    row = lax.broadcasted_iota(jnp.int32, (192, width), 0)
    sums[...] = jnp.zeros(sums.shape, jnp.float32)

    def out_copy(step):
        out = send if step < 2 else mine
        return pltpu.make_async_copy(staged.at[step], out.at[pl.ds(192 * (step % 2), 192)], sem_out.at[step])

    def one_block(step, carry):
        for j in range(4):

            @pl.when(step == j)
            def _():
                for copy in sub_copies(j):
                    copy.wait()

        within = 2 * jnp.where(step < 2, 1 - core, core) + step % 2
        here = pl.ds(pl.multiple_of(192 * within, 192), 192)

        def one_site(i, inner):
            rel = (i + 4 - site) % 4
            for q in range(4):
                start = table[RIGHT_START + 4 * i + q]
                base = pl.multiple_of((start // 128) * 128, 128)
                shift = start - base
                first = pltpu.roll(acc_v[rel, here, q * SLOT_COLS : q * SLOT_COLS + 128], shift, 1)
                second = pltpu.roll(acc_v[rel, here, q * SLOT_COLS + 128 : (q + 1) * SLOT_COLS], shift, 1)
                low = lane < shift
                total[:, pl.ds(base, 128)] = jnp.where(low, total[:, pl.ds(base, 128)], first)
                total[:, pl.ds(base + 128, 128)] = jnp.where(low, first, second)
                total[:, pl.ds(base + 256, 128)] = second
            return inner

        lax.fori_loop(0, 4, one_site, 0)
        per = 192 // DIAGONAL_ROWS

        @pl.when(member // per == within)
        def _():
            at = pl.multiple_of(DIAGONAL_ROWS * (member % per), DIAGONAL_ROWS)
            part = pl.ds(at, DIAGONAL_ROWS)
            energy = energies[pl.ds(pl.multiple_of(192 * within + at, DIAGONAL_ROWS), DIAGONAL_ROWS), :]
            total[part, :width] += (energy + right_energy[...]) * rows_v[...].astype(jnp.float32)

        kept = jnp.where(row < table[MY_SIZE + within], total[:, :width], 0.0)
        for k in range(2):
            part = sub_v[step, k].astype(jnp.float32) * kept
            sums[k] += jnp.sum(part.reshape(24, 8, width), axis=0)
        staged[step] = kept.astype(jnp.bfloat16)
        for j in range(4):

            @pl.when(step == j)
            def _():
                out_copy(j).start()

        return carry

    lax.fori_loop(0, 4, one_block, 0)
    for k in range(2):
        added = sums[k, :, :128]
        for j in range(1, width // 128):
            added = added + sums[k, :, 128 * j : 128 * (j + 1)]
        proj[k] = added
    for j in range(4):
        out_copy(j).wait()


def finish(slots, where, count, table, own, near, far, left, psi, rows, subspace, energies, right_energy, late=()):
    width = rows.shape[1]
    smem = pl.BlockSpec(memory_space=pltpu.SMEM)
    hbm = pl.BlockSpec(memory_space=pltpu.HBM)
    vmem = pl.BlockSpec(memory_space=pltpu.VMEM)
    half = jax.ShapeDtypeStruct((384, width), jnp.bfloat16)
    scratch = [
        pltpu.VMEM((CHUNK, 4, 192, 192), jnp.bfloat16),
        pltpu.VMEM((2, CHUNK, 3, 192, 128), jnp.bfloat16),
        pltpu.VMEM((4, 768, GROUP_COLS), jnp.bfloat16),
        pltpu.VMEM((2, 768, GROUP_COLS), jnp.bfloat16),
        pltpu.VMEM((4, 768, GROUP_COLS), jnp.float32),
        pltpu.VMEM((DIAGONAL_ROWS, width), jnp.bfloat16),
        pltpu.VMEM((4, 2, 192, width), jnp.bfloat16),
        pltpu.VMEM((192, width + 256), jnp.float32),
        pltpu.VMEM((4, 192, width), jnp.bfloat16),
        pltpu.VMEM((2, 8, width), jnp.float32),
        pltpu.SemaphoreType.DMA((2,)),
        pltpu.SemaphoreType.DMA((2,)),
        pltpu.SemaphoreType.DMA((4,)),
        pltpu.SemaphoreType.DMA((4,)),
        pltpu.SemaphoreType.DMA(()),
        pltpu.SemaphoreType.DMA((4, 2)),
        pltpu.SemaphoreType.DMA((4,)),
    ]
    if slots:
        scratch += [
            pltpu.VMEM((slots, 12, 192, 128), jnp.bfloat16),
            pltpu.VMEM((4, slots, 6, 192, 128), jnp.bfloat16),
            pltpu.SemaphoreType.DMA((4,)),
            pltpu.SemaphoreType.DMA((3,)),
        ]
    return pl.pallas_call(
        functools.partial(finish_body, slots),
        in_specs=[smem] * 3 + [hbm] * 8 + [vmem, vmem] + ([smem] * 4 + [hbm] * 7 if slots else []),
        out_specs=[hbm, hbm, vmem],
        out_shape=[half, half, jax.ShapeDtypeStruct((2, 8, 128), jnp.float32)],
        scratch_shapes=scratch,
        compiler_params=params(),
        cost_estimate=pl.CostEstimate(flops=8 * 10**9, bytes_accessed=30 * 2**20, transcendentals=0),
        name="finish",
    )(where, count, table, own, near, *far, left, psi, rows, subspace, energies, right_energy, *late)


def place_body(which, where, half, *rest):
    out, sems = rest[-2:]
    core = where[CORE] if which == 0 else 1 - where[CORE]
    copies = [
        pltpu.make_async_copy(
            half.at[n // 2, pl.ds(96 * (n % 2), 96)],
            out.at[2 * core + n // 2, pl.ds(96 * (n % 2), 96)],
            sems.at[n],
        )
        for n in range(4)
    ]
    for copy in copies:
        copy.start()
    for copy in copies:
        copy.wait()


def place(which, where, half, whole=None):
    hbm = pl.BlockSpec(memory_space=pltpu.HBM)
    args = (where, half) if whole is None else (where, half, whole)
    return pl.pallas_call(
        functools.partial(place_body, which),
        in_specs=[pl.BlockSpec(memory_space=pltpu.SMEM), pl.BlockSpec(memory_space=pltpu.VMEM)]
        + [hbm] * (len(args) - 2),
        out_specs=hbm,
        out_shape=jax.ShapeDtypeStruct((4,) + half.shape[1:], half.dtype),
        scratch_shapes=[pltpu.SemaphoreType.DMA((4,))],
        input_output_aliases={} if whole is None else {2: 0},
        cost_estimate=pl.CostEstimate(flops=10**9, bytes_accessed=2**22, transcendentals=0),
        name="place",
    )(*args)


def shifted(value, axis, by):
    size = lax.axis_size(axis)
    return lax.ppermute(value, axis, [(i, (i + by) % size) for i in range(size)])


def small_sum(value, axis):
    size = lax.axis_size(axis)
    me = lax.axis_index(axis)
    got = [value] + [shifted(value, axis, k) for k in range(1, size)]
    total = None
    for source in range(size):
        one = sum(jnp.where((me - source) % size == k, got[k], 0.0) for k in range(size))
        total = one if total is None else total + one
    return total


def local(
    wavefunction,
    left_blocks,
    right_blocks,
    left_sector,
    right_sector,
    term_count,
    left_energy,
    right_energy,
    subspace,
):
    bond = wavefunction.shape[0]
    site = lax.axis_index("site")
    core = lax.axis_index("core")
    mine_early = pack_early(right_blocks)
    prev = [shifted(half, "site", 1) for half in mine_early]
    following = [shifted(half, "site", -1) for half in mine_early]
    left_later, right_later, count_later, _ = lax.optimization_barrier(
        (left_blocks, right_blocks, term_count, mine_early[0])
    )

    ways = (("y", 1), ("y", -1), ("z", 1), ("z", -1))
    late = pack_late(left_later, right_later)
    extras = [shifted(late[k], axis, by) for k, (axis, by) in enumerate(ways)]
    counts = [shifted(count_later, axis, by) for axis, by in ways]
    there = [counts[k][0] > CHUNK + k for k in range(4)]
    number = sum(one.astype(jnp.int32) for one in there)

    where = jnp.stack([site, core, lax.axis_index(OPS)])
    table, rows, psi, energies = select(where, left_sector, right_sector, left_energy, wavefunction)
    own = products((0,), where, term_count, left_blocks, psi, [mine_early])

    def rest(slots, going, prev, following):
        far = (shifted(prev[0], "site", 1), shifted(following[1], "site", -1))
        arrived = []
        if slots:
            arrived = [*counts, *extras] + [shifted(going, "site", by) for by in (-1, 2, 1)]
        near = products((1, 3), where, term_count, left_blocks, psi, [following, prev])
        return tuple(
            finish(
                slots,
                where,
                term_count,
                table,
                own,
                near,
                far,
                left_blocks,
                psi,
                rows,
                subspace,
                energies,
                right_energy[None, :],
                late=arrived,
            )
        )

    def none(*moved):
        return rest(0, None, *moved)

    def one(*moved):
        going = extras[3][6:12]
        for k in (2, 1, 0):
            going = jnp.where(there[k], extras[k][6:12], going)
        return rest(1, going[None], *moved)

    def many(*moved):
        return rest(4, jnp.stack([one[6:12] for one in extras]), *moved)

    send, mine, proj = lax.switch(jnp.minimum(number, 2), [none, one, many], prev, following)
    swap = [(0, 1), (1, 0)]
    away = lax.ppermute(send, "core", swap)
    proj = small_sum(jnp.broadcast_to(jnp.sum(proj, axis=(1, 2))[None, :], (8, 2)), "site")[0]
    both = (mine.astype(jnp.float32) + away.astype(jnp.float32)).astype(jnp.bfloat16)

    high = lax.reduce_precision(proj, 8, 7)
    middle = lax.reduce_precision(proj - high, 8, 7)
    thirds = jnp.concatenate([high, middle, proj - high - middle]).astype(jnp.bfloat16)
    plane = lax.axis_size(("z", "y"))
    half = both.shape[0]
    share = half // plane
    extra = jnp.broadcast_to(jnp.pad(thirds, (0, EXTRA - 6))[None, :], (half, EXTRA))
    both = jnp.concatenate([both, extra], axis=1)

    pieces = lax.all_to_all(both.reshape(plane, share, bond + EXTRA), ("z", "y"), 0, 0, tiled=True)
    added = jnp.sum(pieces.astype(jnp.float32), axis=0)
    summed = added[:, :bond].astype(jnp.bfloat16)
    gathered = lax.all_to_all(
        jnp.broadcast_to(summed[None], (plane, share, bond)), ("z", "y"), 0, 0, tiled=True
    ).reshape(half, bond)
    whole = added[:8, bond : bond + 2] + added[:8, bond + 2 : bond + 4] + added[:8, bond + 4 : bond + 6]
    gathered = gathered.reshape(2, 192, bond)
    other = lax.ppermute(gathered, "core", swap)
    placed = place(0, where, gathered)
    projections = whole + lax.ppermute(whole, "core", swap)
    sigma = place(1, where, other, placed)
    return sigma, projections[0]


def solution(mesh):
    shape = dict(mesh.shape)
    ops = shape["ops"]
    parts = Mesh(mesh.devices.reshape(4, ops // 8, 2, shape["site"]), ("z", "y", "core", "site"))
    in_specs = (
        P(),
        P(OPS, "site", None, None),
        P(OPS, "site", None, None),
        P(),
        P(),
        P(OPS),
        P(),
        P(),
        P(None, "site", None, None),
    )
    out_specs = (P("site", None, None), P())
    return jax.shard_map(local, mesh=parts, in_specs=in_specs, out_specs=out_specs, check_vma=False)
```

```python
import functools

import jax
import jax.numpy as jnp
from jax import lax
from jax.experimental import pallas as pl
from jax.experimental.pallas import tpu as pltpu
from jax.sharding import Mesh
from jax.sharding import PartitionSpec as P


OPS = ("z", "y", "core")
CHUNK = 4
WIN_ROWS = 256
WIN_COLS = 384
SLOT_COLS = 256
GROUP_COLS = 4 * SLOT_COLS
EXTRA = 128

MY_START, MY_SIZE, RIGHT_START, RIGHT_SIZE = 0, 4, 8, 24
SITE, CORE, MEMBER = 0, 1, 2
DIAGONAL_ROWS = 32


def params():
    return pltpu.CompilerParams(vmem_limit_bytes=56 * 1024 * 1024)


def pack_one(blocks, slot, half, out, index, at=0):
    out[index + (at,)] = blocks[slot, 2 * half, :, :128]
    out[index + (at + 1,)] = blocks[slot, 2 * half + 1, :, :128]
    out[index + (at + 2,)] = jnp.concatenate(
        [blocks[slot, 2 * half, :, 128:192], blocks[slot, 2 * half + 1, :, 128:192]], axis=1
    )


def pack_early_body(blocks, first, second):
    for slot in range(2):
        pack_one(blocks, slot, 0, first, (slot,))
        pack_one(blocks, slot, 1, second, (slot,))


def pack_late_body(left, right, *outs):
    for k in range(4):

        @pl.when(pl.program_id(0) == k)
        def _():
            for half in range(2):
                pack_one(left, 0, half, outs[k], (), 3 * half)
                pack_one(right, 0, half, outs[k], (), 6 + 3 * half)


def pack_early(blocks):
    spec = pl.BlockSpec((2, 3, 192, 128), lambda i: (i, 0, 0, 0))
    shape = jax.ShapeDtypeStruct((CHUNK, 3, 192, 128), jnp.bfloat16)
    return pl.pallas_call(
        pack_early_body,
        grid=(2,),
        in_specs=[pl.BlockSpec((2, 4, 192, 192), lambda i: (i, 0, 0, 0))],
        out_specs=[spec, spec],
        out_shape=[shape, shape],
        name="pack_early",
    )(blocks)


def pack_late(left, right):
    block = pl.BlockSpec((1, 4, 192, 192), lambda i: (i + CHUNK, 0, 0, 0))
    return pl.pallas_call(
        pack_late_body,
        grid=(4,),
        in_specs=[block, block],
        out_specs=[pl.BlockSpec((12, 192, 128), lambda i: (0, 0, 0))] * 4,
        out_shape=[jax.ShapeDtypeStruct((12, 192, 128), jnp.bfloat16)] * 4,
        cost_estimate=pl.CostEstimate(flops=2 * 10**9, bytes_accessed=2**22, transcendentals=0),
        name="pack_late",
    )(left, right)


def select_body(where, left_sector, right_sector, left_energy, psi, table, rows, cols, energies, window, sems):
    group = pl.program_id(0)

    @pl.when(group == 0)
    def _():
        site = where[SITE]
        left_ids = left_sector[...]
        right_ids = right_sector[...]
        for within in range(4):
            sector = 4 * site + within
            table[MY_START + within] = jnp.sum((left_ids < sector).astype(jnp.int32))
            table[MY_SIZE + within] = jnp.sum((left_ids == sector).astype(jnp.int32))
        before = jnp.int32(0)
        for sector in range(16):
            size = jnp.sum((right_ids == sector).astype(jnp.int32))
            table[RIGHT_START + sector] = before
            table[RIGHT_SIZE + sector] = size
            before = before + size
        copies = []
        shifts = []
        for within in range(4):
            start = table[MY_START + within]
            base = pl.multiple_of(jnp.minimum((start // 16) * 16, psi.shape[0] - WIN_ROWS), 16)
            shifts.append(start - base)
            copies.append(
                pltpu.make_async_copy(psi.at[pl.ds(base, WIN_ROWS), :], window.at[within], sems.at[within])
            )
        for copy in copies:
            copy.start()
        row = lax.broadcasted_iota(jnp.int32, (192, WIN_ROWS), 0)
        col = lax.broadcasted_iota(jnp.int32, (192, WIN_ROWS), 1)
        wide_row = lax.broadcasted_iota(jnp.int32, (192, WIN_COLS), 0)
        wide_col = lax.broadcasted_iota(jnp.int32, (192, WIN_COLS), 1)
        for within in range(4):
            start = table[MY_START + within]
            size = table[MY_SIZE + within]
            base = pl.multiple_of(jnp.minimum((start // 128) * 128, psi.shape[0] - WIN_COLS), 128)
            kept = (wide_col == wide_row + (start - base)) & (wide_row < size)
            near = jnp.where(kept, left_energy[:, pl.ds(base, WIN_COLS)], 0.0)
            energies[pl.ds(within * 192, 192), :] = jnp.sum(near, axis=1, keepdims=True)
        for within in range(4):
            copies[within].wait()
            kept = (col == row + shifts[within]) & (row < table[MY_SIZE + within])
            pick = jnp.where(kept, 1.0, 0.0).astype(jnp.bfloat16)
            got = jnp.dot(pick, window[within], preferred_element_type=jnp.float32)
            rows[pl.ds(within * 192, 192), :] = got.astype(jnp.bfloat16)

    row = lax.broadcasted_iota(jnp.int32, (WIN_COLS, SLOT_COLS), 0)
    lane = lax.broadcasted_iota(jnp.int32, (WIN_COLS, SLOT_COLS), 1)
    for q in range(4):
        start = table[RIGHT_START + 4 * group + q]
        size = table[RIGHT_SIZE + 4 * group + q]
        base = pl.multiple_of(jnp.minimum((start // 128) * 128, rows.shape[1] - WIN_COLS), 128)
        if q % 2:
            at = jnp.where(lane < 128, lane, jnp.where(lane < 192, size, lane - 64))
        else:
            at = lane
        kept = (row == at + (start - base)) & (at < size)
        pick = jnp.where(kept, 1.0, 0.0).astype(jnp.bfloat16)
        got = jnp.dot(rows[:, pl.ds(base, WIN_COLS)], pick, preferred_element_type=jnp.float32)
        cols[0, :, q * SLOT_COLS : (q + 1) * SLOT_COLS] = got.astype(jnp.bfloat16)


def select(where, left_sector, right_sector, left_energy, psi):
    bond = psi.shape[1]
    smem = pl.BlockSpec(memory_space=pltpu.SMEM)
    ids = pl.BlockSpec((bond // 128, 128), lambda g: (0, 0))
    return pl.pallas_call(
        select_body,
        grid=(4,),
        in_specs=[smem, ids, ids, pl.BlockSpec((1, bond), lambda g: (0, 0)), pl.BlockSpec(memory_space=pltpu.HBM)],
        out_specs=[
            smem,
            pl.BlockSpec((768, bond), lambda g: (0, 0)),
            pl.BlockSpec((1, 768, GROUP_COLS), lambda g: (g, 0, 0)),
            pl.BlockSpec((768, 1), lambda g: (0, 0)),
        ],
        out_shape=[
            jax.ShapeDtypeStruct((40,), jnp.int32),
            jax.ShapeDtypeStruct((768, bond), jnp.bfloat16),
            jax.ShapeDtypeStruct((4, 768, GROUP_COLS), jnp.bfloat16),
            jax.ShapeDtypeStruct((768, 1), jnp.float32),
        ],
        scratch_shapes=[
            pltpu.VMEM((4, WIN_ROWS, bond), jnp.bfloat16),
            pltpu.SemaphoreType.DMA((4,)),
        ],
        compiler_params=params(),
        cost_estimate=pl.CostEstimate(flops=5 * 10**9, bytes_accessed=2**24, transcendentals=0),
        name="select",
    )(
        where,
        left_sector.reshape(bond // 128, 128),
        right_sector.reshape(bond // 128, 128),
        left_energy[None, :],
        psi,
    )


def multiply_slots(lefts, rights, psi, image, acc, last_live):
    count = len(lefts)
    for u in range(count):
        for within in range(4):
            got = jnp.dot(
                lefts[u](within), psi[within * 192 : (within + 1) * 192, :], preferred_element_type=jnp.float32
            )
            if u == 1:
                got = jnp.where(last_live, got, 0.0)
            image[u, within * 192 : (within + 1) * 192, :] = got.astype(jnp.bfloat16)
    for q in range(4):
        parts = None
        for u in range(count):
            block = jnp.concatenate([rights[u](q), jnp.zeros((64, 256), jnp.bfloat16)], axis=0)
            part = lax.dot_general(
                image[u, :, q * SLOT_COLS : (q + 1) * SLOT_COLS],
                block,
                (((1,), (1,)), ((), ())),
                preferred_element_type=jnp.float32,
            )
            parts = part if parts is None else parts + part
        acc[:, q * SLOT_COLS : (q + 1) * SLOT_COLS] += parts


def products_body(rels, where, count, left, psi, *refs):
    groups = len(rels)
    live = jnp.minimum(count[0], CHUNK)
    rights = [refs[2 * i : 2 * i + 2] for i in range(groups)]
    out, left_v, right_v, psi_v, image, acc_v, sem_left, sem_right, sem_psi, sem_out = refs[2 * groups :]
    site = where[SITE]
    left_copies = [
        pltpu.make_async_copy(left.at[pl.ds(2 * p, 2)], left_v.at[pl.ds(2 * p, 2)], sem_left.at[p])
        for p in range(2)
    ]
    copies = []
    for i in range(groups):
        copies.append(
            [
                pltpu.make_async_copy(rights[i][0], right_v.at[i, 0], sem_right.at[i, 0]),
                pltpu.make_async_copy(rights[i][1], right_v.at[i, 1], sem_right.at[i, 1]),
                pltpu.make_async_copy(psi.at[(site + rels[i]) % 4], psi_v.at[i], sem_psi.at[i]),
            ]
        )
    out_copies = [
        [
            pltpu.make_async_copy(
                acc_v.at[i, pl.ds(192 * w, 192)], out.at[i, pl.ds(192 * w, 192)], sem_out.at[i, w]
            )
            for w in range(4)
        ]
        for i in range(groups)
    ]
    for copy in left_copies + copies[0]:
        copy.start()
    acc_v[0] = jnp.zeros(acc_v.shape[1:], jnp.float32)
    for copy in left_copies:
        copy.wait()

    def one_group(i, carry):
        for j in range(groups):

            @pl.when(i == j)
            def _():
                for copy in copies[j]:
                    copy.wait()
                if j + 1 < groups:
                    for copy in copies[j + 1]:
                        copy.start()
                    acc_v[j + 1] = jnp.zeros(acc_v.shape[1:], jnp.float32)

        def one_pair(p, inner):
            lefts = [lambda within, u=u: left_v[2 * p + u, within] for u in range(2)]
            block = [
                lambda q, u=u: jnp.concatenate(
                    [right_v[i, q // 2, 2 * p + u, q % 2], right_v[i, q // 2, 2 * p + u, 2]], axis=1
                )
                for u in range(2)
            ]
            multiply_slots(lefts, block, psi_v.at[i], image, acc_v.at[i], 2 * p + 1 < live)
            return inner

        lax.fori_loop(0, (live + 1) // 2, one_pair, 0)
        for j in range(groups):

            @pl.when(i == j)
            def _():
                for copy in out_copies[j]:
                    copy.start()

        return carry

    lax.fori_loop(0, groups, one_group, 0)
    for found in out_copies:
        for copy in found:
            copy.wait()


def products(rels, where, count, left, psi, rights):
    groups = len(rels)
    smem = pl.BlockSpec(memory_space=pltpu.SMEM)
    hbm = pl.BlockSpec(memory_space=pltpu.HBM)
    flops = groups * 2 * 1024 * 768 * (192 + 256) * 4
    return pl.pallas_call(
        functools.partial(products_body, tuple(rels)),
        in_specs=[smem, smem, hbm, hbm] + [hbm] * (2 * groups),
        out_specs=hbm,
        out_shape=jax.ShapeDtypeStruct((groups, 768, GROUP_COLS), jnp.float32),
        scratch_shapes=[
            pltpu.VMEM((CHUNK, 4, 192, 192), jnp.bfloat16),
            pltpu.VMEM((groups, 2, CHUNK, 3, 192, 128), jnp.bfloat16),
            pltpu.VMEM((groups, 768, GROUP_COLS), jnp.bfloat16),
            pltpu.VMEM((2, 768, GROUP_COLS), jnp.bfloat16),
            pltpu.VMEM((groups, 768, GROUP_COLS), jnp.float32),
            pltpu.SemaphoreType.DMA((2,)),
            pltpu.SemaphoreType.DMA((groups, 2)),
            pltpu.SemaphoreType.DMA((groups,)),
            pltpu.SemaphoreType.DMA((groups, 4)),
        ],
        compiler_params=params(),
        cost_estimate=pl.CostEstimate(flops=flops, bytes_accessed=8 * 2**20, transcendentals=0),
        name="products",
    )(where, count, left, psi, *[half for halves in rights for half in halves])


def finish_body(slots, where, count, table, own, near, far_a, far_b, left, psi, *refs):
    live = jnp.minimum(count[0], CHUNK)
    rows, subspace, energies, right_energy = refs[:4]
    refs = list(refs[4:])
    if slots:
        counts, extras, moved = refs[:4], refs[4:8], refs[8:11]
        there = [counts[k][0] > CHUNK + k for k in range(4)]
        refs = refs[11:]
    send, mine, proj, left_v, right_v, psi_v, image, acc_v, rows_v, sub_v, total, staged, sums = refs[:13]
    sem_left, sem_right, sem_psi, sem_acc, sem_rows, sem_sub, sem_out = refs[13:20]
    width = subspace.shape[3]
    core = where[CORE]
    site = where[SITE]
    member = where[MEMBER]

    left_copies = [
        pltpu.make_async_copy(left.at[pl.ds(2 * p, 2)], left_v.at[pl.ds(2 * p, 2)], sem_left.at[p])
        for p in range(2)
    ]
    far_copies = [
        pltpu.make_async_copy(far_a, right_v.at[0], sem_right.at[0]),
        pltpu.make_async_copy(far_b, right_v.at[1], sem_right.at[1]),
    ]
    psi_copies = {
        i: pltpu.make_async_copy(psi.at[(site + i) % 4], psi_v.at[i], sem_psi.at[i])
        for i in ((2, 0, 1, 3) if slots else (2,))
    }
    acc_copies = [
        pltpu.make_async_copy(source, acc_v.at[rel], sem_acc.at[rel])
        for rel, source in ((0, own.at[0]), (1, near.at[0]), (3, near.at[1]))
    ]
    their = jnp.minimum(member, 768 // DIAGONAL_ROWS - 1)
    rows_copy = pltpu.make_async_copy(
        rows.at[pl.ds(pl.multiple_of(DIAGONAL_ROWS * their, DIAGONAL_ROWS), DIAGONAL_ROWS)],
        rows_v,
        sem_rows,
    )

    def sub_copies(step):
        within = 2 * ((1 - core) if step < 2 else core) + step % 2
        return [
            pltpu.make_async_copy(subspace.at[k, within], sub_v.at[step, k], sem_sub.at[step, k]) for k in range(2)
        ]

    for copy in left_copies + far_copies:
        copy.start()
    psi_copies[2].start()
    if slots:
        extra_v, moved_v, sem_extra, sem_moved = refs[20:]
        extra_copies = []
        taken = False
        for k in range(4):
            place = 0 if slots == 1 else k
            copy = pltpu.make_async_copy(extras[k], extra_v.at[place], sem_extra.at[place])
            extra_copies.append((there[k] & jnp.logical_not(taken) if slots == 1 else there[k], copy))
            taken = there[k] | taken
        moved_copies = [
            pltpu.make_async_copy(moved[i], moved_v.at[i + 1], sem_moved.at[i]) for i in range(3)
        ]
    acc_v[2] = jnp.zeros(acc_v.shape[1:], jnp.float32)
    for copy in left_copies + far_copies:
        copy.wait()
    psi_copies[2].wait()

    for copy in acc_copies:
        copy.start()
    if slots:
        for wanted, copy in extra_copies:

            @pl.when(wanted)
            def _():
                copy.start()

        for i in (0, 1, 3):
            psi_copies[i].start()
        for copy in moved_copies:
            copy.start()
    else:
        rows_copy.start()
        for step in range(4):
            for copy in sub_copies(step):
                copy.start()

    def one_pair(p, inner):
        lefts = [lambda within, u=u: left_v[2 * p + u, within] for u in range(2)]
        blocks = [
            lambda q, u=u: jnp.concatenate(
                [right_v[q // 2, 2 * p + u, q % 2], right_v[q // 2, 2 * p + u, 2]], axis=1
            )
            for u in range(2)
        ]
        multiply_slots(lefts, blocks, psi_v.at[2], image, acc_v.at[2], 2 * p + 1 < live)
        return inner

    lax.fori_loop(0, (live + 1) // 2, one_pair, 0)
    for copy in acc_copies:
        copy.wait()
    if slots:
        for wanted, copy in extra_copies:

            @pl.when(wanted)
            def _():
                copy.wait()

        for i in (0, 1, 3):
            psi_copies[i].wait()
        for copy in moved_copies:
            copy.wait()
        rows_copy.start()
        for step in range(4):
            for copy in sub_copies(step):
                copy.start()
        moved_v[0] = extra_v[:, 6:12]
        alive = [jnp.int32(1)] if slots == 1 else [one.astype(jnp.int32) for one in there]

        def one_group(i, carry):
            def one_slot(n, inner):
                wanted = alive[0]
                for k in range(1, slots):
                    wanted = jnp.where(n == k, alive[k], wanted)

                @pl.when(wanted > 0)
                def _():
                    def left_block(within):
                        at = 3 * (within // 2)
                        lane = 64 * (within % 2)
                        high = extra_v[n, at + 2]
                        return jnp.concatenate([extra_v[n, at + within % 2], high[:, lane : lane + 64]], axis=1)

                    def right_block(q):
                        at = 3 * (q // 2)
                        return jnp.concatenate([moved_v[i, n, at + q % 2], moved_v[i, n, at + 2]], axis=1)

                    multiply_slots([left_block], [right_block], psi_v.at[i], image, acc_v.at[i], None)

                return inner

            lax.fori_loop(0, slots, one_slot, 0)
            return carry

        lax.fori_loop(0, 4, one_group, 0)
    rows_copy.wait()

    lane = lax.broadcasted_iota(jnp.int32, (192, 128), 1)
    row = lax.broadcasted_iota(jnp.int32, (192, width), 0)
    sums[...] = jnp.zeros(sums.shape, jnp.float32)

    def out_copy(step):
        out = send if step < 2 else mine
        return pltpu.make_async_copy(staged.at[step], out.at[pl.ds(192 * (step % 2), 192)], sem_out.at[step])

    def one_block(step, carry):
        for j in range(4):

            @pl.when(step == j)
            def _():
                for copy in sub_copies(j):
                    copy.wait()

        within = 2 * jnp.where(step < 2, 1 - core, core) + step % 2
        here = pl.ds(pl.multiple_of(192 * within, 192), 192)

        def one_site(i, inner):
            rel = (i + 4 - site) % 4
            for q in range(4):
                start = table[RIGHT_START + 4 * i + q]
                base = pl.multiple_of((start // 128) * 128, 128)
                shift = start - base
                first = pltpu.roll(acc_v[rel, here, q * SLOT_COLS : q * SLOT_COLS + 128], shift, 1)
                second = pltpu.roll(acc_v[rel, here, q * SLOT_COLS + 128 : (q + 1) * SLOT_COLS], shift, 1)
                low = lane < shift
                total[:, pl.ds(base, 128)] = jnp.where(low, total[:, pl.ds(base, 128)], first)
                total[:, pl.ds(base + 128, 128)] = jnp.where(low, first, second)
                total[:, pl.ds(base + 256, 128)] = second
            return inner

        lax.fori_loop(0, 4, one_site, 0)
        per = 192 // DIAGONAL_ROWS

        @pl.when(member // per == within)
        def _():
            at = pl.multiple_of(DIAGONAL_ROWS * (member % per), DIAGONAL_ROWS)
            part = pl.ds(at, DIAGONAL_ROWS)
            energy = energies[pl.ds(pl.multiple_of(192 * within + at, DIAGONAL_ROWS), DIAGONAL_ROWS), :]
            total[part, :width] += (energy + right_energy[...]) * rows_v[...].astype(jnp.float32)

        kept = jnp.where(row < table[MY_SIZE + within], total[:, :width], 0.0)
        for k in range(2):
            part = sub_v[step, k].astype(jnp.float32) * kept
            sums[k] += jnp.sum(part.reshape(24, 8, width), axis=0)
        staged[step] = kept.astype(jnp.bfloat16)
        for j in range(4):

            @pl.when(step == j)
            def _():
                out_copy(j).start()

        return carry

    lax.fori_loop(0, 4, one_block, 0)
    for k in range(2):
        added = sums[k, :, :128]
        for j in range(1, width // 128):
            added = added + sums[k, :, 128 * j : 128 * (j + 1)]
        proj[k] = added
    for j in range(4):
        out_copy(j).wait()


def finish(slots, where, count, table, own, near, far, left, psi, rows, subspace, energies, right_energy, late=()):
    width = rows.shape[1]
    smem = pl.BlockSpec(memory_space=pltpu.SMEM)
    hbm = pl.BlockSpec(memory_space=pltpu.HBM)
    vmem = pl.BlockSpec(memory_space=pltpu.VMEM)
    half = jax.ShapeDtypeStruct((384, width), jnp.bfloat16)
    scratch = [
        pltpu.VMEM((CHUNK, 4, 192, 192), jnp.bfloat16),
        pltpu.VMEM((2, CHUNK, 3, 192, 128), jnp.bfloat16),
        pltpu.VMEM((4, 768, GROUP_COLS), jnp.bfloat16),
        pltpu.VMEM((2, 768, GROUP_COLS), jnp.bfloat16),
        pltpu.VMEM((4, 768, GROUP_COLS), jnp.float32),
        pltpu.VMEM((DIAGONAL_ROWS, width), jnp.bfloat16),
        pltpu.VMEM((4, 2, 192, width), jnp.bfloat16),
        pltpu.VMEM((192, width + 256), jnp.float32),
        pltpu.VMEM((4, 192, width), jnp.bfloat16),
        pltpu.VMEM((2, 8, width), jnp.float32),
        pltpu.SemaphoreType.DMA((2,)),
        pltpu.SemaphoreType.DMA((2,)),
        pltpu.SemaphoreType.DMA((4,)),
        pltpu.SemaphoreType.DMA((4,)),
        pltpu.SemaphoreType.DMA(()),
        pltpu.SemaphoreType.DMA((4, 2)),
        pltpu.SemaphoreType.DMA((4,)),
    ]
    if slots:
        scratch += [
            pltpu.VMEM((slots, 12, 192, 128), jnp.bfloat16),
            pltpu.VMEM((4, slots, 6, 192, 128), jnp.bfloat16),
            pltpu.SemaphoreType.DMA((4,)),
            pltpu.SemaphoreType.DMA((3,)),
        ]
    return pl.pallas_call(
        functools.partial(finish_body, slots),
        in_specs=[smem] * 3 + [hbm] * 8 + [vmem, vmem] + ([smem] * 4 + [hbm] * 7 if slots else []),
        out_specs=[hbm, hbm, vmem],
        out_shape=[half, half, jax.ShapeDtypeStruct((2, 8, 128), jnp.float32)],
        scratch_shapes=scratch,
        compiler_params=params(),
        cost_estimate=pl.CostEstimate(flops=8 * 10**9, bytes_accessed=30 * 2**20, transcendentals=0),
        name="finish",
    )(where, count, table, own, near, *far, left, psi, rows, subspace, energies, right_energy, *late)


def place_body(which, where, half, *rest):
    out, sems = rest[-2:]
    core = where[CORE] if which == 0 else 1 - where[CORE]
    copies = [
        pltpu.make_async_copy(
            half.at[n // 2, pl.ds(96 * (n % 2), 96)],
            out.at[2 * core + n // 2, pl.ds(96 * (n % 2), 96)],
            sems.at[n],
        )
        for n in range(4)
    ]
    for copy in copies:
        copy.start()
    for copy in copies:
        copy.wait()


def place(which, where, half, whole=None):
    hbm = pl.BlockSpec(memory_space=pltpu.HBM)
    args = (where, half) if whole is None else (where, half, whole)
    return pl.pallas_call(
        functools.partial(place_body, which),
        in_specs=[pl.BlockSpec(memory_space=pltpu.SMEM), pl.BlockSpec(memory_space=pltpu.VMEM)]
        + [hbm] * (len(args) - 2),
        out_specs=hbm,
        out_shape=jax.ShapeDtypeStruct((4,) + half.shape[1:], half.dtype),
        scratch_shapes=[pltpu.SemaphoreType.DMA((4,))],
        input_output_aliases={} if whole is None else {2: 0},
        cost_estimate=pl.CostEstimate(flops=10**9, bytes_accessed=2**22, transcendentals=0),
        name="place",
    )(*args)


def shifted(value, axis, by):
    size = lax.axis_size(axis)
    return lax.ppermute(value, axis, [(i, (i + by) % size) for i in range(size)])


def small_sum(value, axis):
    size = lax.axis_size(axis)
    me = lax.axis_index(axis)
    got = [value] + [shifted(value, axis, k) for k in range(1, size)]
    total = None
    for source in range(size):
        one = sum(jnp.where((me - source) % size == k, got[k], 0.0) for k in range(size))
        total = one if total is None else total + one
    return total


def local(
    wavefunction,
    left_blocks,
    right_blocks,
    left_sector,
    right_sector,
    term_count,
    left_energy,
    right_energy,
    subspace,
):
    bond = wavefunction.shape[0]
    site = lax.axis_index("site")
    core = lax.axis_index("core")
    mine_early = pack_early(right_blocks)
    prev = [shifted(half, "site", 1) for half in mine_early]
    following = [shifted(half, "site", -1) for half in mine_early]
    left_later, right_later, count_later, _ = lax.optimization_barrier(
        (left_blocks, right_blocks, term_count, mine_early[0])
    )

    ways = (("y", 1), ("y", -1), ("z", 1), ("z", -1))
    late = pack_late(left_later, right_later)
    extras = [shifted(late[k], axis, by) for k, (axis, by) in enumerate(ways)]
    counts = [shifted(count_later, axis, by) for axis, by in ways]
    there = [counts[k][0] > CHUNK + k for k in range(4)]
    number = sum(one.astype(jnp.int32) for one in there)

    where = jnp.stack([site, core, lax.axis_index(OPS)])
    table, rows, psi, energies = select(where, left_sector, right_sector, left_energy, wavefunction)
    own = products((0,), where, term_count, left_blocks, psi, [mine_early])

    far = (shifted(prev[0], "site", 1), shifted(following[1], "site", -1))
    going = extras[3][6:12]
    for k in (2, 1, 0):
        going = jnp.where(there[k], extras[k][6:12], going)
    moved = [shifted(going[None], "site", by) for by in (-1, 2, 1)]
    near = products((1, 3), where, term_count, left_blocks, psi, [following, prev])

    def rest(slots, late):
        return tuple(
            finish(
                slots,
                where,
                term_count,
                table,
                own,
                near,
                far,
                left_blocks,
                psi,
                rows,
                subspace,
                energies,
                right_energy[None, :],
                late=late,
            )
        )

    def none():
        return rest(0, [])

    def one():
        return rest(1, [*counts, *extras, *moved])

    def many():
        every = jnp.stack([one[6:12] for one in extras])
        return rest(4, [*counts, *extras] + [shifted(every, "site", by) for by in (-1, 2, 1)])

    send, mine, proj = lax.switch(jnp.minimum(number, 2), [none, one, many])
    swap = [(0, 1), (1, 0)]
    away = lax.ppermute(send, "core", swap)
    proj = small_sum(jnp.broadcast_to(jnp.sum(proj, axis=(1, 2))[None, :], (8, 2)), "site")[0]
    both = (mine.astype(jnp.float32) + away.astype(jnp.float32)).astype(jnp.bfloat16)

    high = lax.reduce_precision(proj, 8, 7)
    middle = lax.reduce_precision(proj - high, 8, 7)
    thirds = jnp.concatenate([high, middle, proj - high - middle]).astype(jnp.bfloat16)
    plane = lax.axis_size(("z", "y"))
    half = both.shape[0]
    share = half // plane
    extra = jnp.broadcast_to(jnp.pad(thirds, (0, EXTRA - 6))[None, :], (half, EXTRA))
    both = jnp.concatenate([both, extra], axis=1)

    pieces = lax.all_to_all(both.reshape(plane, share, bond + EXTRA), ("z", "y"), 0, 0, tiled=True)
    added = jnp.sum(pieces.astype(jnp.float32), axis=0)
    summed = added[:, :bond].astype(jnp.bfloat16)
    gathered = lax.all_to_all(
        jnp.broadcast_to(summed[None], (plane, share, bond)), ("z", "y"), 0, 0, tiled=True
    ).reshape(half, bond)
    whole = added[:8, bond : bond + 2] + added[:8, bond + 2 : bond + 4] + added[:8, bond + 4 : bond + 6]
    gathered = gathered.reshape(2, 192, bond)
    other = lax.ppermute(gathered, "core", swap)
    placed = place(0, where, gathered)
    whole_beside = lax.ppermute(whole, "core", swap)
    projections = whole + whole_beside
    sigma = place(1, where, other, placed)
    return sigma, projections[0]


def solution(mesh):
    shape = dict(mesh.shape)
    ops = shape["ops"]
    parts = Mesh(mesh.devices.reshape(4, ops // 8, 2, shape["site"]), ("z", "y", "core", "site"))
    in_specs = (
        P(),
        P(OPS, "site", None, None),
        P(OPS, "site", None, None),
        P(),
        P(),
        P(OPS),
        P(),
        P(),
        P(None, "site", None, None),
    )
    out_specs = (P("site", None, None), P())
    return jax.shard_map(local, mesh=parts, in_specs=in_specs, out_specs=out_specs, check_vma=False)
```

```python
import functools

import jax
import jax.numpy as jnp
from jax import lax
from jax.experimental import pallas as pl
from jax.experimental.pallas import tpu as pltpu
from jax.sharding import Mesh
from jax.sharding import PartitionSpec as P


OPS = ("z", "y", "core")
CHUNK = 4
WIN_ROWS = 256
WIN_COLS = 384
SLOT_COLS = 256
GROUP_COLS = 4 * SLOT_COLS
EXTRA = 128

MY_START, MY_SIZE, RIGHT_START, RIGHT_SIZE = 0, 4, 8, 24
SITE, CORE, MEMBER = 0, 1, 2
DIAGONAL_ROWS = 32


def params():
    return pltpu.CompilerParams(vmem_limit_bytes=56 * 1024 * 1024)


def pack_one(blocks, slot, half, out, index, at=0):
    out[index + (at,)] = blocks[slot, 2 * half, :, :128]
    out[index + (at + 1,)] = blocks[slot, 2 * half + 1, :, :128]
    out[index + (at + 2,)] = jnp.concatenate(
        [blocks[slot, 2 * half, :, 128:192], blocks[slot, 2 * half + 1, :, 128:192]], axis=1
    )


def pack_early_body(blocks, first, second):
    for slot in range(2):
        pack_one(blocks, slot, 0, first, (slot,))
        pack_one(blocks, slot, 1, second, (slot,))


def pack_late_body(count, left, right, *outs):
    for k in range(4):

        @pl.when(pl.program_id(0) == k)
        def _():
            for half in range(2):
                pack_one(left, 0, half, outs[k], (), 3 * half)
                pack_one(right, 0, half, outs[k], (), 6 + 3 * half)
            outs[k][12] = jnp.full((192, 128), count[0].astype(jnp.float32)).astype(jnp.bfloat16)


def pack_early(blocks):
    spec = pl.BlockSpec((2, 3, 192, 128), lambda i: (i, 0, 0, 0))
    shape = jax.ShapeDtypeStruct((CHUNK, 3, 192, 128), jnp.bfloat16)
    return pl.pallas_call(
        pack_early_body,
        grid=(2,),
        in_specs=[pl.BlockSpec((2, 4, 192, 192), lambda i: (i, 0, 0, 0))],
        out_specs=[spec, spec],
        out_shape=[shape, shape],
        name="pack_early",
    )(blocks)


def pack_late(count, left, right):
    block = pl.BlockSpec((1, 4, 192, 192), lambda i: (i + CHUNK, 0, 0, 0))
    return pl.pallas_call(
        pack_late_body,
        grid=(4,),
        in_specs=[pl.BlockSpec(memory_space=pltpu.SMEM), block, block],
        out_specs=[pl.BlockSpec((13, 192, 128), lambda i: (0, 0, 0))] * 4,
        out_shape=[jax.ShapeDtypeStruct((13, 192, 128), jnp.bfloat16)] * 4,
        cost_estimate=pl.CostEstimate(flops=2 * 10**9, bytes_accessed=2**22, transcendentals=0),
        name="pack_late",
    )(count, left, right)


def pick_body(*refs):
    extras = refs[:4]
    flags, going, tiles, sem_tile, sem_going = refs[4:]
    copies = [pltpu.make_async_copy(extras[k].at[12, pl.ds(0, 16)], tiles.at[k], sem_tile.at[k]) for k in range(4)]
    for copy in copies:
        copy.start()
    for copy in copies:
        copy.wait()
    number = jnp.int32(0)
    first = jnp.int32(3)
    for k in (3, 2, 1, 0):
        count = jnp.max(tiles[k].astype(jnp.float32)).astype(jnp.int32)
        there = count > CHUNK + k
        flags[k] = there.astype(jnp.int32)
        number = number + there.astype(jnp.int32)
        first = jnp.where(there, k, first)
    flags[4] = jnp.minimum(number, 2)
    flags[5] = first
    for k in range(4):

        @pl.when(first == k)
        def _():
            copy = pltpu.make_async_copy(extras[k].at[pl.ds(6, 6)], going.at[0], sem_going)
            copy.start()
            copy.wait()


def pick(extras):
    return pl.pallas_call(
        pick_body,
        in_specs=[pl.BlockSpec(memory_space=pltpu.HBM)] * 4,
        out_specs=[pl.BlockSpec(memory_space=pltpu.SMEM), pl.BlockSpec(memory_space=pltpu.VMEM)],
        out_shape=[jax.ShapeDtypeStruct((6,), jnp.int32), jax.ShapeDtypeStruct((1, 6, 192, 128), jnp.bfloat16)],
        scratch_shapes=[
            pltpu.VMEM((4, 16, 128), jnp.bfloat16),
            pltpu.SemaphoreType.DMA((4,)),
            pltpu.SemaphoreType.DMA(()),
        ],
        name="pick",
    )(*extras)


def select_body(where, left_sector, right_sector, left_energy, psi, table, rows, cols, energies, window, sems):
    group = pl.program_id(0)

    @pl.when(group == 0)
    def _():
        site = where[SITE]
        left_ids = left_sector[...]
        right_ids = right_sector[...]
        for within in range(4):
            sector = 4 * site + within
            table[MY_START + within] = jnp.sum((left_ids < sector).astype(jnp.int32))
            table[MY_SIZE + within] = jnp.sum((left_ids == sector).astype(jnp.int32))
        before = jnp.int32(0)
        for sector in range(16):
            size = jnp.sum((right_ids == sector).astype(jnp.int32))
            table[RIGHT_START + sector] = before
            table[RIGHT_SIZE + sector] = size
            before = before + size
        copies = []
        shifts = []
        for within in range(4):
            start = table[MY_START + within]
            base = pl.multiple_of(jnp.minimum((start // 16) * 16, psi.shape[0] - WIN_ROWS), 16)
            shifts.append(start - base)
            copies.append(
                pltpu.make_async_copy(psi.at[pl.ds(base, WIN_ROWS), :], window.at[within], sems.at[within])
            )
        for copy in copies:
            copy.start()
        row = lax.broadcasted_iota(jnp.int32, (192, WIN_ROWS), 0)
        col = lax.broadcasted_iota(jnp.int32, (192, WIN_ROWS), 1)
        wide_row = lax.broadcasted_iota(jnp.int32, (192, WIN_COLS), 0)
        wide_col = lax.broadcasted_iota(jnp.int32, (192, WIN_COLS), 1)
        for within in range(4):
            start = table[MY_START + within]
            size = table[MY_SIZE + within]
            base = pl.multiple_of(jnp.minimum((start // 128) * 128, psi.shape[0] - WIN_COLS), 128)
            kept = (wide_col == wide_row + (start - base)) & (wide_row < size)
            near = jnp.where(kept, left_energy[:, pl.ds(base, WIN_COLS)], 0.0)
            energies[pl.ds(within * 192, 192), :] = jnp.sum(near, axis=1, keepdims=True)
        for within in range(4):
            copies[within].wait()
            kept = (col == row + shifts[within]) & (row < table[MY_SIZE + within])
            pick = jnp.where(kept, 1.0, 0.0).astype(jnp.bfloat16)
            got = jnp.dot(pick, window[within], preferred_element_type=jnp.float32)
            rows[pl.ds(within * 192, 192), :] = got.astype(jnp.bfloat16)

    row = lax.broadcasted_iota(jnp.int32, (WIN_COLS, SLOT_COLS), 0)
    lane = lax.broadcasted_iota(jnp.int32, (WIN_COLS, SLOT_COLS), 1)
    for q in range(4):
        start = table[RIGHT_START + 4 * group + q]
        size = table[RIGHT_SIZE + 4 * group + q]
        base = pl.multiple_of(jnp.minimum((start // 128) * 128, rows.shape[1] - WIN_COLS), 128)
        if q % 2:
            at = jnp.where(lane < 128, lane, jnp.where(lane < 192, size, lane - 64))
        else:
            at = lane
        kept = (row == at + (start - base)) & (at < size)
        pick = jnp.where(kept, 1.0, 0.0).astype(jnp.bfloat16)
        got = jnp.dot(rows[:, pl.ds(base, WIN_COLS)], pick, preferred_element_type=jnp.float32)
        cols[0, :, q * SLOT_COLS : (q + 1) * SLOT_COLS] = got.astype(jnp.bfloat16)


def select(where, left_sector, right_sector, left_energy, psi):
    bond = psi.shape[1]
    smem = pl.BlockSpec(memory_space=pltpu.SMEM)
    ids = pl.BlockSpec((bond // 128, 128), lambda g: (0, 0))
    return pl.pallas_call(
        select_body,
        grid=(4,),
        in_specs=[smem, ids, ids, pl.BlockSpec((1, bond), lambda g: (0, 0)), pl.BlockSpec(memory_space=pltpu.HBM)],
        out_specs=[
            smem,
            pl.BlockSpec((768, bond), lambda g: (0, 0)),
            pl.BlockSpec((1, 768, GROUP_COLS), lambda g: (g, 0, 0)),
            pl.BlockSpec((768, 1), lambda g: (0, 0)),
        ],
        out_shape=[
            jax.ShapeDtypeStruct((40,), jnp.int32),
            jax.ShapeDtypeStruct((768, bond), jnp.bfloat16),
            jax.ShapeDtypeStruct((4, 768, GROUP_COLS), jnp.bfloat16),
            jax.ShapeDtypeStruct((768, 1), jnp.float32),
        ],
        scratch_shapes=[
            pltpu.VMEM((4, WIN_ROWS, bond), jnp.bfloat16),
            pltpu.SemaphoreType.DMA((4,)),
        ],
        compiler_params=params(),
        cost_estimate=pl.CostEstimate(flops=5 * 10**9, bytes_accessed=2**24, transcendentals=0),
        name="select",
    )(
        where,
        left_sector.reshape(bond // 128, 128),
        right_sector.reshape(bond // 128, 128),
        left_energy[None, :],
        psi,
    )


def multiply_slots(lefts, rights, psi, image, acc, last_live):
    count = len(lefts)
    for u in range(count):
        for within in range(4):
            got = jnp.dot(
                lefts[u](within), psi[within * 192 : (within + 1) * 192, :], preferred_element_type=jnp.float32
            )
            if u == 1:
                got = jnp.where(last_live, got, 0.0)
            image[u, within * 192 : (within + 1) * 192, :] = got.astype(jnp.bfloat16)
    for q in range(4):
        parts = None
        for u in range(count):
            block = jnp.concatenate([rights[u](q), jnp.zeros((64, 256), jnp.bfloat16)], axis=0)
            part = lax.dot_general(
                image[u, :, q * SLOT_COLS : (q + 1) * SLOT_COLS],
                block,
                (((1,), (1,)), ((), ())),
                preferred_element_type=jnp.float32,
            )
            parts = part if parts is None else parts + part
        acc[:, q * SLOT_COLS : (q + 1) * SLOT_COLS] += parts


def products_body(rels, where, count, left, psi, *refs):
    groups = len(rels)
    live = jnp.minimum(count[0], CHUNK)
    rights = [refs[2 * i : 2 * i + 2] for i in range(groups)]
    out, left_v, right_v, psi_v, image, acc_v, sem_left, sem_right, sem_psi, sem_out = refs[2 * groups :]
    site = where[SITE]
    left_copies = [
        pltpu.make_async_copy(left.at[pl.ds(2 * p, 2)], left_v.at[pl.ds(2 * p, 2)], sem_left.at[p])
        for p in range(2)
    ]
    copies = []
    for i in range(groups):
        copies.append(
            [
                pltpu.make_async_copy(rights[i][0], right_v.at[i, 0], sem_right.at[i, 0]),
                pltpu.make_async_copy(rights[i][1], right_v.at[i, 1], sem_right.at[i, 1]),
                pltpu.make_async_copy(psi.at[(site + rels[i]) % 4], psi_v.at[i], sem_psi.at[i]),
            ]
        )
    out_copies = [
        [
            pltpu.make_async_copy(
                acc_v.at[i, pl.ds(192 * w, 192)], out.at[i, pl.ds(192 * w, 192)], sem_out.at[i, w]
            )
            for w in range(4)
        ]
        for i in range(groups)
    ]
    for copy in left_copies + copies[0]:
        copy.start()
    acc_v[0] = jnp.zeros(acc_v.shape[1:], jnp.float32)
    for copy in left_copies:
        copy.wait()

    def one_group(i, carry):
        for j in range(groups):

            @pl.when(i == j)
            def _():
                for copy in copies[j]:
                    copy.wait()
                if j + 1 < groups:
                    for copy in copies[j + 1]:
                        copy.start()
                    acc_v[j + 1] = jnp.zeros(acc_v.shape[1:], jnp.float32)

        def one_pair(p, inner):
            lefts = [lambda within, u=u: left_v[2 * p + u, within] for u in range(2)]
            block = [
                lambda q, u=u: jnp.concatenate(
                    [right_v[i, q // 2, 2 * p + u, q % 2], right_v[i, q // 2, 2 * p + u, 2]], axis=1
                )
                for u in range(2)
            ]
            multiply_slots(lefts, block, psi_v.at[i], image, acc_v.at[i], 2 * p + 1 < live)
            return inner

        lax.fori_loop(0, (live + 1) // 2, one_pair, 0)
        for j in range(groups):

            @pl.when(i == j)
            def _():
                for copy in out_copies[j]:
                    copy.start()

        return carry

    lax.fori_loop(0, groups, one_group, 0)
    for found in out_copies:
        for copy in found:
            copy.wait()


def products(rels, where, count, left, psi, rights):
    groups = len(rels)
    smem = pl.BlockSpec(memory_space=pltpu.SMEM)
    hbm = pl.BlockSpec(memory_space=pltpu.HBM)
    flops = groups * 2 * 1024 * 768 * (192 + 256) * 4
    return pl.pallas_call(
        functools.partial(products_body, tuple(rels)),
        in_specs=[smem, smem, hbm, hbm] + [hbm] * (2 * groups),
        out_specs=hbm,
        out_shape=jax.ShapeDtypeStruct((groups, 768, GROUP_COLS), jnp.float32),
        scratch_shapes=[
            pltpu.VMEM((CHUNK, 4, 192, 192), jnp.bfloat16),
            pltpu.VMEM((groups, 2, CHUNK, 3, 192, 128), jnp.bfloat16),
            pltpu.VMEM((groups, 768, GROUP_COLS), jnp.bfloat16),
            pltpu.VMEM((2, 768, GROUP_COLS), jnp.bfloat16),
            pltpu.VMEM((groups, 768, GROUP_COLS), jnp.float32),
            pltpu.SemaphoreType.DMA((2,)),
            pltpu.SemaphoreType.DMA((groups, 2)),
            pltpu.SemaphoreType.DMA((groups,)),
            pltpu.SemaphoreType.DMA((groups, 4)),
        ],
        compiler_params=params(),
        cost_estimate=pl.CostEstimate(flops=flops, bytes_accessed=8 * 2**20, transcendentals=0),
        name="products",
    )(where, count, left, psi, *[half for halves in rights for half in halves])


def finish_body(slots, where, count, table, own, near, far_a, far_b, left, psi, *refs):
    live = jnp.minimum(count[0], CHUNK)
    rows, subspace, energies, right_energy = refs[:4]
    refs = list(refs[4:])
    if slots:
        flags, extras, moved = refs[0], refs[1:5], refs[5:8]
        there = [flags[k] > 0 for k in range(4)]
        refs = refs[8:]
    send, mine, proj, left_v, right_v, psi_v, image, acc_v, rows_v, sub_v, total, staged, sums = refs[:13]
    sem_left, sem_right, sem_psi, sem_acc, sem_rows, sem_sub, sem_out = refs[13:20]
    width = subspace.shape[3]
    core = where[CORE]
    site = where[SITE]
    member = where[MEMBER]

    left_copies = [
        pltpu.make_async_copy(left.at[pl.ds(2 * p, 2)], left_v.at[pl.ds(2 * p, 2)], sem_left.at[p])
        for p in range(2)
    ]
    far_copies = [
        pltpu.make_async_copy(far_a, right_v.at[0], sem_right.at[0]),
        pltpu.make_async_copy(far_b, right_v.at[1], sem_right.at[1]),
    ]
    psi_copies = {
        i: pltpu.make_async_copy(psi.at[(site + i) % 4], psi_v.at[i], sem_psi.at[i])
        for i in ((2, 0, 1, 3) if slots else (2,))
    }
    acc_copies = [
        pltpu.make_async_copy(source, acc_v.at[rel], sem_acc.at[rel])
        for rel, source in ((0, own.at[0]), (1, near.at[0]), (3, near.at[1]))
    ]
    their = jnp.minimum(member, 768 // DIAGONAL_ROWS - 1)
    rows_copy = pltpu.make_async_copy(
        rows.at[pl.ds(pl.multiple_of(DIAGONAL_ROWS * their, DIAGONAL_ROWS), DIAGONAL_ROWS)],
        rows_v,
        sem_rows,
    )

    def sub_copies(step):
        within = 2 * ((1 - core) if step < 2 else core) + step % 2
        return [
            pltpu.make_async_copy(subspace.at[k, within], sub_v.at[step, k], sem_sub.at[step, k]) for k in range(2)
        ]

    for copy in left_copies + far_copies:
        copy.start()
    psi_copies[2].start()
    if slots:
        extra_v, moved_v, sem_extra, sem_moved = refs[20:]
        extra_copies = []
        for k in range(4):
            place = 0 if slots == 1 else k
            source = extras[k].at[pl.ds(0, 12)]
            copy = pltpu.make_async_copy(source, extra_v.at[place], sem_extra.at[place])
            extra_copies.append((flags[5] == k if slots == 1 else there[k], copy))
        moved_copies = [
            pltpu.make_async_copy(moved[i], moved_v.at[i + 1], sem_moved.at[i]) for i in range(3)
        ]
    acc_v[2] = jnp.zeros(acc_v.shape[1:], jnp.float32)
    for copy in left_copies + far_copies:
        copy.wait()
    psi_copies[2].wait()

    for copy in acc_copies:
        copy.start()
    if slots:
        for wanted, copy in extra_copies:

            @pl.when(wanted)
            def _():
                copy.start()

        for i in (0, 1, 3):
            psi_copies[i].start()
        for copy in moved_copies:
            copy.start()
    else:
        rows_copy.start()
        for step in range(4):
            for copy in sub_copies(step):
                copy.start()

    def one_pair(p, inner):
        lefts = [lambda within, u=u: left_v[2 * p + u, within] for u in range(2)]
        blocks = [
            lambda q, u=u: jnp.concatenate(
                [right_v[q // 2, 2 * p + u, q % 2], right_v[q // 2, 2 * p + u, 2]], axis=1
            )
            for u in range(2)
        ]
        multiply_slots(lefts, blocks, psi_v.at[2], image, acc_v.at[2], 2 * p + 1 < live)
        return inner

    lax.fori_loop(0, (live + 1) // 2, one_pair, 0)
    for copy in acc_copies:
        copy.wait()
    if slots:
        for wanted, copy in extra_copies:

            @pl.when(wanted)
            def _():
                copy.wait()

        for i in (0, 1, 3):
            psi_copies[i].wait()
        for copy in moved_copies:
            copy.wait()
        rows_copy.start()
        for step in range(4):
            for copy in sub_copies(step):
                copy.start()
        moved_v[0] = extra_v[:, 6:12]
        alive = [jnp.int32(1)] if slots == 1 else [one.astype(jnp.int32) for one in there]

        def one_group(i, carry):
            def one_slot(n, inner):
                wanted = alive[0]
                for k in range(1, slots):
                    wanted = jnp.where(n == k, alive[k], wanted)

                @pl.when(wanted > 0)
                def _():
                    def left_block(within):
                        at = 3 * (within // 2)
                        lane = 64 * (within % 2)
                        high = extra_v[n, at + 2]
                        return jnp.concatenate([extra_v[n, at + within % 2], high[:, lane : lane + 64]], axis=1)

                    def right_block(q):
                        at = 3 * (q // 2)
                        return jnp.concatenate([moved_v[i, n, at + q % 2], moved_v[i, n, at + 2]], axis=1)

                    multiply_slots([left_block], [right_block], psi_v.at[i], image, acc_v.at[i], None)

                return inner

            lax.fori_loop(0, slots, one_slot, 0)
            return carry

        lax.fori_loop(0, 4, one_group, 0)
    rows_copy.wait()

    lane = lax.broadcasted_iota(jnp.int32, (192, 128), 1)
    row = lax.broadcasted_iota(jnp.int32, (192, width), 0)
    sums[...] = jnp.zeros(sums.shape, jnp.float32)

    def out_copy(step):
        out = send if step < 2 else mine
        return pltpu.make_async_copy(staged.at[step], out.at[pl.ds(192 * (step % 2), 192)], sem_out.at[step])

    def one_block(step, carry):
        for j in range(4):

            @pl.when(step == j)
            def _():
                for copy in sub_copies(j):
                    copy.wait()

        within = 2 * jnp.where(step < 2, 1 - core, core) + step % 2
        here = pl.ds(pl.multiple_of(192 * within, 192), 192)

        def one_site(i, inner):
            rel = (i + 4 - site) % 4
            for q in range(4):
                start = table[RIGHT_START + 4 * i + q]
                base = pl.multiple_of((start // 128) * 128, 128)
                shift = start - base
                first = pltpu.roll(acc_v[rel, here, q * SLOT_COLS : q * SLOT_COLS + 128], shift, 1)
                second = pltpu.roll(acc_v[rel, here, q * SLOT_COLS + 128 : (q + 1) * SLOT_COLS], shift, 1)
                low = lane < shift
                total[:, pl.ds(base, 128)] = jnp.where(low, total[:, pl.ds(base, 128)], first)
                total[:, pl.ds(base + 128, 128)] = jnp.where(low, first, second)
                total[:, pl.ds(base + 256, 128)] = second
            return inner

        lax.fori_loop(0, 4, one_site, 0)
        per = 192 // DIAGONAL_ROWS

        @pl.when(member // per == within)
        def _():
            at = pl.multiple_of(DIAGONAL_ROWS * (member % per), DIAGONAL_ROWS)
            part = pl.ds(at, DIAGONAL_ROWS)
            energy = energies[pl.ds(pl.multiple_of(192 * within + at, DIAGONAL_ROWS), DIAGONAL_ROWS), :]
            total[part, :width] += (energy + right_energy[...]) * rows_v[...].astype(jnp.float32)

        kept = jnp.where(row < table[MY_SIZE + within], total[:, :width], 0.0)
        for k in range(2):
            part = sub_v[step, k].astype(jnp.float32) * kept
            sums[k] += jnp.sum(part.reshape(24, 8, width), axis=0)
        staged[step] = kept.astype(jnp.bfloat16)
        for j in range(4):

            @pl.when(step == j)
            def _():
                out_copy(j).start()

        return carry

    lax.fori_loop(0, 4, one_block, 0)
    for k in range(2):
        added = sums[k, :, :128]
        for j in range(1, width // 128):
            added = added + sums[k, :, 128 * j : 128 * (j + 1)]
        proj[k] = added
    for j in range(4):
        out_copy(j).wait()


def finish(slots, where, count, table, own, near, far, left, psi, rows, subspace, energies, right_energy, late=()):
    width = rows.shape[1]
    smem = pl.BlockSpec(memory_space=pltpu.SMEM)
    hbm = pl.BlockSpec(memory_space=pltpu.HBM)
    vmem = pl.BlockSpec(memory_space=pltpu.VMEM)
    half = jax.ShapeDtypeStruct((384, width), jnp.bfloat16)
    scratch = [
        pltpu.VMEM((CHUNK, 4, 192, 192), jnp.bfloat16),
        pltpu.VMEM((2, CHUNK, 3, 192, 128), jnp.bfloat16),
        pltpu.VMEM((4, 768, GROUP_COLS), jnp.bfloat16),
        pltpu.VMEM((2, 768, GROUP_COLS), jnp.bfloat16),
        pltpu.VMEM((4, 768, GROUP_COLS), jnp.float32),
        pltpu.VMEM((DIAGONAL_ROWS, width), jnp.bfloat16),
        pltpu.VMEM((4, 2, 192, width), jnp.bfloat16),
        pltpu.VMEM((192, width + 256), jnp.float32),
        pltpu.VMEM((4, 192, width), jnp.bfloat16),
        pltpu.VMEM((2, 8, width), jnp.float32),
        pltpu.SemaphoreType.DMA((2,)),
        pltpu.SemaphoreType.DMA((2,)),
        pltpu.SemaphoreType.DMA((4,)),
        pltpu.SemaphoreType.DMA((4,)),
        pltpu.SemaphoreType.DMA(()),
        pltpu.SemaphoreType.DMA((4, 2)),
        pltpu.SemaphoreType.DMA((4,)),
    ]
    if slots:
        scratch += [
            pltpu.VMEM((slots, 12, 192, 128), jnp.bfloat16),
            pltpu.VMEM((4, slots, 6, 192, 128), jnp.bfloat16),
            pltpu.SemaphoreType.DMA((4,)),
            pltpu.SemaphoreType.DMA((3,)),
        ]
    return pl.pallas_call(
        functools.partial(finish_body, slots),
        in_specs=[smem] * 3 + [hbm] * 8 + [vmem, vmem] + ([smem] + [hbm] * 7 if slots else []),
        out_specs=[hbm, hbm, vmem],
        out_shape=[half, half, jax.ShapeDtypeStruct((2, 8, 128), jnp.float32)],
        scratch_shapes=scratch,
        compiler_params=params(),
        cost_estimate=pl.CostEstimate(flops=8 * 10**9, bytes_accessed=30 * 2**20, transcendentals=0),
        name="finish",
    )(where, count, table, own, near, *far, left, psi, rows, subspace, energies, right_energy, *late)


def place_body(which, where, half, *rest):
    out, sems = rest[-2:]
    core = where[CORE] if which == 0 else 1 - where[CORE]
    copies = [
        pltpu.make_async_copy(
            half.at[n // 2, pl.ds(96 * (n % 2), 96)],
            out.at[2 * core + n // 2, pl.ds(96 * (n % 2), 96)],
            sems.at[n],
        )
        for n in range(4)
    ]
    for copy in copies:
        copy.start()
    for copy in copies:
        copy.wait()


def place(which, where, half, whole=None):
    hbm = pl.BlockSpec(memory_space=pltpu.HBM)
    args = (where, half) if whole is None else (where, half, whole)
    return pl.pallas_call(
        functools.partial(place_body, which),
        in_specs=[pl.BlockSpec(memory_space=pltpu.SMEM), pl.BlockSpec(memory_space=pltpu.VMEM)]
        + [hbm] * (len(args) - 2),
        out_specs=hbm,
        out_shape=jax.ShapeDtypeStruct((4,) + half.shape[1:], half.dtype),
        scratch_shapes=[pltpu.SemaphoreType.DMA((4,))],
        input_output_aliases={} if whole is None else {2: 0},
        cost_estimate=pl.CostEstimate(flops=10**9, bytes_accessed=2**22, transcendentals=0),
        name="place",
    )(*args)


def shifted(value, axis, by):
    size = lax.axis_size(axis)
    return lax.ppermute(value, axis, [(i, (i + by) % size) for i in range(size)])


def small_sum(value, axis):
    size = lax.axis_size(axis)
    me = lax.axis_index(axis)
    got = [value] + [shifted(value, axis, k) for k in range(1, size)]
    total = None
    for source in range(size):
        one = sum(jnp.where((me - source) % size == k, got[k], 0.0) for k in range(size))
        total = one if total is None else total + one
    return total


def local(
    wavefunction,
    left_blocks,
    right_blocks,
    left_sector,
    right_sector,
    term_count,
    left_energy,
    right_energy,
    subspace,
):
    bond = wavefunction.shape[0]
    site = lax.axis_index("site")
    core = lax.axis_index("core")
    mine_early = pack_early(right_blocks)
    prev = [shifted(half, "site", 1) for half in mine_early]
    following = [shifted(half, "site", -1) for half in mine_early]
    left_later, right_later, _ = lax.optimization_barrier((left_blocks, right_blocks, mine_early[0]))

    ways = (("y", 1), ("y", -1), ("z", 1), ("z", -1))
    late = pack_late(term_count, left_later, right_later)
    extras = [shifted(late[k], axis, by) for k, (axis, by) in enumerate(ways)]
    flags, going = pick(extras)

    where = jnp.stack([site, core, lax.axis_index(OPS)])
    table, rows, psi, energies = select(where, left_sector, right_sector, left_energy, wavefunction)
    own = products((0,), where, term_count, left_blocks, psi, [mine_early])

    far = (shifted(prev[0], "site", 1), shifted(following[1], "site", -1))
    moved = [shifted(going, "site", by) for by in (-1, 2, 1)]
    near = products((1, 3), where, term_count, left_blocks, psi, [following, prev])

    def rest(slots, late):
        return tuple(
            finish(
                slots,
                where,
                term_count,
                table,
                own,
                near,
                far,
                left_blocks,
                psi,
                rows,
                subspace,
                energies,
                right_energy[None, :],
                late=late,
            )
        )

    def none():
        return rest(0, [])

    def one():
        return rest(1, [flags, *extras, *moved])

    def many():
        every = jnp.stack([one[6:12] for one in extras])
        return rest(4, [flags, *extras] + [shifted(every, "site", by) for by in (-1, 2, 1)])

    send, mine, proj = lax.switch(flags[4], [none, one, many])
    swap = [(0, 1), (1, 0)]
    away = lax.ppermute(send, "core", swap)
    proj = small_sum(jnp.broadcast_to(jnp.sum(proj, axis=(1, 2))[None, :], (8, 2)), "site")[0]
    both = (mine.astype(jnp.float32) + away.astype(jnp.float32)).astype(jnp.bfloat16)

    high = lax.reduce_precision(proj, 8, 7)
    middle = lax.reduce_precision(proj - high, 8, 7)
    thirds = jnp.concatenate([high, middle, proj - high - middle]).astype(jnp.bfloat16)
    plane = lax.axis_size(("z", "y"))
    half = both.shape[0]
    share = half // plane
    extra = jnp.broadcast_to(jnp.pad(thirds, (0, EXTRA - 6))[None, :], (half, EXTRA))
    both = jnp.concatenate([both, extra], axis=1)

    pieces = lax.all_to_all(both.reshape(plane, share, bond + EXTRA), ("z", "y"), 0, 0, tiled=True)
    added = jnp.sum(pieces.astype(jnp.float32), axis=0)
    summed = added[:, :bond].astype(jnp.bfloat16)
    gathered = lax.all_to_all(
        jnp.broadcast_to(summed[None], (plane, share, bond)), ("z", "y"), 0, 0, tiled=True
    ).reshape(half, bond)
    whole = added[:8, bond : bond + 2] + added[:8, bond + 2 : bond + 4] + added[:8, bond + 4 : bond + 6]
    gathered = gathered.reshape(2, 192, bond)
    other = lax.ppermute(gathered, "core", swap)
    placed = place(0, where, gathered)
    whole_beside = lax.ppermute(whole, "core", swap)
    projections = whole + whole_beside
    sigma = place(1, where, other, placed)
    return sigma, projections[0]


def solution(mesh):
    shape = dict(mesh.shape)
    ops = shape["ops"]
    parts = Mesh(mesh.devices.reshape(4, ops // 8, 2, shape["site"]), ("z", "y", "core", "site"))
    in_specs = (
        P(),
        P(OPS, "site", None, None),
        P(OPS, "site", None, None),
        P(),
        P(),
        P(OPS),
        P(),
        P(),
        P(None, "site", None, None),
    )
    out_specs = (P("site", None, None), P())
    return jax.shard_map(local, mesh=parts, in_specs=in_specs, out_specs=out_specs, check_vma=False)
```

```python
import functools

import jax
import jax.numpy as jnp
from jax import lax
from jax.experimental import pallas as pl
from jax.experimental.pallas import tpu as pltpu
from jax.sharding import Mesh
from jax.sharding import PartitionSpec as P


OPS = ("z", "y", "core")
CHUNK = 4
WIN_ROWS = 256
WIN_COLS = 384
SLOT_COLS = 256
GROUP_COLS = 4 * SLOT_COLS
EXTRA = 128

MY_START, MY_SIZE, RIGHT_START, RIGHT_SIZE = 0, 4, 8, 24
SITE, CORE, MEMBER = 0, 1, 2
DIAGONAL_ROWS = 32


def params():
    return pltpu.CompilerParams(vmem_limit_bytes=56 * 1024 * 1024)


def pack_one(blocks, slot, half, out, index, at=0):
    out[index + (at,)] = blocks[slot, 2 * half, :, :128]
    out[index + (at + 1,)] = blocks[slot, 2 * half + 1, :, :128]
    out[index + (at + 2,)] = jnp.concatenate(
        [blocks[slot, 2 * half, :, 128:192], blocks[slot, 2 * half + 1, :, 128:192]], axis=1
    )


def pack_early_body(blocks, first, second):
    for slot in range(2):
        pack_one(blocks, slot, 0, first, (slot,))
        pack_one(blocks, slot, 1, second, (slot,))


def pack_late_body(count, left, right, *outs):
    for k in range(4):

        @pl.when(pl.program_id(0) == k)
        def _():
            for half in range(2):
                pack_one(left, 0, half, outs[k], (), 3 * half)
                pack_one(right, 0, half, outs[k], (), 6 + 3 * half)
            outs[k][12] = jnp.full((192, 128), count[0].astype(jnp.float32)).astype(jnp.bfloat16)


def pack_early(blocks):
    spec = pl.BlockSpec((2, 3, 192, 128), lambda i: (i, 0, 0, 0))
    shape = jax.ShapeDtypeStruct((CHUNK, 3, 192, 128), jnp.bfloat16)
    return pl.pallas_call(
        pack_early_body,
        grid=(2,),
        in_specs=[pl.BlockSpec((2, 4, 192, 192), lambda i: (i, 0, 0, 0))],
        out_specs=[spec, spec],
        out_shape=[shape, shape],
        name="pack_early",
    )(blocks)


def pack_late(count, left, right):
    block = pl.BlockSpec((1, 4, 192, 192), lambda i: (i + CHUNK, 0, 0, 0))
    return pl.pallas_call(
        pack_late_body,
        grid=(4,),
        in_specs=[pl.BlockSpec(memory_space=pltpu.SMEM), block, block],
        out_specs=[pl.BlockSpec((13, 192, 128), lambda i: (0, 0, 0))] * 4,
        out_shape=[jax.ShapeDtypeStruct((13, 192, 128), jnp.bfloat16)] * 4,
        cost_estimate=pl.CostEstimate(flops=2 * 10**9, bytes_accessed=2**22, transcendentals=0),
        name="pack_late",
    )(count, left, right)


def pick_body(*refs):
    extras = refs[:4]
    flags, branch, going, tiles, sem_tile, sem_going = refs[4:]
    copies = [pltpu.make_async_copy(extras[k].at[12, pl.ds(0, 16)], tiles.at[k], sem_tile.at[k]) for k in range(4)]
    for copy in copies:
        copy.start()
    for copy in copies:
        copy.wait()
    number = jnp.int32(0)
    first = jnp.int32(3)
    for k in (3, 2, 1, 0):
        count = jnp.max(tiles[k].astype(jnp.float32)).astype(jnp.int32)
        there = count > CHUNK + k
        flags[k] = there.astype(jnp.int32)
        number = number + there.astype(jnp.int32)
        first = jnp.where(there, k, first)
    flags[4] = first
    branch[0] = jnp.minimum(number, 2)
    for k in range(4):

        @pl.when(first == k)
        def _():
            copy = pltpu.make_async_copy(extras[k].at[pl.ds(6, 6)], going.at[0], sem_going)
            copy.start()
            copy.wait()


def pick(extras):
    return pl.pallas_call(
        pick_body,
        in_specs=[pl.BlockSpec(memory_space=pltpu.HBM)] * 4,
        out_specs=[pl.BlockSpec(memory_space=pltpu.SMEM)] * 2 + [pl.BlockSpec(memory_space=pltpu.VMEM)],
        out_shape=[jax.ShapeDtypeStruct((5,), jnp.int32), jax.ShapeDtypeStruct((1,), jnp.int32), jax.ShapeDtypeStruct((1, 6, 192, 128), jnp.bfloat16)],
        scratch_shapes=[
            pltpu.VMEM((4, 16, 128), jnp.bfloat16),
            pltpu.SemaphoreType.DMA((4,)),
            pltpu.SemaphoreType.DMA(()),
        ],
        name="pick",
    )(*extras)


def select_body(where, left_sector, right_sector, left_energy, psi, table, rows, cols, energies, window, sems):
    group = pl.program_id(0)

    @pl.when(group == 0)
    def _():
        site = where[SITE]
        left_ids = left_sector[...]
        right_ids = right_sector[...]
        for within in range(4):
            sector = 4 * site + within
            table[MY_START + within] = jnp.sum((left_ids < sector).astype(jnp.int32))
            table[MY_SIZE + within] = jnp.sum((left_ids == sector).astype(jnp.int32))
        before = jnp.int32(0)
        for sector in range(16):
            size = jnp.sum((right_ids == sector).astype(jnp.int32))
            table[RIGHT_START + sector] = before
            table[RIGHT_SIZE + sector] = size
            before = before + size
        copies = []
        shifts = []
        for within in range(4):
            start = table[MY_START + within]
            base = pl.multiple_of(jnp.minimum((start // 16) * 16, psi.shape[0] - WIN_ROWS), 16)
            shifts.append(start - base)
            copies.append(
                pltpu.make_async_copy(psi.at[pl.ds(base, WIN_ROWS), :], window.at[within], sems.at[within])
            )
        for copy in copies:
            copy.start()
        row = lax.broadcasted_iota(jnp.int32, (192, WIN_ROWS), 0)
        col = lax.broadcasted_iota(jnp.int32, (192, WIN_ROWS), 1)
        wide_row = lax.broadcasted_iota(jnp.int32, (192, WIN_COLS), 0)
        wide_col = lax.broadcasted_iota(jnp.int32, (192, WIN_COLS), 1)
        for within in range(4):
            start = table[MY_START + within]
            size = table[MY_SIZE + within]
            base = pl.multiple_of(jnp.minimum((start // 128) * 128, psi.shape[0] - WIN_COLS), 128)
            kept = (wide_col == wide_row + (start - base)) & (wide_row < size)
            near = jnp.where(kept, left_energy[:, pl.ds(base, WIN_COLS)], 0.0)
            energies[pl.ds(within * 192, 192), :] = jnp.sum(near, axis=1, keepdims=True)
        for within in range(4):
            copies[within].wait()
            kept = (col == row + shifts[within]) & (row < table[MY_SIZE + within])
            pick = jnp.where(kept, 1.0, 0.0).astype(jnp.bfloat16)
            got = jnp.dot(pick, window[within], preferred_element_type=jnp.float32)
            rows[pl.ds(within * 192, 192), :] = got.astype(jnp.bfloat16)

    row = lax.broadcasted_iota(jnp.int32, (WIN_COLS, SLOT_COLS), 0)
    lane = lax.broadcasted_iota(jnp.int32, (WIN_COLS, SLOT_COLS), 1)
    for q in range(4):
        start = table[RIGHT_START + 4 * group + q]
        size = table[RIGHT_SIZE + 4 * group + q]
        base = pl.multiple_of(jnp.minimum((start // 128) * 128, rows.shape[1] - WIN_COLS), 128)
        if q % 2:
            at = jnp.where(lane < 128, lane, jnp.where(lane < 192, size, lane - 64))
        else:
            at = lane
        kept = (row == at + (start - base)) & (at < size)
        pick = jnp.where(kept, 1.0, 0.0).astype(jnp.bfloat16)
        got = jnp.dot(rows[:, pl.ds(base, WIN_COLS)], pick, preferred_element_type=jnp.float32)
        cols[0, :, q * SLOT_COLS : (q + 1) * SLOT_COLS] = got.astype(jnp.bfloat16)


def select(where, left_sector, right_sector, left_energy, psi):
    bond = psi.shape[1]
    smem = pl.BlockSpec(memory_space=pltpu.SMEM)
    ids = pl.BlockSpec((bond // 128, 128), lambda g: (0, 0))
    return pl.pallas_call(
        select_body,
        grid=(4,),
        in_specs=[smem, ids, ids, pl.BlockSpec((1, bond), lambda g: (0, 0)), pl.BlockSpec(memory_space=pltpu.HBM)],
        out_specs=[
            smem,
            pl.BlockSpec((768, bond), lambda g: (0, 0)),
            pl.BlockSpec((1, 768, GROUP_COLS), lambda g: (g, 0, 0)),
            pl.BlockSpec((768, 1), lambda g: (0, 0)),
        ],
        out_shape=[
            jax.ShapeDtypeStruct((40,), jnp.int32),
            jax.ShapeDtypeStruct((768, bond), jnp.bfloat16),
            jax.ShapeDtypeStruct((4, 768, GROUP_COLS), jnp.bfloat16),
            jax.ShapeDtypeStruct((768, 1), jnp.float32),
        ],
        scratch_shapes=[
            pltpu.VMEM((4, WIN_ROWS, bond), jnp.bfloat16),
            pltpu.SemaphoreType.DMA((4,)),
        ],
        compiler_params=params(),
        cost_estimate=pl.CostEstimate(flops=5 * 10**9, bytes_accessed=2**24, transcendentals=0),
        name="select",
    )(
        where,
        left_sector.reshape(bond // 128, 128),
        right_sector.reshape(bond // 128, 128),
        left_energy[None, :],
        psi,
    )


def multiply_slots(lefts, rights, psi, image, acc, last_live):
    count = len(lefts)
    for u in range(count):
        for within in range(4):
            got = jnp.dot(
                lefts[u](within), psi[within * 192 : (within + 1) * 192, :], preferred_element_type=jnp.float32
            )
            if u == 1:
                got = jnp.where(last_live, got, 0.0)
            image[u, within * 192 : (within + 1) * 192, :] = got.astype(jnp.bfloat16)
    for q in range(4):
        parts = None
        for u in range(count):
            block = jnp.concatenate([rights[u](q), jnp.zeros((64, 256), jnp.bfloat16)], axis=0)
            part = lax.dot_general(
                image[u, :, q * SLOT_COLS : (q + 1) * SLOT_COLS],
                block,
                (((1,), (1,)), ((), ())),
                preferred_element_type=jnp.float32,
            )
            parts = part if parts is None else parts + part
        acc[:, q * SLOT_COLS : (q + 1) * SLOT_COLS] += parts


def products_body(rels, where, count, left, psi, *refs):
    groups = len(rels)
    live = jnp.minimum(count[0], CHUNK)
    rights = [refs[2 * i : 2 * i + 2] for i in range(groups)]
    out, left_v, right_v, psi_v, image, acc_v, sem_left, sem_right, sem_psi, sem_out = refs[2 * groups :]
    site = where[SITE]
    left_copies = [
        pltpu.make_async_copy(left.at[pl.ds(2 * p, 2)], left_v.at[pl.ds(2 * p, 2)], sem_left.at[p])
        for p in range(2)
    ]
    copies = []
    for i in range(groups):
        copies.append(
            [
                pltpu.make_async_copy(rights[i][0], right_v.at[i, 0], sem_right.at[i, 0]),
                pltpu.make_async_copy(rights[i][1], right_v.at[i, 1], sem_right.at[i, 1]),
                pltpu.make_async_copy(psi.at[(site + rels[i]) % 4], psi_v.at[i], sem_psi.at[i]),
            ]
        )
    out_copies = [
        [
            pltpu.make_async_copy(
                acc_v.at[i, pl.ds(192 * w, 192)], out.at[i, pl.ds(192 * w, 192)], sem_out.at[i, w]
            )
            for w in range(4)
        ]
        for i in range(groups)
    ]
    for copy in left_copies + copies[0]:
        copy.start()
    acc_v[0] = jnp.zeros(acc_v.shape[1:], jnp.float32)
    for copy in left_copies:
        copy.wait()

    def one_group(i, carry):
        for j in range(groups):

            @pl.when(i == j)
            def _():
                for copy in copies[j]:
                    copy.wait()
                if j + 1 < groups:
                    for copy in copies[j + 1]:
                        copy.start()
                    acc_v[j + 1] = jnp.zeros(acc_v.shape[1:], jnp.float32)

        def one_pair(p, inner):
            lefts = [lambda within, u=u: left_v[2 * p + u, within] for u in range(2)]
            block = [
                lambda q, u=u: jnp.concatenate(
                    [right_v[i, q // 2, 2 * p + u, q % 2], right_v[i, q // 2, 2 * p + u, 2]], axis=1
                )
                for u in range(2)
            ]
            multiply_slots(lefts, block, psi_v.at[i], image, acc_v.at[i], 2 * p + 1 < live)
            return inner

        lax.fori_loop(0, (live + 1) // 2, one_pair, 0)
        for j in range(groups):

            @pl.when(i == j)
            def _():
                for copy in out_copies[j]:
                    copy.start()

        return carry

    lax.fori_loop(0, groups, one_group, 0)
    for found in out_copies:
        for copy in found:
            copy.wait()


def products(rels, where, count, left, psi, rights):
    groups = len(rels)
    smem = pl.BlockSpec(memory_space=pltpu.SMEM)
    hbm = pl.BlockSpec(memory_space=pltpu.HBM)
    flops = groups * 2 * 1024 * 768 * (192 + 256) * 4
    return pl.pallas_call(
        functools.partial(products_body, tuple(rels)),
        in_specs=[smem, smem, hbm, hbm] + [hbm] * (2 * groups),
        out_specs=hbm,
        out_shape=jax.ShapeDtypeStruct((groups, 768, GROUP_COLS), jnp.float32),
        scratch_shapes=[
            pltpu.VMEM((CHUNK, 4, 192, 192), jnp.bfloat16),
            pltpu.VMEM((groups, 2, CHUNK, 3, 192, 128), jnp.bfloat16),
            pltpu.VMEM((groups, 768, GROUP_COLS), jnp.bfloat16),
            pltpu.VMEM((2, 768, GROUP_COLS), jnp.bfloat16),
            pltpu.VMEM((groups, 768, GROUP_COLS), jnp.float32),
            pltpu.SemaphoreType.DMA((2,)),
            pltpu.SemaphoreType.DMA((groups, 2)),
            pltpu.SemaphoreType.DMA((groups,)),
            pltpu.SemaphoreType.DMA((groups, 4)),
        ],
        compiler_params=params(),
        cost_estimate=pl.CostEstimate(flops=flops, bytes_accessed=8 * 2**20, transcendentals=0),
        name="products",
    )(where, count, left, psi, *[half for halves in rights for half in halves])


def finish_body(slots, where, count, table, own, near, far_a, far_b, left, psi, *refs):
    live = jnp.minimum(count[0], CHUNK)
    rows, subspace, energies, right_energy = refs[:4]
    refs = list(refs[4:])
    if slots:
        flags, extras, moved = refs[0], refs[1:5], refs[5:8]
        there = [flags[k] > 0 for k in range(4)]
        refs = refs[8:]
    send, mine, proj, left_v, right_v, psi_v, image, acc_v, rows_v, sub_v, total, staged, sums = refs[:13]
    sem_left, sem_right, sem_psi, sem_acc, sem_rows, sem_sub, sem_out = refs[13:20]
    width = subspace.shape[3]
    core = where[CORE]
    site = where[SITE]
    member = where[MEMBER]

    left_copies = [
        pltpu.make_async_copy(left.at[pl.ds(2 * p, 2)], left_v.at[pl.ds(2 * p, 2)], sem_left.at[p])
        for p in range(2)
    ]
    far_copies = [
        pltpu.make_async_copy(far_a, right_v.at[0], sem_right.at[0]),
        pltpu.make_async_copy(far_b, right_v.at[1], sem_right.at[1]),
    ]
    psi_copies = {
        i: pltpu.make_async_copy(psi.at[(site + i) % 4], psi_v.at[i], sem_psi.at[i])
        for i in ((2, 0, 1, 3) if slots else (2,))
    }
    acc_copies = [
        pltpu.make_async_copy(source, acc_v.at[rel], sem_acc.at[rel])
        for rel, source in ((0, own.at[0]), (1, near.at[0]), (3, near.at[1]))
    ]
    their = jnp.minimum(member, 768 // DIAGONAL_ROWS - 1)
    rows_copy = pltpu.make_async_copy(
        rows.at[pl.ds(pl.multiple_of(DIAGONAL_ROWS * their, DIAGONAL_ROWS), DIAGONAL_ROWS)],
        rows_v,
        sem_rows,
    )

    def sub_copies(step):
        within = 2 * ((1 - core) if step < 2 else core) + step % 2
        return [
            pltpu.make_async_copy(subspace.at[k, within], sub_v.at[step, k], sem_sub.at[step, k]) for k in range(2)
        ]

    for copy in left_copies + far_copies:
        copy.start()
    psi_copies[2].start()
    if slots:
        extra_v, moved_v, sem_extra, sem_moved = refs[20:]
        extra_copies = []
        for k in range(4):
            place = 0 if slots == 1 else k
            source = extras[k].at[pl.ds(0, 12)]
            copy = pltpu.make_async_copy(source, extra_v.at[place], sem_extra.at[place])
            extra_copies.append((flags[4] == k if slots == 1 else there[k], copy))
        moved_copies = [
            pltpu.make_async_copy(moved[i], moved_v.at[i + 1], sem_moved.at[i]) for i in range(3)
        ]
    acc_v[2] = jnp.zeros(acc_v.shape[1:], jnp.float32)
    for copy in left_copies + far_copies:
        copy.wait()
    psi_copies[2].wait()

    for copy in acc_copies:
        copy.start()
    if slots:
        for wanted, copy in extra_copies:

            @pl.when(wanted)
            def _():
                copy.start()

        for i in (0, 1, 3):
            psi_copies[i].start()
        for copy in moved_copies:
            copy.start()
    else:
        rows_copy.start()
        for step in range(4):
            for copy in sub_copies(step):
                copy.start()

    def one_pair(p, inner):
        lefts = [lambda within, u=u: left_v[2 * p + u, within] for u in range(2)]
        blocks = [
            lambda q, u=u: jnp.concatenate(
                [right_v[q // 2, 2 * p + u, q % 2], right_v[q // 2, 2 * p + u, 2]], axis=1
            )
            for u in range(2)
        ]
        multiply_slots(lefts, blocks, psi_v.at[2], image, acc_v.at[2], 2 * p + 1 < live)
        return inner

    lax.fori_loop(0, (live + 1) // 2, one_pair, 0)
    for copy in acc_copies:
        copy.wait()
    if slots:
        for wanted, copy in extra_copies:

            @pl.when(wanted)
            def _():
                copy.wait()

        for i in (0, 1, 3):
            psi_copies[i].wait()
        for copy in moved_copies:
            copy.wait()
        rows_copy.start()
        for step in range(4):
            for copy in sub_copies(step):
                copy.start()
        moved_v[0] = extra_v[:, 6:12]
        alive = [jnp.int32(1)] if slots == 1 else [one.astype(jnp.int32) for one in there]

        def one_group(i, carry):
            def one_slot(n, inner):
                wanted = alive[0]
                for k in range(1, slots):
                    wanted = jnp.where(n == k, alive[k], wanted)

                @pl.when(wanted > 0)
                def _():
                    def left_block(within):
                        at = 3 * (within // 2)
                        lane = 64 * (within % 2)
                        high = extra_v[n, at + 2]
                        return jnp.concatenate([extra_v[n, at + within % 2], high[:, lane : lane + 64]], axis=1)

                    def right_block(q):
                        at = 3 * (q // 2)
                        return jnp.concatenate([moved_v[i, n, at + q % 2], moved_v[i, n, at + 2]], axis=1)

                    multiply_slots([left_block], [right_block], psi_v.at[i], image, acc_v.at[i], None)

                return inner

            lax.fori_loop(0, slots, one_slot, 0)
            return carry

        lax.fori_loop(0, 4, one_group, 0)
    rows_copy.wait()

    lane = lax.broadcasted_iota(jnp.int32, (192, 128), 1)
    row = lax.broadcasted_iota(jnp.int32, (192, width), 0)
    sums[...] = jnp.zeros(sums.shape, jnp.float32)

    def out_copy(step):
        out = send if step < 2 else mine
        return pltpu.make_async_copy(staged.at[step], out.at[pl.ds(192 * (step % 2), 192)], sem_out.at[step])

    def one_block(step, carry):
        for j in range(4):

            @pl.when(step == j)
            def _():
                for copy in sub_copies(j):
                    copy.wait()

        within = 2 * jnp.where(step < 2, 1 - core, core) + step % 2
        here = pl.ds(pl.multiple_of(192 * within, 192), 192)

        def one_site(i, inner):
            rel = (i + 4 - site) % 4
            for q in range(4):
                start = table[RIGHT_START + 4 * i + q]
                base = pl.multiple_of((start // 128) * 128, 128)
                shift = start - base
                first = pltpu.roll(acc_v[rel, here, q * SLOT_COLS : q * SLOT_COLS + 128], shift, 1)
                second = pltpu.roll(acc_v[rel, here, q * SLOT_COLS + 128 : (q + 1) * SLOT_COLS], shift, 1)
                low = lane < shift
                total[:, pl.ds(base, 128)] = jnp.where(low, total[:, pl.ds(base, 128)], first)
                total[:, pl.ds(base + 128, 128)] = jnp.where(low, first, second)
                total[:, pl.ds(base + 256, 128)] = second
            return inner

        lax.fori_loop(0, 4, one_site, 0)
        per = 192 // DIAGONAL_ROWS

        @pl.when(member // per == within)
        def _():
            at = pl.multiple_of(DIAGONAL_ROWS * (member % per), DIAGONAL_ROWS)
            part = pl.ds(at, DIAGONAL_ROWS)
            energy = energies[pl.ds(pl.multiple_of(192 * within + at, DIAGONAL_ROWS), DIAGONAL_ROWS), :]
            total[part, :width] += (energy + right_energy[...]) * rows_v[...].astype(jnp.float32)

        kept = jnp.where(row < table[MY_SIZE + within], total[:, :width], 0.0)
        for k in range(2):
            part = sub_v[step, k].astype(jnp.float32) * kept
            sums[k] += jnp.sum(part.reshape(24, 8, width), axis=0)
        staged[step] = kept.astype(jnp.bfloat16)
        for j in range(4):

            @pl.when(step == j)
            def _():
                out_copy(j).start()

        return carry

    lax.fori_loop(0, 4, one_block, 0)
    for k in range(2):
        added = sums[k, :, :128]
        for j in range(1, width // 128):
            added = added + sums[k, :, 128 * j : 128 * (j + 1)]
        proj[k] = added
    for j in range(4):
        out_copy(j).wait()


def finish(slots, where, count, table, own, near, far, left, psi, rows, subspace, energies, right_energy, late=()):
    width = rows.shape[1]
    smem = pl.BlockSpec(memory_space=pltpu.SMEM)
    hbm = pl.BlockSpec(memory_space=pltpu.HBM)
    vmem = pl.BlockSpec(memory_space=pltpu.VMEM)
    half = jax.ShapeDtypeStruct((384, width), jnp.bfloat16)
    scratch = [
        pltpu.VMEM((CHUNK, 4, 192, 192), jnp.bfloat16),
        pltpu.VMEM((2, CHUNK, 3, 192, 128), jnp.bfloat16),
        pltpu.VMEM((4, 768, GROUP_COLS), jnp.bfloat16),
        pltpu.VMEM((2, 768, GROUP_COLS), jnp.bfloat16),
        pltpu.VMEM((4, 768, GROUP_COLS), jnp.float32),
        pltpu.VMEM((DIAGONAL_ROWS, width), jnp.bfloat16),
        pltpu.VMEM((4, 2, 192, width), jnp.bfloat16),
        pltpu.VMEM((192, width + 256), jnp.float32),
        pltpu.VMEM((4, 192, width), jnp.bfloat16),
        pltpu.VMEM((2, 8, width), jnp.float32),
        pltpu.SemaphoreType.DMA((2,)),
        pltpu.SemaphoreType.DMA((2,)),
        pltpu.SemaphoreType.DMA((4,)),
        pltpu.SemaphoreType.DMA((4,)),
        pltpu.SemaphoreType.DMA(()),
        pltpu.SemaphoreType.DMA((4, 2)),
        pltpu.SemaphoreType.DMA((4,)),
    ]
    if slots:
        scratch += [
            pltpu.VMEM((slots, 12, 192, 128), jnp.bfloat16),
            pltpu.VMEM((4, slots, 6, 192, 128), jnp.bfloat16),
            pltpu.SemaphoreType.DMA((4,)),
            pltpu.SemaphoreType.DMA((3,)),
        ]
    return pl.pallas_call(
        functools.partial(finish_body, slots),
        in_specs=[smem] * 3 + [hbm] * 8 + [vmem, vmem] + ([smem] + [hbm] * 7 if slots else []),
        out_specs=[hbm, hbm, vmem],
        out_shape=[half, half, jax.ShapeDtypeStruct((2, 8, 128), jnp.float32)],
        scratch_shapes=scratch,
        compiler_params=params(),
        cost_estimate=pl.CostEstimate(flops=8 * 10**9, bytes_accessed=30 * 2**20, transcendentals=0),
        name="finish",
    )(where, count, table, own, near, *far, left, psi, rows, subspace, energies, right_energy, *late)


def place_body(which, where, half, *rest):
    out, sems = rest[-2:]
    core = where[CORE] if which == 0 else 1 - where[CORE]
    copies = [
        pltpu.make_async_copy(
            half.at[n // 2, pl.ds(96 * (n % 2), 96)],
            out.at[2 * core + n // 2, pl.ds(96 * (n % 2), 96)],
            sems.at[n],
        )
        for n in range(4)
    ]
    for copy in copies:
        copy.start()
    for copy in copies:
        copy.wait()


def place(which, where, half, whole=None):
    hbm = pl.BlockSpec(memory_space=pltpu.HBM)
    args = (where, half) if whole is None else (where, half, whole)
    return pl.pallas_call(
        functools.partial(place_body, which),
        in_specs=[pl.BlockSpec(memory_space=pltpu.SMEM), pl.BlockSpec(memory_space=pltpu.VMEM)]
        + [hbm] * (len(args) - 2),
        out_specs=hbm,
        out_shape=jax.ShapeDtypeStruct((4,) + half.shape[1:], half.dtype),
        scratch_shapes=[pltpu.SemaphoreType.DMA((4,))],
        input_output_aliases={} if whole is None else {2: 0},
        cost_estimate=pl.CostEstimate(flops=10**9, bytes_accessed=2**22, transcendentals=0),
        name="place",
    )(*args)


def shifted(value, axis, by):
    size = lax.axis_size(axis)
    return lax.ppermute(value, axis, [(i, (i + by) % size) for i in range(size)])


def small_sum(value, axis):
    size = lax.axis_size(axis)
    me = lax.axis_index(axis)
    got = [value] + [shifted(value, axis, k) for k in range(1, size)]
    total = None
    for source in range(size):
        one = sum(jnp.where((me - source) % size == k, got[k], 0.0) for k in range(size))
        total = one if total is None else total + one
    return total


def local(
    wavefunction,
    left_blocks,
    right_blocks,
    left_sector,
    right_sector,
    term_count,
    left_energy,
    right_energy,
    subspace,
):
    bond = wavefunction.shape[0]
    site = lax.axis_index("site")
    core = lax.axis_index("core")
    mine_early = pack_early(right_blocks)
    prev_first = shifted(mine_early[0], "site", 1)
    next_second = shifted(mine_early[1], "site", -1)
    second_after, first_after, _, _ = lax.optimization_barrier((mine_early[1], mine_early[0], left_blocks, term_count))
    prev = [prev_first, shifted(second_after, "site", 1)]
    following = [shifted(first_after, "site", -1), next_second]
    left_later, right_later, _ = lax.optimization_barrier((left_blocks, right_blocks, mine_early[0]))

    ways = (("y", 1), ("y", -1), ("z", 1), ("z", -1))
    late = pack_late(term_count, left_later, right_later)
    extras = [shifted(late[k], axis, by) for k, (axis, by) in enumerate(ways)]
    flags, branch, going = pick(extras)

    where = jnp.stack([site, core, lax.axis_index(OPS)])
    table, rows, psi, energies = select(where, left_sector, right_sector, left_energy, wavefunction)
    own = products((0,), where, term_count, left_blocks, psi, [mine_early])

    far = (shifted(prev[0], "site", 1), shifted(following[1], "site", -1))
    moved = [shifted(going, "site", by) for by in (-1, 2, 1)]
    near = products((1, 3), where, term_count, left_blocks, psi, [following, prev])

    def rest(slots, late):
        return tuple(
            finish(
                slots,
                where,
                term_count,
                table,
                own,
                near,
                far,
                left_blocks,
                psi,
                rows,
                subspace,
                energies,
                right_energy[None, :],
                late=late,
            )
        )

    def none():
        return rest(0, [])

    def one():
        return rest(1, [flags, *extras, *moved])

    def many():
        every = jnp.stack([one[6:12] for one in extras])
        return rest(4, [flags, *extras] + [shifted(every, "site", by) for by in (-1, 2, 1)])

    send, mine, proj = lax.switch(branch[0], [none, one, many])
    swap = [(0, 1), (1, 0)]
    away = lax.ppermute(send, "core", swap)
    proj = small_sum(jnp.broadcast_to(jnp.sum(proj, axis=(1, 2))[None, :], (8, 2)), "site")[0]
    both = (mine.astype(jnp.float32) + away.astype(jnp.float32)).astype(jnp.bfloat16)

    high = lax.reduce_precision(proj, 8, 7)
    middle = lax.reduce_precision(proj - high, 8, 7)
    thirds = jnp.concatenate([high, middle, proj - high - middle]).astype(jnp.bfloat16)
    plane = lax.axis_size(("z", "y"))
    half = both.shape[0]
    share = half // plane
    extra = jnp.broadcast_to(jnp.pad(thirds, (0, EXTRA - 6))[None, :], (half, EXTRA))
    both = jnp.concatenate([both, extra], axis=1)

    pieces = lax.all_to_all(both.reshape(plane, share, bond + EXTRA), ("z", "y"), 0, 0, tiled=True)
    added = jnp.sum(pieces.astype(jnp.float32), axis=0)
    summed = added[:, :bond].astype(jnp.bfloat16)
    gathered = lax.all_to_all(
        jnp.broadcast_to(summed[None], (plane, share, bond)), ("z", "y"), 0, 0, tiled=True
    ).reshape(half, bond)
    whole = added[:8, bond : bond + 2] + added[:8, bond + 2 : bond + 4] + added[:8, bond + 4 : bond + 6]
    gathered = gathered.reshape(2, 192, bond)
    other = lax.ppermute(gathered, "core", swap)
    placed = place(0, where, gathered)
    whole_beside = lax.ppermute(whole, "core", swap)
    projections = whole + whole_beside
    sigma = place(1, where, other, placed)
    return sigma, projections[0]


def solution(mesh):
    shape = dict(mesh.shape)
    ops = shape["ops"]
    parts = Mesh(mesh.devices.reshape(4, ops // 8, 2, shape["site"]), ("z", "y", "core", "site"))
    in_specs = (
        P(),
        P(OPS, "site", None, None),
        P(OPS, "site", None, None),
        P(),
        P(),
        P(OPS),
        P(),
        P(),
        P(None, "site", None, None),
    )
    out_specs = (P("site", None, None), P())
    return jax.shard_map(local, mesh=parts, in_specs=in_specs, out_specs=out_specs, check_vma=False)
```

```python
import functools

import jax
import jax.numpy as jnp
from jax import lax
from jax.experimental import pallas as pl
from jax.experimental.pallas import tpu as pltpu
from jax.sharding import Mesh
from jax.sharding import PartitionSpec as P


OPS = ("z", "y", "core")
CHUNK = 4
WIN_ROWS = 256
WIN_COLS = 384
SLOT_COLS = 256
GROUP_COLS = 4 * SLOT_COLS
EXTRA = 128

MY_START, MY_SIZE, RIGHT_START, RIGHT_SIZE = 0, 4, 8, 24
SITE, CORE, MEMBER = 0, 1, 2
DIAGONAL_ROWS = 32


def params():
    return pltpu.CompilerParams(vmem_limit_bytes=56 * 1024 * 1024)


def pack_one(blocks, slot, half, out, index, at=0):
    out[index + (at,)] = blocks[slot, 2 * half, :, :128]
    out[index + (at + 1,)] = blocks[slot, 2 * half + 1, :, :128]
    out[index + (at + 2,)] = jnp.concatenate(
        [blocks[slot, 2 * half, :, 128:192], blocks[slot, 2 * half + 1, :, 128:192]], axis=1
    )


def pack_early_body(blocks, first, second):
    for slot in range(2):
        pack_one(blocks, slot, 0, first, (slot,))
        pack_one(blocks, slot, 1, second, (slot,))


def pack_late_body(count, left, right, *outs):
    for k in range(4):

        @pl.when(pl.program_id(0) == k)
        def _():
            for half in range(2):
                pack_one(left, 0, half, outs[k], (), 3 * half)
                pack_one(right, 0, half, outs[k], (), 6 + 3 * half)
            outs[k][12] = jnp.full((192, 128), count[0].astype(jnp.float32)).astype(jnp.bfloat16)


def pack_early(blocks):
    spec = pl.BlockSpec((2, 3, 192, 128), lambda i: (i, 0, 0, 0))
    shape = jax.ShapeDtypeStruct((CHUNK, 3, 192, 128), jnp.bfloat16)
    return pl.pallas_call(
        pack_early_body,
        grid=(2,),
        in_specs=[pl.BlockSpec((2, 4, 192, 192), lambda i: (i, 0, 0, 0))],
        out_specs=[spec, spec],
        out_shape=[shape, shape],
        name="pack_early",
    )(blocks)


def pack_late(count, left, right):
    block = pl.BlockSpec((1, 4, 192, 192), lambda i: (i + CHUNK, 0, 0, 0))
    return pl.pallas_call(
        pack_late_body,
        grid=(4,),
        in_specs=[pl.BlockSpec(memory_space=pltpu.SMEM), block, block],
        out_specs=[pl.BlockSpec((13, 192, 128), lambda i: (0, 0, 0))] * 4,
        out_shape=[jax.ShapeDtypeStruct((13, 192, 128), jnp.bfloat16)] * 4,
        cost_estimate=pl.CostEstimate(flops=2 * 10**9, bytes_accessed=2**22, transcendentals=0),
        name="pack_late",
    )(count, left, right)


def pick_body(*refs):
    extras = refs[:4]
    flags, branch, going, tiles, sem_tile, sem_going = refs[4:]
    copies = [pltpu.make_async_copy(extras[k].at[12, pl.ds(0, 16)], tiles.at[k], sem_tile.at[k]) for k in range(4)]
    for copy in copies:
        copy.start()
    for copy in copies:
        copy.wait()
    number = jnp.int32(0)
    first = jnp.int32(3)
    for k in (3, 2, 1, 0):
        count = jnp.max(tiles[k].astype(jnp.float32)).astype(jnp.int32)
        there = count > CHUNK + k
        flags[k] = there.astype(jnp.int32)
        number = number + there.astype(jnp.int32)
        first = jnp.where(there, k, first)
    flags[4] = first
    branch[0] = jnp.minimum(number, 2)
    for k in range(4):

        @pl.when(first == k)
        def _():
            copy = pltpu.make_async_copy(extras[k].at[pl.ds(6, 6)], going.at[0], sem_going)
            copy.start()
            copy.wait()


def pick(extras):
    return pl.pallas_call(
        pick_body,
        in_specs=[pl.BlockSpec(memory_space=pltpu.HBM)] * 4,
        out_specs=[pl.BlockSpec(memory_space=pltpu.SMEM)] * 2 + [pl.BlockSpec(memory_space=pltpu.VMEM)],
        out_shape=[jax.ShapeDtypeStruct((5,), jnp.int32), jax.ShapeDtypeStruct((1,), jnp.int32), jax.ShapeDtypeStruct((1, 6, 192, 128), jnp.bfloat16)],
        scratch_shapes=[
            pltpu.VMEM((4, 16, 128), jnp.bfloat16),
            pltpu.SemaphoreType.DMA((4,)),
            pltpu.SemaphoreType.DMA(()),
        ],
        name="pick",
    )(*extras)


def select_body(where, left_sector, right_sector, left_energy, psi, table, rows, cols, energies, window, sems):
    group = pl.program_id(0)

    @pl.when(group == 0)
    def _():
        site = where[SITE]
        left_ids = left_sector[...]
        right_ids = right_sector[...]
        for within in range(4):
            sector = 4 * site + within
            table[MY_START + within] = jnp.sum((left_ids < sector).astype(jnp.int32))
            table[MY_SIZE + within] = jnp.sum((left_ids == sector).astype(jnp.int32))
        before = jnp.int32(0)
        for sector in range(16):
            size = jnp.sum((right_ids == sector).astype(jnp.int32))
            table[RIGHT_START + sector] = before
            table[RIGHT_SIZE + sector] = size
            before = before + size
        copies = []
        shifts = []
        for within in range(4):
            start = table[MY_START + within]
            base = pl.multiple_of(jnp.minimum((start // 16) * 16, psi.shape[0] - WIN_ROWS), 16)
            shifts.append(start - base)
            copies.append(
                pltpu.make_async_copy(psi.at[pl.ds(base, WIN_ROWS), :], window.at[within], sems.at[within])
            )
        for copy in copies:
            copy.start()
        row = lax.broadcasted_iota(jnp.int32, (192, WIN_ROWS), 0)
        col = lax.broadcasted_iota(jnp.int32, (192, WIN_ROWS), 1)
        wide_row = lax.broadcasted_iota(jnp.int32, (192, WIN_COLS), 0)
        wide_col = lax.broadcasted_iota(jnp.int32, (192, WIN_COLS), 1)
        for within in range(4):
            start = table[MY_START + within]
            size = table[MY_SIZE + within]
            base = pl.multiple_of(jnp.minimum((start // 128) * 128, psi.shape[0] - WIN_COLS), 128)
            kept = (wide_col == wide_row + (start - base)) & (wide_row < size)
            near = jnp.where(kept, left_energy[:, pl.ds(base, WIN_COLS)], 0.0)
            energies[pl.ds(within * 192, 192), :] = jnp.sum(near, axis=1, keepdims=True)
        for within in range(4):
            copies[within].wait()
            kept = (col == row + shifts[within]) & (row < table[MY_SIZE + within])
            pick = jnp.where(kept, 1.0, 0.0).astype(jnp.bfloat16)
            got = jnp.dot(pick, window[within], preferred_element_type=jnp.float32)
            rows[pl.ds(within * 192, 192), :] = got.astype(jnp.bfloat16)

    row = lax.broadcasted_iota(jnp.int32, (WIN_COLS, SLOT_COLS), 0)
    lane = lax.broadcasted_iota(jnp.int32, (WIN_COLS, SLOT_COLS), 1)
    for q in range(4):
        start = table[RIGHT_START + 4 * group + q]
        size = table[RIGHT_SIZE + 4 * group + q]
        base = pl.multiple_of(jnp.minimum((start // 128) * 128, rows.shape[1] - WIN_COLS), 128)
        if q % 2:
            at = jnp.where(lane < 128, lane, jnp.where(lane < 192, size, lane - 64))
        else:
            at = lane
        kept = (row == at + (start - base)) & (at < size)
        pick = jnp.where(kept, 1.0, 0.0).astype(jnp.bfloat16)
        got = jnp.dot(rows[:, pl.ds(base, WIN_COLS)], pick, preferred_element_type=jnp.float32)
        cols[0, :, q * SLOT_COLS : (q + 1) * SLOT_COLS] = got.astype(jnp.bfloat16)


def select(where, left_sector, right_sector, left_energy, psi):
    bond = psi.shape[1]
    smem = pl.BlockSpec(memory_space=pltpu.SMEM)
    ids = pl.BlockSpec((bond // 128, 128), lambda g: (0, 0))
    return pl.pallas_call(
        select_body,
        grid=(4,),
        in_specs=[smem, ids, ids, pl.BlockSpec((1, bond), lambda g: (0, 0)), pl.BlockSpec(memory_space=pltpu.HBM)],
        out_specs=[
            smem,
            pl.BlockSpec((768, bond), lambda g: (0, 0)),
            pl.BlockSpec((1, 768, GROUP_COLS), lambda g: (g, 0, 0)),
            pl.BlockSpec((768, 1), lambda g: (0, 0)),
        ],
        out_shape=[
            jax.ShapeDtypeStruct((40,), jnp.int32),
            jax.ShapeDtypeStruct((768, bond), jnp.bfloat16),
            jax.ShapeDtypeStruct((4, 768, GROUP_COLS), jnp.bfloat16),
            jax.ShapeDtypeStruct((768, 1), jnp.float32),
        ],
        scratch_shapes=[
            pltpu.VMEM((4, WIN_ROWS, bond), jnp.bfloat16),
            pltpu.SemaphoreType.DMA((4,)),
        ],
        compiler_params=params(),
        cost_estimate=pl.CostEstimate(flops=5 * 10**9, bytes_accessed=2**24, transcendentals=0),
        name="select",
    )(
        where,
        left_sector.reshape(bond // 128, 128),
        right_sector.reshape(bond // 128, 128),
        left_energy[None, :],
        psi,
    )


def multiply_slots(lefts, rights, psi, image, acc, last_live):
    count = len(lefts)
    for u in range(count):
        for within in range(4):
            got = jnp.dot(
                lefts[u](within), psi[within * 192 : (within + 1) * 192, :], preferred_element_type=jnp.float32
            )
            if u == 1:
                got = jnp.where(last_live, got, 0.0)
            image[u, within * 192 : (within + 1) * 192, :] = got.astype(jnp.bfloat16)
    for q in range(4):
        parts = None
        for u in range(count):
            block = jnp.concatenate([rights[u](q), jnp.zeros((64, 256), jnp.bfloat16)], axis=0)
            part = lax.dot_general(
                image[u, :, q * SLOT_COLS : (q + 1) * SLOT_COLS],
                block,
                (((1,), (1,)), ((), ())),
                preferred_element_type=jnp.float32,
            )
            parts = part if parts is None else parts + part
        acc[:, q * SLOT_COLS : (q + 1) * SLOT_COLS] += parts


def products_body(rels, where, count, left, psi, *refs):
    groups = len(rels)
    live = jnp.minimum(count[0], CHUNK)
    rights = [refs[2 * i : 2 * i + 2] for i in range(groups)]
    out, left_v, right_v, psi_v, image, acc_v, sem_left, sem_right, sem_psi, sem_out = refs[2 * groups :]
    site = where[SITE]
    left_copies = [
        pltpu.make_async_copy(left.at[pl.ds(2 * p, 2)], left_v.at[pl.ds(2 * p, 2)], sem_left.at[p])
        for p in range(2)
    ]
    copies = []
    for i in range(groups):
        copies.append(
            [
                pltpu.make_async_copy(rights[i][0], right_v.at[i, 0], sem_right.at[i, 0]),
                pltpu.make_async_copy(rights[i][1], right_v.at[i, 1], sem_right.at[i, 1]),
                pltpu.make_async_copy(psi.at[(site + rels[i]) % 4], psi_v.at[i], sem_psi.at[i]),
            ]
        )
    out_copies = [
        [
            pltpu.make_async_copy(
                acc_v.at[i, pl.ds(192 * w, 192)], out.at[i, pl.ds(192 * w, 192)], sem_out.at[i, w]
            )
            for w in range(4)
        ]
        for i in range(groups)
    ]
    for copy in left_copies + copies[0]:
        copy.start()
    acc_v[0] = jnp.zeros(acc_v.shape[1:], jnp.float32)
    for copy in left_copies:
        copy.wait()

    def one_group(i, carry):
        for j in range(groups):

            @pl.when(i == j)
            def _():
                for copy in copies[j]:
                    copy.wait()
                if j + 1 < groups:
                    for copy in copies[j + 1]:
                        copy.start()
                    acc_v[j + 1] = jnp.zeros(acc_v.shape[1:], jnp.float32)

        def one_pair(p, inner):
            lefts = [lambda within, u=u: left_v[2 * p + u, within] for u in range(2)]
            block = [
                lambda q, u=u: jnp.concatenate(
                    [right_v[i, q // 2, 2 * p + u, q % 2], right_v[i, q // 2, 2 * p + u, 2]], axis=1
                )
                for u in range(2)
            ]
            multiply_slots(lefts, block, psi_v.at[i], image, acc_v.at[i], 2 * p + 1 < live)
            return inner

        lax.fori_loop(0, (live + 1) // 2, one_pair, 0)
        for j in range(groups):

            @pl.when(i == j)
            def _():
                for copy in out_copies[j]:
                    copy.start()

        return carry

    lax.fori_loop(0, groups, one_group, 0)
    for found in out_copies:
        for copy in found:
            copy.wait()


def products(rels, where, count, left, psi, rights):
    groups = len(rels)
    smem = pl.BlockSpec(memory_space=pltpu.SMEM)
    hbm = pl.BlockSpec(memory_space=pltpu.HBM)
    flops = groups * 2 * 1024 * 768 * (192 + 256) * 4
    return pl.pallas_call(
        functools.partial(products_body, tuple(rels)),
        in_specs=[smem, smem, hbm, hbm] + [hbm] * (2 * groups),
        out_specs=hbm,
        out_shape=jax.ShapeDtypeStruct((groups, 768, GROUP_COLS), jnp.float32),
        scratch_shapes=[
            pltpu.VMEM((CHUNK, 4, 192, 192), jnp.bfloat16),
            pltpu.VMEM((groups, 2, CHUNK, 3, 192, 128), jnp.bfloat16),
            pltpu.VMEM((groups, 768, GROUP_COLS), jnp.bfloat16),
            pltpu.VMEM((2, 768, GROUP_COLS), jnp.bfloat16),
            pltpu.VMEM((groups, 768, GROUP_COLS), jnp.float32),
            pltpu.SemaphoreType.DMA((2,)),
            pltpu.SemaphoreType.DMA((groups, 2)),
            pltpu.SemaphoreType.DMA((groups,)),
            pltpu.SemaphoreType.DMA((groups, 4)),
        ],
        compiler_params=params(),
        cost_estimate=pl.CostEstimate(flops=flops, bytes_accessed=8 * 2**20, transcendentals=0),
        name="products",
    )(where, count, left, psi, *[half for halves in rights for half in halves])


def finish_body(slots, where, count, table, own, near, far_a, far_b, left, psi, *refs):
    live = jnp.minimum(count[0], CHUNK)
    rows, subspace, energies, right_energy = refs[:4]
    refs = list(refs[4:])
    if slots:
        flags, extras, moved = refs[0], refs[1:5], refs[5:8]
        there = [flags[k] > 0 for k in range(4)]
        refs = refs[8:]
    send, mine, proj, left_v, right_v, psi_v, image, acc_v, rows_v, sub_v, total, staged, sums = refs[:13]
    sem_left, sem_right, sem_psi, sem_acc, sem_rows, sem_sub, sem_out = refs[13:20]
    width = subspace.shape[3]
    core = where[CORE]
    site = where[SITE]
    member = where[MEMBER]

    left_copies = [
        pltpu.make_async_copy(left.at[pl.ds(2 * p, 2)], left_v.at[pl.ds(2 * p, 2)], sem_left.at[p])
        for p in range(2)
    ]
    far_copies = [
        pltpu.make_async_copy(far_a, right_v.at[0], sem_right.at[0]),
        pltpu.make_async_copy(far_b, right_v.at[1], sem_right.at[1]),
    ]
    psi_copies = {
        i: pltpu.make_async_copy(psi.at[(site + i) % 4], psi_v.at[i], sem_psi.at[i])
        for i in ((2, 0, 1, 3) if slots else (2,))
    }
    acc_copies = [
        pltpu.make_async_copy(
            source.at[at, pl.ds(192 * w, 192)], acc_v.at[rel, pl.ds(192 * w, 192)], sem_acc.at[rel, w]
        )
        for rel, source, at in ((0, own, 0), (1, near, 0), (3, near, 1))
        for w in range(4)
    ]
    their = jnp.minimum(member, 768 // DIAGONAL_ROWS - 1)
    rows_copy = pltpu.make_async_copy(
        rows.at[pl.ds(pl.multiple_of(DIAGONAL_ROWS * their, DIAGONAL_ROWS), DIAGONAL_ROWS)],
        rows_v,
        sem_rows,
    )

    def sub_copies(step):
        within = 2 * ((1 - core) if step < 2 else core) + step % 2
        return [
            pltpu.make_async_copy(subspace.at[k, within], sub_v.at[step, k], sem_sub.at[step, k]) for k in range(2)
        ]

    for copy in left_copies + far_copies:
        copy.start()
    psi_copies[2].start()
    if slots:
        extra_v, moved_v, sem_extra, sem_moved = refs[20:]
        extra_copies = []
        for k in range(4):
            place = 0 if slots == 1 else k
            source = extras[k].at[pl.ds(0, 12)]
            copy = pltpu.make_async_copy(source, extra_v.at[place], sem_extra.at[place])
            extra_copies.append((flags[4] == k if slots == 1 else there[k], copy))
        moved_copies = [
            pltpu.make_async_copy(moved[i], moved_v.at[i + 1], sem_moved.at[i]) for i in range(3)
        ]
    acc_v[2] = jnp.zeros(acc_v.shape[1:], jnp.float32)
    for copy in left_copies + far_copies:
        copy.wait()
    psi_copies[2].wait()

    for copy in acc_copies:
        copy.start()
    if slots:
        for wanted, copy in extra_copies:

            @pl.when(wanted)
            def _():
                copy.start()

        for i in (0, 1, 3):
            psi_copies[i].start()
        for copy in moved_copies:
            copy.start()
    else:
        rows_copy.start()
        for step in range(4):
            for copy in sub_copies(step):
                copy.start()

    def one_pair(p, inner):
        lefts = [lambda within, u=u: left_v[2 * p + u, within] for u in range(2)]
        blocks = [
            lambda q, u=u: jnp.concatenate(
                [right_v[q // 2, 2 * p + u, q % 2], right_v[q // 2, 2 * p + u, 2]], axis=1
            )
            for u in range(2)
        ]
        multiply_slots(lefts, blocks, psi_v.at[2], image, acc_v.at[2], 2 * p + 1 < live)
        return inner

    lax.fori_loop(0, (live + 1) // 2, one_pair, 0)
    for copy in acc_copies:
        copy.wait()
    if slots:
        for wanted, copy in extra_copies:

            @pl.when(wanted)
            def _():
                copy.wait()

        for i in (0, 1, 3):
            psi_copies[i].wait()
        for copy in moved_copies:
            copy.wait()
        rows_copy.start()
        for step in range(4):
            for copy in sub_copies(step):
                copy.start()
        moved_v[0] = extra_v[:, 6:12]
        alive = [jnp.int32(1)] if slots == 1 else [one.astype(jnp.int32) for one in there]

        def one_group(i, carry):
            def one_slot(n, inner):
                wanted = alive[0]
                for k in range(1, slots):
                    wanted = jnp.where(n == k, alive[k], wanted)

                @pl.when(wanted > 0)
                def _():
                    def left_block(within):
                        at = 3 * (within // 2)
                        lane = 64 * (within % 2)
                        high = extra_v[n, at + 2]
                        return jnp.concatenate([extra_v[n, at + within % 2], high[:, lane : lane + 64]], axis=1)

                    def right_block(q):
                        at = 3 * (q // 2)
                        return jnp.concatenate([moved_v[i, n, at + q % 2], moved_v[i, n, at + 2]], axis=1)

                    multiply_slots([left_block], [right_block], psi_v.at[i], image, acc_v.at[i], None)

                return inner

            lax.fori_loop(0, slots, one_slot, 0)
            return carry

        lax.fori_loop(0, 4, one_group, 0)
    rows_copy.wait()

    lane = lax.broadcasted_iota(jnp.int32, (192, 128), 1)
    row = lax.broadcasted_iota(jnp.int32, (192, width), 0)
    sums[...] = jnp.zeros(sums.shape, jnp.float32)

    def out_copy(step):
        out = send if step < 2 else mine
        return pltpu.make_async_copy(staged.at[step], out.at[pl.ds(192 * (step % 2), 192)], sem_out.at[step])

    def one_block(step, carry):
        for j in range(4):

            @pl.when(step == j)
            def _():
                for copy in sub_copies(j):
                    copy.wait()

        within = 2 * jnp.where(step < 2, 1 - core, core) + step % 2
        here = pl.ds(pl.multiple_of(192 * within, 192), 192)

        def one_site(i, inner):
            rel = (i + 4 - site) % 4
            for q in range(4):
                start = table[RIGHT_START + 4 * i + q]
                base = pl.multiple_of((start // 128) * 128, 128)
                shift = start - base
                first = pltpu.roll(acc_v[rel, here, q * SLOT_COLS : q * SLOT_COLS + 128], shift, 1)
                second = pltpu.roll(acc_v[rel, here, q * SLOT_COLS + 128 : (q + 1) * SLOT_COLS], shift, 1)
                low = lane < shift
                total[:, pl.ds(base, 128)] = jnp.where(low, total[:, pl.ds(base, 128)], first)
                total[:, pl.ds(base + 128, 128)] = jnp.where(low, first, second)
                total[:, pl.ds(base + 256, 128)] = second
            return inner

        lax.fori_loop(0, 4, one_site, 0)
        per = 192 // DIAGONAL_ROWS

        @pl.when(member // per == within)
        def _():
            at = pl.multiple_of(DIAGONAL_ROWS * (member % per), DIAGONAL_ROWS)
            part = pl.ds(at, DIAGONAL_ROWS)
            energy = energies[pl.ds(pl.multiple_of(192 * within + at, DIAGONAL_ROWS), DIAGONAL_ROWS), :]
            total[part, :width] += (energy + right_energy[...]) * rows_v[...].astype(jnp.float32)

        kept = jnp.where(row < table[MY_SIZE + within], total[:, :width], 0.0)
        for k in range(2):
            part = sub_v[step, k].astype(jnp.float32) * kept
            sums[k] += jnp.sum(part.reshape(24, 8, width), axis=0)
        staged[step] = kept.astype(jnp.bfloat16)
        for j in range(4):

            @pl.when(step == j)
            def _():
                out_copy(j).start()

        return carry

    lax.fori_loop(0, 4, one_block, 0)
    for k in range(2):
        added = sums[k, :, :128]
        for j in range(1, width // 128):
            added = added + sums[k, :, 128 * j : 128 * (j + 1)]
        proj[k] = added
    for j in range(4):
        out_copy(j).wait()


def finish(slots, where, count, table, own, near, far, left, psi, rows, subspace, energies, right_energy, late=()):
    width = rows.shape[1]
    smem = pl.BlockSpec(memory_space=pltpu.SMEM)
    hbm = pl.BlockSpec(memory_space=pltpu.HBM)
    vmem = pl.BlockSpec(memory_space=pltpu.VMEM)
    half = jax.ShapeDtypeStruct((384, width), jnp.bfloat16)
    scratch = [
        pltpu.VMEM((CHUNK, 4, 192, 192), jnp.bfloat16),
        pltpu.VMEM((2, CHUNK, 3, 192, 128), jnp.bfloat16),
        pltpu.VMEM((4, 768, GROUP_COLS), jnp.bfloat16),
        pltpu.VMEM((2, 768, GROUP_COLS), jnp.bfloat16),
        pltpu.VMEM((4, 768, GROUP_COLS), jnp.float32),
        pltpu.VMEM((DIAGONAL_ROWS, width), jnp.bfloat16),
        pltpu.VMEM((4, 2, 192, width), jnp.bfloat16),
        pltpu.VMEM((192, width + 256), jnp.float32),
        pltpu.VMEM((4, 192, width), jnp.bfloat16),
        pltpu.VMEM((2, 8, width), jnp.float32),
        pltpu.SemaphoreType.DMA((2,)),
        pltpu.SemaphoreType.DMA((2,)),
        pltpu.SemaphoreType.DMA((4,)),
        pltpu.SemaphoreType.DMA((4, 4)),
        pltpu.SemaphoreType.DMA(()),
        pltpu.SemaphoreType.DMA((4, 2)),
        pltpu.SemaphoreType.DMA((4,)),
    ]
    if slots:
        scratch += [
            pltpu.VMEM((slots, 12, 192, 128), jnp.bfloat16),
            pltpu.VMEM((4, slots, 6, 192, 128), jnp.bfloat16),
            pltpu.SemaphoreType.DMA((4,)),
            pltpu.SemaphoreType.DMA((3,)),
        ]
    return pl.pallas_call(
        functools.partial(finish_body, slots),
        in_specs=[smem] * 3 + [hbm] * 8 + [vmem, vmem] + ([smem] + [hbm] * 7 if slots else []),
        out_specs=[hbm, hbm, vmem],
        out_shape=[half, half, jax.ShapeDtypeStruct((2, 8, 128), jnp.float32)],
        scratch_shapes=scratch,
        compiler_params=params(),
        cost_estimate=pl.CostEstimate(flops=8 * 10**9, bytes_accessed=30 * 2**20, transcendentals=0),
        name="finish",
    )(where, count, table, own, near, *far, left, psi, rows, subspace, energies, right_energy, *late)


def place_body(which, where, half, *rest):
    out, sems = rest[-2:]
    core = where[CORE] if which == 0 else 1 - where[CORE]
    copies = [
        pltpu.make_async_copy(
            half.at[n // 6, pl.ds(32 * (n % 6), 32)],
            out.at[2 * core + n // 6, pl.ds(32 * (n % 6), 32)],
            sems.at[n],
        )
        for n in range(12)
    ]
    for copy in copies:
        copy.start()
    for copy in copies:
        copy.wait()


def place(which, where, half, whole=None):
    hbm = pl.BlockSpec(memory_space=pltpu.HBM)
    args = (where, half) if whole is None else (where, half, whole)
    return pl.pallas_call(
        functools.partial(place_body, which),
        in_specs=[pl.BlockSpec(memory_space=pltpu.SMEM), pl.BlockSpec(memory_space=pltpu.VMEM)]
        + [hbm] * (len(args) - 2),
        out_specs=hbm,
        out_shape=jax.ShapeDtypeStruct((4,) + half.shape[1:], half.dtype),
        scratch_shapes=[pltpu.SemaphoreType.DMA((12,))],
        input_output_aliases={} if whole is None else {2: 0},
        cost_estimate=pl.CostEstimate(flops=10**9, bytes_accessed=2**22, transcendentals=0),
        name="place",
    )(*args)


def shifted(value, axis, by):
    size = lax.axis_size(axis)
    return lax.ppermute(value, axis, [(i, (i + by) % size) for i in range(size)])


def small_sum(value, axis):
    size = lax.axis_size(axis)
    me = lax.axis_index(axis)
    got = [value] + [shifted(value, axis, k) for k in range(1, size)]
    total = None
    for source in range(size):
        one = sum(jnp.where((me - source) % size == k, got[k], 0.0) for k in range(size))
        total = one if total is None else total + one
    return total


def local(
    wavefunction,
    left_blocks,
    right_blocks,
    left_sector,
    right_sector,
    term_count,
    left_energy,
    right_energy,
    subspace,
):
    bond = wavefunction.shape[0]
    site = lax.axis_index("site")
    core = lax.axis_index("core")
    mine_early = pack_early(right_blocks)
    prev_first = shifted(mine_early[0], "site", 1)
    next_second = shifted(mine_early[1], "site", -1)
    second_after, first_after, _, _ = lax.optimization_barrier((mine_early[1], mine_early[0], left_blocks, term_count))
    prev = [prev_first, shifted(second_after, "site", 1)]
    following = [shifted(first_after, "site", -1), next_second]
    left_later, right_later, _ = lax.optimization_barrier((left_blocks, right_blocks, mine_early[0]))

    ways = (("y", 1), ("y", -1), ("z", 1), ("z", -1))
    late = pack_late(term_count, left_later, right_later)
    extras = [shifted(late[k], axis, by) for k, (axis, by) in enumerate(ways)]
    flags, branch, going = pick(extras)

    where = jnp.stack([site, core, lax.axis_index(OPS)])
    table, rows, psi, energies = select(where, left_sector, right_sector, left_energy, wavefunction)
    own = products((0,), where, term_count, left_blocks, psi, [mine_early])

    far = (shifted(prev[0], "site", 1), shifted(following[1], "site", -1))
    moved = [shifted(going, "site", by) for by in (-1, 2, 1)]
    near = products((1, 3), where, term_count, left_blocks, psi, [following, prev])

    def rest(slots, late):
        return tuple(
            finish(
                slots,
                where,
                term_count,
                table,
                own,
                near,
                far,
                left_blocks,
                psi,
                rows,
                subspace,
                energies,
                right_energy[None, :],
                late=late,
            )
        )

    def none():
        return rest(0, [])

    def one():
        return rest(1, [flags, *extras, *moved])

    def many():
        every = jnp.stack([one[6:12] for one in extras])
        return rest(4, [flags, *extras] + [shifted(every, "site", by) for by in (-1, 2, 1)])

    send, mine, proj = lax.switch(branch[0], [none, one, many])
    swap = [(0, 1), (1, 0)]
    away = lax.ppermute(send, "core", swap)
    proj = small_sum(jnp.broadcast_to(jnp.sum(proj, axis=(1, 2))[None, :], (8, 2)), "site")[0]
    both = (mine.astype(jnp.float32) + away.astype(jnp.float32)).astype(jnp.bfloat16)

    high = lax.reduce_precision(proj, 8, 7)
    middle = lax.reduce_precision(proj - high, 8, 7)
    thirds = jnp.concatenate([high, middle, proj - high - middle]).astype(jnp.bfloat16)
    plane = lax.axis_size(("z", "y"))
    half = both.shape[0]
    share = half // plane
    extra = jnp.broadcast_to(jnp.pad(thirds, (0, EXTRA - 6))[None, :], (half, EXTRA))
    both = jnp.concatenate([both, extra], axis=1)

    pieces = lax.all_to_all(both.reshape(plane, share, bond + EXTRA), ("z", "y"), 0, 0, tiled=True)
    added = jnp.sum(pieces.astype(jnp.float32), axis=0)
    summed = added[:, :bond].astype(jnp.bfloat16)
    gathered = lax.all_to_all(
        jnp.broadcast_to(summed[None], (plane, share, bond)), ("z", "y"), 0, 0, tiled=True
    ).reshape(half, bond)
    whole = added[:8, bond : bond + 2] + added[:8, bond + 2 : bond + 4] + added[:8, bond + 4 : bond + 6]
    gathered = gathered.reshape(2, 192, bond)
    other = lax.ppermute(gathered, "core", swap)
    placed = place(0, where, gathered)
    whole_beside = lax.ppermute(whole, "core", swap)
    projections = whole + whole_beside
    sigma = place(1, where, other, placed)
    return sigma, projections[0]


def solution(mesh):
    shape = dict(mesh.shape)
    ops = shape["ops"]
    parts = Mesh(mesh.devices.reshape(4, ops // 8, 2, shape["site"]), ("z", "y", "core", "site"))
    in_specs = (
        P(),
        P(OPS, "site", None, None),
        P(OPS, "site", None, None),
        P(),
        P(),
        P(OPS),
        P(),
        P(),
        P(None, "site", None, None),
    )
    out_specs = (P("site", None, None), P())
    return jax.shard_map(local, mesh=parts, in_specs=in_specs, out_specs=out_specs, check_vma=False)
```
